32 devices in a mesh: gx: 4 (over y, core), gy: 2 (over x), gz: 4 (over z).
Axes of the slice: x: 2, y: 2, z: 4, core: 2. Of those that a mesh axis runs over, the one named last changes fastest.
Arguments:
- old_basis: float32 [4, 32, 32, 512], P(None, 'gx', 'gy', 'gz'), may hold values from -4 to 4, as said below
- previous: float32 [4, 32, 32, 512], P(None, 'gx', 'gy', 'gz'), as said below
- incoming: float32 [4, 32, 32, 512], P(None, 'gx', 'gy', 'gz'), may hold values from -6 to 6
- coefficient: float32 [32, 32, 512], P('gx', 'gy', 'gz'), may hold values from 0.5 to 4
Outputs:
- orthonormal: float32 [4, 32, 32, 512], P(None, 'gx', 'gy', 'gz')
- projection: float32 [4, 4], replicated
- triangle: float32 [4, 4], replicated
- preconditioned: float32 [4, 32, 32, 512], P(None, 'gx', 'gy', 'gz')
- operated: float32 [4, 32, 32, 512], P(None, 'gx', 'gy', 'gz')
The draws below stay inside these ranges and needn't reach their ends.
Inputs may be any that keep to these rules, and one draw needn't show every extreme that they name: `old_basis`: entries of order one; the basis vectors are independent, so every Gram matrix formed from them is well conditioned. `previous`: entries of order one; each vector has a part outside the span of old_basis of norm of order one under the inner product.
All inputs are finite; a program needn't handle non-finite values.
Results may differ from the reference program's by a relative error of at most 0.0003.
Values sent between devices are 32-bit elements; how exact they have to be, the bound alone decides.
No kernel may reach another device: no remote copies, remote signals or barrier semaphores. Data moves between devices by JAX's collectives and lax.ppermute only.
A program may use at most 64 MiB of HBM per device.

```python
import math
import jax
import jax.numpy as jnp
from jax import lax

BLOCK = 4
BASIS = 4
LEVELS = 6
COARSE_SWEEPS = 4
NX = 32
NY = 32
NZ = 512


def joint_draw(key):
    inner = jax.random.fold_in(key, 4242)
    basis = jax.random.truncated_normal(jax.random.fold_in(inner, 1), -4.0, 4.0, (BASIS, NX, NY, NZ), jnp.float32)
    mixing = jax.random.truncated_normal(jax.random.fold_in(inner, 2), -2.0, 2.0, (BASIS, BLOCK), jnp.float32)
    noise = jax.random.truncated_normal(jax.random.fold_in(inner, 3), -4.0, 4.0, (BLOCK, NX, NY, NZ), jnp.float32)
    ramp_x = 1.0 + 2.0 * jnp.arange(NX, dtype=jnp.float32) / max(NX - 1, 1)
    noise = noise * ramp_x[None, :, None, None]
    combined = jnp.einsum('mj,mxyz->jxyz', mixing, basis) + noise
    return (basis, combined)


def draw_old_basis(key, part):
    return joint_draw(key)[0]


def draw_previous(key, part):
    return joint_draw(key)[1]


def block_levels(own_key, extent, shards, low, top_value):
    def one(position, blocks):
        steps = jax.random.uniform(jax.random.fold_in(jax.random.fold_in(own_key, 6), position), (blocks,), jnp.float32, low / len(shards), top_value / len(shards))
        return jnp.repeat(jnp.exp(steps), extent[position] // blocks).reshape((-1,) + (1,) * (len(extent) - position - 1))

    loudness = one(*shards[0])
    for cut in shards[1:]:
        loudness = loudness * one(*cut)
    return loudness


def bell_draw(own_key, extent, width, reach, split=(), kind=jnp.bfloat16):
    gain = block_levels(own_key, extent, split, -0.22, 0.18) if split else 1.0
    values = jax.random.normal(own_key, extent, jnp.float32) * width * gain
    return jnp.minimum(jnp.maximum(values, -reach), reach).astype(kind)


def setup_inputs(seed: int = 0) -> dict:
    arg_keys = jax.random.split(jax.random.key(seed), 5)
    return {
        "old_basis": draw_old_basis(jax.random.fold_in(arg_keys[4], 71), 0),
        "previous": draw_previous(jax.random.fold_in(arg_keys[4], 71), 0),
        "incoming": bell_draw(arg_keys[2], (BLOCK, NX, NY, NZ), 1.0, 6.0, ((1, 4), (2, 2), (3, 4)), jnp.float32),
        "coefficient": jnp.clip(jnp.exp(math.log(4.0) - 2.0794415 * jax.random.uniform(arg_keys[3], (NX, NY, NZ), jnp.float32) ** block_levels(arg_keys[3], (NX, NY, NZ), ((0, 4), (1, 2), (2, 4)), -0.2, 0.2)), 0.5, 4.0),
    }


OMEGA = 0.8
HIGH = lax.Precision.HIGHEST

def neighbours(field):
    padded = jnp.pad(field, ((0, 0), (1, 1), (1, 1), (1, 1)))
    total = padded[:, 2:, 1:-1, 1:-1] + padded[:, :-2, 1:-1, 1:-1]
    total = total + padded[:, 1:-1, 2:, 1:-1] + padded[:, 1:-1, :-2, 1:-1]
    total = total + padded[:, 1:-1, 1:-1, 2:] + padded[:, 1:-1, 1:-1, :-2]
    return total

def apply_operator(field, coeffs, factor):
    return factor * coeffs * (6.0 * field - neighbours(field))

def restrict(field):
    depth, size_a, size_b, size_c = field.shape
    return field.reshape(depth, size_a // 2, 2, size_b // 2, 2, size_c // 2, 2).mean(axis=(2, 4, 6))

def prolong(field):
    return jnp.repeat(jnp.repeat(jnp.repeat(field, 2, axis=1), 2, axis=2), 2, axis=3)

def vcycle(source, coeff_list, level):
    coeffs = coeff_list[level]
    factor = 0.25 ** level
    diagonal = 6.0 * factor * coeffs
    iterate = OMEGA * source / diagonal
    if level == LEVELS - 1:
        for sweep in range(COARSE_SWEEPS - 1):
            iterate = iterate + OMEGA * (source - apply_operator(iterate, coeffs, factor)) / diagonal
        return iterate
    iterate = iterate + OMEGA * (source - apply_operator(iterate, coeffs, factor)) / diagonal
    residue = source - apply_operator(iterate, coeffs, factor)
    iterate = iterate + prolong(vcycle(restrict(residue), coeff_list, level + 1))
    iterate = iterate + OMEGA * (source - apply_operator(iterate, coeffs, factor)) / diagonal
    return iterate

def triangular_inverse(lower):
    order = lower.shape[0]
    identity = jnp.eye(order, dtype=lower.dtype)
    inverse = jnp.zeros_like(lower)
    for row in range(order):
        values = identity[row] - jnp.dot(lower[row, :row], inverse[:row], precision=HIGH)
        inverse = inverse.at[row].set(values / lower[row, row])
    return inverse

def reference(old_basis, previous, incoming, coefficient):
    total_cells = float(NX * NY * NZ)
    projection = jnp.einsum('mxyz,jxyz->mj', old_basis, previous, precision=HIGH) / total_cells
    remainder = previous - jnp.einsum('mxyz,mj->jxyz', old_basis, projection, precision=HIGH)
    gram = jnp.einsum('ixyz,jxyz->ij', remainder, remainder, precision=HIGH) / total_cells
    lower = jnp.linalg.cholesky(gram)
    inverse = triangular_inverse(lower)
    orthonormal = jnp.einsum('ji,ixyz->jxyz', inverse, remainder, precision=HIGH)
    coeff_list = [coefficient]
    for level in range(LEVELS - 1):
        coeff_list.append(restrict(coeff_list[-1][None])[0])
    preconditioned = vcycle(incoming, coeff_list, 0)
    operated = apply_operator(preconditioned, coefficient, 1.0)
    return (orthonormal, projection, lower.T, preconditioned, operated)
```

```python
import functools

import jax
import jax.numpy as jnp
from jax import lax
from jax.experimental import pallas as pl
from jax.experimental.pallas import tpu as pltpu
from jax.sharding import PartitionSpec as P

LEVELS = 6
COARSE_SWEEPS = 4
OMEGA = 0.8
KEEP = 1.0 - OMEGA
SIXTH = OMEGA / 6.0
PRE_G = OMEGA * (2.0 - OMEGA)
PRE_N = OMEGA * OMEGA / 6.0
AXES = ("gx", "gy", "gz")
HIGH = lax.Precision.HIGHEST
H = 3
NN = (((1,), (0,)), ((), ()))
NT = (((1,), (1,)), ((), ()))
TN = (((0,), (0,)), ((), ()))
VM = pl.BlockSpec(memory_space=pltpu.VMEM)


def dot(a, b, dims=NN):
    return lax.dot_general(a, b, dims, precision=HIGH, preferred_element_type=jnp.float32)


def iota(shape, dim):
    return lax.broadcasted_iota(jnp.int32, shape, dim)


def onehot(cond, scale=1.0):
    return jnp.where(cond, jnp.float32(scale), jnp.float32(0.0))


def roll(a, shift, axis):
    size = a.shape[axis]
    shift = shift % size
    return a if shift == 0 else pltpu.roll(a, shift, axis)


class Place:
    def __init__(self, counts):
        self.counts = counts
        self.at = tuple(lax.axis_index(a) for a in AXES)
        self.me = self.linear(self.at)

    def linear(self, p):
        nx, ny, nz = self.counts
        return (p[0] * ny + p[1]) * nz + p[2]

    def lo(self, axis):
        return self.at[axis] > 0

    def hi(self, axis):
        return self.at[axis] < self.counts[axis] - 1

    def has(self, d):
        ok = None
        for axis in range(3):
            if d[axis]:
                one = self.hi(axis) if d[axis] > 0 else self.lo(axis)
                ok = one if ok is None else jnp.logical_and(ok, one)
        return ok

    def slot(self, d):
        there = self.linear(tuple(p + s for p, s in zip(self.at, d)))
        return jnp.where(self.has(d), there, self.me)


def f32(flag):
    return jnp.where(flag, jnp.float32(1.0), jnp.float32(0.0))


def keep(flag, a):
    return jnp.where(flag, a, jnp.zeros_like(a))


def fill_slots(ref, count, value, rows):
    if count <= 64:
        for t in range(count):
            ref[t, 0:rows] = value
    else:
        def body(t, carry):
            ref[t, 0:rows] = value
            return carry
        lax.fori_loop(0, count, body, 0)


def first_kernel(counts, merge_y, inc, c, *refs):
    if merge_y:
        g, xlo, xhi, ymsg, slots, c2p = refs
    else:
        g, xlo, xhi, ylo, yhi, slots, c2p = refs
    V, X, Y, Z = inc.shape
    place = Place(counts)
    for x in range(X):
        scale = 1.0 / (6.0 * c[x])
        for v in range(V):
            value = inc[v, x] * scale
            g[v, x] = value
            if x < H:
                xlo[v, x] = value
            if x >= X - H:
                xhi[v, x - (X - H)] = value
    sub = iota((8, Z), 0)

    def packed(v, j, start, own):
        return jnp.where(own, g[v, 2 * j, pl.ds(start, 8)], roll(g[v, 2 * j + 1, pl.ds(start, 8)], 4, 0))

    for v in range(V):
        for j in range(X // 2):
            if merge_y:
                up = place.at[1] == 0
                start = pl.multiple_of(jnp.where(up, Y - 8, 0), 8)
                own = (sub + jnp.where(up, 0, 4)) % 8 >= 4
                ymsg[v, j] = packed(v, j, start, own)
            else:
                yhi[v, j] = packed(v, j, Y - 8, sub >= 4)
                ylo[v, j] = packed(v, j, 0, sub < 4)
    ny2, nz2 = Y // 4, Z // 4
    total = None
    for y in range(ny2):
        sums = []
        for x in range(X // 4):
            quad = c[4 * x] + c[4 * x + 1] + c[4 * x + 2] + c[4 * x + 3]
            sums.append(jnp.sum(quad[4 * y : 4 * y + 4], axis=0, keepdims=True))
        rows = jnp.where(sub % 2 == 0, sums[0], sums[1])
        li, lo = iota((Z, Z), 0), iota((Z, Z), 1)
        part = dot(rows, onehot(lo == y * nz2 + li // 4, 1.0 / 64.0))
        total = part if total is None else total + part
    c2p[...] = total
    row, lane = iota((32, Z), 0), iota((32, Z), 1)
    layer = row % 4
    wanted = jnp.where(row < 16, Z - H, 0) + layer
    faces = None
    for v in range(V):
        pick = onehot((lane == wanted) & (layer < H) & ((row % 16) // 4 == v))
        part = dot(pick, g[v].reshape(X * Y, Z), NT)
        faces = part if faces is None else faces + part
    row = iota((16, Z), 0)
    c2_rows = jnp.where(row == 3, total[0:1], jnp.where(row == 7, total[1:2], jnp.zeros((16, Z), jnp.float32)))
    special = (row == 3) | (row == 7)
    up_faces = jnp.where(special, c2_rows, faces[0:16])
    down_faces = jnp.where(special, c2_rows, faces[16:32])
    count = counts[0] * counts[1] * counts[2]
    fill_slots(slots, count, c2_rows[0:8], 8)
    slots[place.me] = c2_rows
    for dx in (-1, 0, 1):
        for dy in (-1, 0, 1):
            slots[place.slot((dx, dy, 1))] = up_faces
            slots[place.slot((dx, dy, -1))] = down_faces
            if dx and dy:
                t = place.slot((dx, dy, 0))
                for cell, (a, b) in enumerate(((0, 0), (0, 1), (1, 0))):
                    x = X - 1 - a if dx > 0 else a
                    y = Y - 1 - b if dy > 0 else b
                    for v in range(V):
                        slots[t, v * 4 + cell] = g[v, x, y]


def spread(cur, below, above, zl, zr):
    return below + above + roll(cur, 1, 0) + roll(cur, -1, 0) + zl + zr


def fine_sum(ref, v, i, V, lane):
    cur = ref[v, i]
    zl, zr = roll(cur, 1, 1), roll(cur, -1, 1)
    if v < V:
        rim = ref[V, i]
        last = lane.shape[1] - 1
        zl = jnp.where(lane == 0, roll(rim, -(16 * v + 2), 1), zl)
        zr = jnp.where(lane == last, roll(rim, last - (16 * v + 10), 1), zr)
    return spread(cur, ref[v, i - 1], ref[v, i + 1], zl, zr)


def fine_masks(place, Y, Z):
    R = Y + 8
    row = iota((R, Z), 0)
    ym = onehot(row < Y) + onehot((row >= Y) & (row < Y + H)) * f32(place.hi(1))
    ym = ym + onehot(row >= R - H) * f32(place.lo(1))
    lane = iota((R, Z), 1)
    k = lane % 8
    outside_lo = ((lane // 8) % 2 == 0) & (k < H)
    outside_hi = ((lane // 8) % 2 == 1) & (k >= 2)
    zm = jnp.where(outside_lo, f32(place.lo(2)), jnp.where(outside_hi, f32(place.hi(2)), jnp.float32(1.0)))
    return ym, ym * zm


def x_flag(place, i, X):
    if i < H:
        return f32(place.lo(0))
    if i >= H + X:
        return f32(place.hi(0))
    return None


def scaled(flag, mask):
    return mask if flag is None else mask * flag


def second_kernel(counts, g, c, xl, xh, yl, yh, slots, gram, G, S, p1, slots1, c1, Q, QC):
    V, X, Y, Z = g.shape
    R = Y + 8
    place = Place(counts)
    sub = iota((8, Z), 0)
    zero8 = jnp.zeros((8, Z), jnp.float32)
    zero_y = jnp.zeros((Y, Z), jnp.float32)
    has_yl, has_yh, has_xl, has_xh = place.lo(1), place.hi(1), place.lo(0), place.hi(0)
    m_hi = jnp.logical_and(sub < H, has_yh)
    m_lo = jnp.logical_and(sub >= 8 - H, has_yl)
    for v in range(V):
        for x in range(X):
            G[v, H + x, 0:Y] = g[v, x]
            hi, lo = yh[v, x // 2], yl[v, x // 2]
            if x % 2:
                hi, lo = roll(hi, 4, 0), roll(lo, 4, 0)
            G[v, H + x, Y:R] = jnp.where(m_hi, hi, jnp.where(m_lo, lo, zero8))
        for i in range(H):
            G[v, i, 0:Y] = keep(has_xl, xl[v, i])
            G[v, i, Y:R] = zero8
            G[v, H + X + i, 0:Y] = keep(has_xh, xh[v, i])
            G[v, H + X + i, Y:R] = zero8
    for dx in (-1, 1):
        for dy in (-1, 1):
            ok, t = place.has((dx, dy, 0)), place.slot((dx, dy, 0))
            for cell, (a, b) in enumerate(((0, 0), (0, 1), (1, 0))):
                i = H + X + a if dx > 0 else H - 1 - a
                r = Y + b if dy > 0 else R - 1 - b
                for v in range(V):
                    G[v, i, r] = keep(ok, slots[t, v * 4 + cell])
    row, lane32 = iota((32, Z), 0), iota((32, Z), 1)
    target = jnp.where(row < 16, 0, 10) + 16 * ((row % 16) // 4) + row % 4
    place_lanes = onehot((lane32 == target) & (row % 4 < H))

    def layers(dx, dy, lanes):
        below, above = (dx, dy, -1), (dx, dy, 1)
        low = keep(place.has(below), slots[place.slot(below)])
        high = keep(place.has(above), slots[place.slot(above)])
        both = jnp.concatenate([low, high], axis=0)
        return dot(both[:, lanes], place_lanes, TN)

    everything = slice(0, X * Y)
    for i in (0, H + X + H - 1):
        G[V, i] = jnp.zeros((R, Z), jnp.float32)
    mid = layers(0, 0, everything)
    up = layers(0, 1, everything)
    down = layers(0, -1, everything)
    for x in range(X):
        G[V, H + x, 0:Y] = mid[x * Y : (x + 1) * Y]
        tile = jnp.where(sub < 2, up[x * Y : x * Y + 8], zero8)
        G[V, H + x, Y:R] = jnp.where(sub >= 6, down[(x + 1) * Y - 8 : (x + 1) * Y], tile)
    for dx in (-1, 1):
        first = slice(0, 2 * Y) if dx > 0 else slice((X - 2) * Y, X * Y)
        side = layers(dx, 0, first)
        base = H + X if dx > 0 else H - 2
        for a in range(2):
            G[V, base + a, 0:Y] = side[a * Y : (a + 1) * Y]
            G[V, base + a, Y:R] = zero8
        near = slice(0, Y) if dx > 0 else slice((X - 1) * Y, X * Y)
        up = layers(dx, 1, near)
        down = layers(dx, -1, near)
        tile = jnp.where(sub < 2, up[0:8], zero8)
        G[V, H + X if dx > 0 else H - 1, Y:R] = jnp.where(sub >= 6, down[Y - 8 : Y], tile)
    lane = iota((R, Z), 1)
    for i in range(1, 2 * H + X - 1):
        rim = G[V, i]
        for v in range(V):
            body = G[v, i]
            rim = jnp.where((lane == 16 * v + 3) | (lane == 16 * v + 4), roll(body, 16 * v + 3, 1), rim)
            rim = jnp.where((lane == 16 * v + 8) | (lane == 16 * v + 9), roll(body, 16 * v + 10, 1), rim)
        G[V, i] = rim
    ym, zm = fine_masks(place, Y, Z)
    for i in range(1, 2 * H + X - 1):
        flag = x_flag(place, i, X)
        for v in range(V + 1):
            mask = scaled(flag, ym if v < V else zm)
            S[v, i] = mask * (PRE_G * G[v, i] + PRE_N * fine_sum(G, v, i, V, lane))
    for x in range(X // 2):
        for v in range(V):
            total = None
            for i in (2 * x, 2 * x + 1):
                inner = 6.0 * (G[v, H + i] - S[v, H + i]) + fine_sum(S, v, H + i, V, lane)
                part = c[i] * inner[0:Y]
                total = part if total is None else total + part
            Q[pl.ds((v * (X // 2) + x) * Y, Y)] = total
        QC[pl.ds(x * Y, Y)] = c[2 * x] + c[2 * x + 1]
    li, lo = iota((Z, Z), 0), iota((Z, Z), 1)
    halve = onehot(lo == li // 2, 0.125)
    n, nc = V * X * Y // 4, X * Y // 4
    b1 = dot(Q[pl.ds(0, n, stride=2)] + Q[pl.ds(1, n, stride=2)], halve)
    cc = dot(QC[pl.ds(0, nc, stride=2)] + QC[pl.ds(1, nc, stride=2)], halve)
    c1[...] = cc.reshape(X // 2, Y // 2, Z)
    scale = 1.0 / (1.5 * jnp.where(iota((nc, Z), 1) < Z // 2, cc, jnp.float32(1.0)))
    U = jnp.concatenate([b1[v * nc : (v + 1) * nc] * scale for v in range(V)], axis=0)
    per = nc
    for vp in range(V // 2):
        both = U[2 * vp * per : (2 * vp + 1) * per] + roll(U[(2 * vp + 1) * per : (2 * vp + 2) * per], Z // 2, 1)
        p1[vp] = both.reshape(X // 2, Y // 2, Z)
    half = Z // 2
    row, lane8 = iota((8, Z), 0), iota((8, Z), 1)
    wanted = jnp.where(row < H, row, half - 2 * H + row)
    faces = dot(onehot((lane8 == wanted) & (row < 2 * H)), U, NT)
    gram_row = gram[0:1]
    base = jnp.where(row == 6, gram_row, zero8)
    faces = jnp.where(row < 6, faces, base)
    fill_slots(slots1, counts[0] * counts[1] * counts[2], base, 8)
    X1, Y1 = X // 2, Y // 2
    for dx in (-1, 0, 1):
        for dy in (-1, 0, 1):
            slots1[place.slot((dx, dy, 1))] = faces
            slots1[place.slot((dx, dy, -1))] = faces
            if dx and dy:
                t = place.slot((dx, dy, 0))
                for vp in range(V // 2):
                    slots1[t, vp] = p1[vp, X1 - 1 if dx > 0 else 0, Y1 - 1 if dy > 0 else 0]


EDGE = ((0, 0), (0, 1), (1, 0))


def edge_steps(merge_y):
    return [(dx, dy) for dx in (1, -1) for dy in ((0,) if merge_y else (1, -1))]


def coarse_masks(place, R, Z):
    half = Z // 2
    row, lane = iota((R, Z), 0), iota((R, Z), 1)
    y = R // 2
    mask = onehot(row < y) + onehot((row >= y) & (row < y + H)) * f32(place.hi(1))
    mask = mask + onehot(row >= R - H) * f32(place.lo(1))
    lanes = onehot(lane < half) + onehot((lane >= half) & (lane < half + H)) * f32(place.hi(2))
    lanes = lanes + onehot(lane >= Z - H) * f32(place.lo(2))
    return mask * lanes


def level1_sum(get, i):
    cur = get(i)
    return spread(cur, get(i - 1), get(i + 1), roll(cur, 1, 1), roll(cur, -1, 1))


def third_kernel(counts, merge_y, p1, c1, xl, xh, yl, yh, slots, c2p, G1, S1, slots2, *refs):
    edges, Q = refs[:-1], refs[-1]
    VP, X, Y, Z = p1.shape
    V, R, half = 2 * VP, 2 * Y, Z // 2
    place = Place(counts)
    row, lane = iota((Y, Z), 0), iota((Y, Z), 1)
    zero = jnp.zeros((Y, Z), jnp.float32)

    def unpack(tile, v):
        return jnp.where(lane < half, roll(tile, half, 1) if v % 2 else tile, zero)

    r16, l16 = iota((16, Z), 0), iota((16, Z), 1)
    target = jnp.where(r16 < 8, Z - 2 * H + r16, half + r16 - 8)
    used = ((r16 >= H) & (r16 < 2 * H)) | ((r16 >= 8) & (r16 < 8 + H))
    place_lanes = onehot((l16 == target) & used)

    def layers(dx, dy):
        below, above = (dx, dy, -1), (dx, dy, 1)
        low = keep(place.has(below), slots[place.slot(below)])
        high = keep(place.has(above), slots[place.slot(above)])
        return dot(jnp.concatenate([low, high], axis=0), place_lanes, TN)

    mid, up, down = layers(0, 0), layers(0, 1), layers(0, -1)
    m_hi = jnp.logical_and(row < H, place.hi(1))
    m_lo = jnp.logical_and(row >= Y - H, place.lo(1))

    def tile_of(d, v, x):
        k = (v * X + x) * Y
        return d[k : k + Y]

    for v in range(V):
        for x in range(X):
            G1[v, H + x, 0:Y] = unpack(p1[v // 2, x], v) + tile_of(mid, v, x)
            hi = unpack(yh[v // 2, x], v) + tile_of(up, v, x)
            lo = unpack(yl[v // 2, x], v) + tile_of(down, v, x)
            G1[v, H + x, Y:R] = jnp.where(m_hi, hi, jnp.where(m_lo, lo, zero))
    for dx in (-1, 1):
        side, up, down = layers(dx, 0), layers(dx, 1), layers(dx, -1)
        src = xh if dx > 0 else xl
        ok = place.hi(0) if dx > 0 else place.lo(0)
        for v in range(V):
            for a in range(H):
                x = a if dx > 0 else X - 1 - a
                i = H + X + a if dx > 0 else H - 1 - a
                G1[v, i, 0:Y] = keep(ok, unpack(src[v // 2, x], v) + tile_of(side, v, x))
                tile = zero
                if a < 2:
                    tile = jnp.where(m_hi, tile_of(up, v, x), jnp.where(m_lo, tile_of(down, v, x), zero))
                G1[v, i, Y:R] = tile
        for dy in (-1, 1):
            ok, t = place.has((dx, dy, 0)), place.slot((dx, dy, 0))
            i = H + X if dx > 0 else H - 1
            r = Y if dy > 0 else R - 1
            for v in range(V):
                line = slots[t, pl.ds(v // 2, 1)]
                line = roll(line, half, 1) if v % 2 else line
                line = jnp.where(lane[0:1] < half, line, jnp.zeros((1, Z), jnp.float32))
                G1[v, i, pl.ds(r, 1)] = G1[v, i, pl.ds(r, 1)] + keep(ok, line)
    mask = coarse_masks(place, R, Z)
    for i in range(1, 2 * H + X - 1):
        m = scaled(x_flag(place, i, X), mask)
        for v in range(V):
            get = lambda j: G1[v, j]
            S1[v, i] = m * (PRE_G * G1[v, i] + PRE_N * level1_sum(get, i))
    for ref, (dx, dy) in zip(edges, edge_steps(merge_y)):
        for cell, (a, b) in enumerate(EDGE):
            i = H + X - 1 - a if dx > 0 else H + a
            if dy == 0:
                y = jnp.where(place.at[1] == 0, Y - 1 - b, b)
            else:
                y = Y - 1 - b if dy > 0 else b
            for vp in range(VP):
                one, two = S1[2 * vp, i, pl.ds(y, 1)], S1[2 * vp + 1, i, pl.ds(y, 1)]
                ref[pl.ds(cell * VP + vp, 1)] = jnp.where(lane[0:1] < half, one, roll(two, half, 1))
                if cell:
                    ref[pl.ds((2 + cell) * VP + vp, 1)] = p1[vp, i - H, pl.ds(y, 1)]
    for x in range(X // 2):
        for v in range(V):
            total = None
            for i in (2 * x, 2 * x + 1):
                get = lambda j: S1[v, j]
                inner = 6.0 * (G1[v, H + i] - S1[v, H + i]) + level1_sum(get, H + i)
                part = c1[i] * inner[0:Y]
                total = part if total is None else total + part
            Q[pl.ds((v * (X // 2) + x) * Y, Y)] = total
    li, lo = iota((Z, Z), 0), iota((Z, Z), 1)
    rows = V * X // 2
    msg = None
    for y in range(Y // 2):
        pair = Q[pl.ds(2 * y, rows, stride=Y)] + Q[pl.ds(2 * y + 1, rows, stride=Y)]
        part = dot(pair, onehot((lo == y * (half // 2) + li // 2) & (li < half), 0.25 * 0.125))
        msg = part if msg is None else msg + part
    msg = msg / (6.0 * 0.0625 * c2p[...])
    fill_slots(slots2, counts[0] * counts[1] * counts[2], msg, 8)


def coarse_kernel(counts, parts_y, slots0, slots2, out, W, pre):
    nx, ny, nz = counts
    Z = 128
    place = Place(counts)
    width = Z // parts_y
    row, lane = iota((8, Z), 0), iota((8, Z), 1)
    odd = row % 2 == 1
    zero = jnp.zeros((8, Z), jnp.float32)

    def assemble(tile):
        grid = []
        for y in range(ny):
            for j in range(parts_y):
                line = []
                for x in range(nx):
                    acc = zero
                    for z in range(nz):
                        moved = roll(tile[(x * ny + y) * nz + z], width * (z - j), 1)
                        acc = jnp.where(lane // width == z, moved, acc)
                    line.append(acc)
                grid.append(line)
        return grid

    count = nx * ny * nz
    g2 = assemble([slots2[t] for t in range(count)])
    c2 = assemble([jnp.where(odd, slots0[t, pl.ds(7, 1)], slots0[t, pl.ds(3, 1)]) for t in range(count)])

    def at(v, y, x):
        inside = 0 <= y < len(v) and 0 <= x < len(v[0])
        return v[y][x] if inside else None

    def add(*terms):
        total = None
        for term in terms:
            if term is not None:
                total = term if total is None else total + term
        return total

    def neighbours(v, level, length):
        rows = [[roll(t, -1, 0) for t in line] for line in v] if level == 2 else None
        back = [[roll(t, 1, 0) for t in line] for line in v] if level == 2 else None
        result = []
        for y in range(len(v)):
            line = []
            for x in range(len(v[0])):
                t = v[y][x]
                zs = jnp.where(lane == 0, zero, roll(t, 1, 1)) + jnp.where(lane == length - 1, zero, roll(t, -1, 1))
                ys = add(zs, at(v, y - 1, x), at(v, y + 1, x))
                if level == 2:
                    xs = jnp.where(odd, add(back[y][x], at(back, y, x + 1)), add(rows[y][x], at(rows, y, x - 1)))
                    line.append(ys + xs)
                else:
                    line.append(add(ys, at(v, y, x - 1), at(v, y, x + 1)))
            result.append(line)
        return result

    def combine(fn, *grids):
        return [[fn(*ts) for ts in zip(*lines)] for lines in zip(*grids)]

    li, lo = iota((Z, Z), 0), iota((Z, Z), 1)
    halve = onehot(lo == li // 2, 0.125)
    double = onehot(li == lo // 2)

    def lanes(grid, matrix):
        flat = [t for line in grid for t in line]
        moved = dot(jnp.concatenate(flat, axis=0) if len(flat) > 1 else flat[0], matrix)
        w = len(grid[0])
        return [[moved[(y * w + x) * 8 : (y * w + x + 1) * 8] for x in range(w)] for y in range(len(grid))]

    def shrink(v, level):
        v = [[a + b for a, b in zip(v[2 * y], v[2 * y + 1])] for y in range(len(v) // 2)]
        if level == 2:
            v = combine(lambda t: t + jnp.where(odd, roll(t, 1, 0), roll(t, -1, 0)), v)
        else:
            v = [[line[2 * x] + line[2 * x + 1] for x in range(len(line) // 2)] for line in v]
        return lanes(v, halve)

    def grow(v, level):
        v = lanes(v, double)
        v = [line for line in v for _ in range(2)]
        return v if level == 2 else [[t for t in line for _ in range(2)] for line in v]

    def sweep(v, g, level, length):
        return combine(lambda a, b, s: KEEP * a + OMEGA * b + SIXTH * s, v, g, neighbours(v, level, length))

    def cycle(g, cs, level, length):
        last = level == LEVELS - 1
        if last:
            v = combine(lambda b: OMEGA * b, g)
            for _ in range(COARSE_SWEEPS - 1):
                v = sweep(v, g, level, length)
            return v
        v = combine(lambda b, s: PRE_G * b + PRE_N * s, g, neighbours(g, level, length))
        if level > 2:
            v = combine(lambda t: jnp.where(lane < length, t, zero), v)
        factor = 0.25**level
        r = combine(
            lambda c, b, a, s: (factor * c) * (6.0 * (b - a) + s), cs, g, v, neighbours(v, level, length)
        )
        down = shrink(r, level)
        c_down = shrink(cs, level)
        inner = lane < length // 2
        d = 6.0 * 0.25 ** (level + 1)
        g_down = combine(lambda b, c: jnp.where(inner, b / (d * jnp.where(inner, c, 1.0)), zero), down, c_down)
        e = grow(cycle(g_down, c_down, level + 1, length // 2), level)
        v = combine(lambda a, b: a + b, v, e)
        v = sweep(v, g, level, length)
        return combine(lambda t: jnp.where(lane < length, t, zero), v) if level > 2 else v

    v = cycle(g2, c2, 2, width * nz)
    for y in range(len(v)):
        for x in range(nx):
            W[y, x] = v[y][x]
    pre[...] = jnp.zeros_like(pre)
    ix, iy, iz = place.at
    for xw in range(4):
        x = ix + (xw + 1) // 2 - 1
        x_ok = jnp.logical_and(x >= 0, x < nx)
        x = jnp.clip(x, 0, nx - 1)
        for j in range(-1, parts_y + 1):
            y = iy * parts_y + j
            ok = jnp.logical_and(x_ok, jnp.logical_and(y >= 0, y < ny * parts_y))
            y = jnp.clip(y, 0, ny * parts_y - 1)
            for vec in range(4):
                pre[vec, xw, pl.ds(j % 8, 1)] = keep(ok, W[y, x, pl.ds(vec * 2 + (xw + 1) % 2, 1)])
    z1 = jnp.where(lo < 96, lo, lo - Z)
    window = onehot(li == iz * width + jnp.floor_divide(z1 + 2, 2) - 1)
    moved = dot(pre[...].reshape(4 * 4 * 8, Z), window)
    out[...] = moved.reshape(4, 4, 8, Z)


def last_kernel(counts, merge_y, e2, G1, S1, G, S, c, *refs):
    edges, (pre, op, E1, C1, E0, C0) = refs[:-6], refs[-6:]
    V, X1, Y1, Z = e2.shape[0], S1.shape[1] - 2 * H, S1.shape[2] // 2, S1.shape[3]
    X, Y = 2 * X1, 2 * Y1
    R1, R = 2 * Y1, Y + 8
    place = Place(counts)
    for v in range(V):
        for x in range(X1):
            k = (v * X1 + x) * R1
            tile = e2[v, x]
            E1[pl.ds(k, 8, stride=2)] = tile
            E1[pl.ds(k + 1, 8, stride=2)] = tile
    for v in range(V):
        for i in range(1, 2 * H + X1 - 1):
            C1[v, i] = S1[v, i] + E1[pl.ds((v * X1 + (i - 1) // 2) * R1, R1)]
    half = Z // 2
    lane = iota((1, Z), 1)
    for ref, (sx, sy) in zip(edges, edge_steps(merge_y)):
        dx = -sx
        for dy in (-1, 1) if sy == 0 else (-sy,):
            ok = place.has((dx, dy, 0))
            for cell, (a, b) in enumerate(EDGE):
                i = H + X1 + a if dx > 0 else H - 1 - a
                r = Y1 + b if dy > 0 else R1 - 1 - b
                for v in range(V):
                    line = ref[pl.ds(cell * (V // 2) + v // 2, 1)]
                    line = roll(line, half, 1) if v % 2 else line
                    line = line + E1[pl.ds((v * X1 + (i - 1) // 2) * R1 + r, 1)]
                    use = jnp.logical_and(lane < half, ok)
                    C1[v, i, pl.ds(r, 1)] = jnp.where(use, line, C1[v, i, pl.ds(r, 1)])
                    if cell:
                        line = ref[pl.ds((2 + cell) * (V // 2) + v // 2, 1)]
                        line = roll(line, half, 1) if v % 2 else line
                        ii, rr = i, r
                        if a:
                            rr = Y1 - 1 if dy > 0 else 0
                        else:
                            ii = H + X1 - 1 if dx > 0 else H
                        line = jnp.where(use, PRE_N * line, jnp.zeros_like(line))
                        C1[v, ii, pl.ds(rr, 1)] = C1[v, ii, pl.ds(rr, 1)] + line
    mask = coarse_masks(place, R1, Z)
    n = X1 + 2
    fine = []
    for v in range(V):
        tiles = []
        for i in range(H - 1, H + X1 + 1):
            m = scaled(x_flag(place, i, X1), mask)
            get = lambda j: C1[v, j]
            tiles.append(m * (KEEP * C1[v, i] + OMEGA * G1[v, i] + SIXTH * level1_sum(get, i)))
        fine.append(jnp.concatenate(tiles, axis=0))
    li, lo = iota((Z, Z), 0), iota((Z, Z), 1)
    double = onehot(li == lo // 2)
    k = lo % 8
    low_side = (lo // 8) % 2 == 0
    source = jnp.where(low_side, jnp.where(k < H, Z - 1, 0), jnp.where(k < 2, half - 1, half))
    rim = None
    for v in range(V):
        part = dot(fine[v], onehot((li == source) & (lo // 16 == v)))
        rim = part if rim is None else rim + part
    sub = iota((8, Z), 0)
    zero8 = jnp.zeros((8, Z), jnp.float32)
    for v in range(V + 1):
        wide = dot(fine[v], double) if v < V else rim
        for i in range(n):
            base = (v * n + i) * R
            tile = wide[i * R1 : i * R1 + Y1]
            edge = wide[i * R1 + Y1 : (i + 1) * R1]
            E0[pl.ds(base, 8, stride=2)] = tile
            E0[pl.ds(base + 1, 8, stride=2)] = tile
            E0[pl.ds(base + Y, 8)] = jnp.where(sub < 2, edge[0:1], jnp.where(sub >= 6, edge[7:8], zero8))
    for v in range(V + 1):
        for i in range(1, 2 * H + X - 1):
            C0[v, i] = S[v, i] + E0[pl.ds((v * n + (i - 1) // 2) * R, R)]
    ym, zm = fine_masks(place, Y, Z)
    lane = iota((R, Z), 1)
    for i in range(H - 1, H + X + 1):
        flag = x_flag(place, i, X)
        for v in range(V + 1):
            m = scaled(flag, ym if v < V else zm)
            value = m * (KEEP * C0[v, i] + OMEGA * G[v, i] + SIXTH * fine_sum(C0, v, i, V, lane))
            E0[pl.ds((v * (X + 2) + i - H + 1) * R, R)] = value
            if v < V and H <= i < H + X:
                pre[v, i - H] = value[0:Y]

    class View:
        def __getitem__(self, key):
            v, i = key
            return E0[pl.ds((v * (X + 2) + i - H + 1) * R, R)]

    view = View()
    for x in range(X):
        for v in range(V):
            around = fine_sum(view, v, H + x, V, lane)
            op[v, x] = c[x] * (6.0 * view[v, H + x][0:Y] - around[0:Y])


def gram_kernel(old, prev, out):
    M, X, Y, Z = old.shape
    J = prev.shape[0]
    pairs = [(a, b) for a in range(M + J) for b in range(a, M + J)]
    sums = [None] * len(pairs)
    for x in range(X):
        for y in range(0, Y, 8):
            tiles = [old[m, x, y : y + 8] for m in range(M)] + [prev[j, x, y : y + 8] for j in range(J)]
            for p, (a, b) in enumerate(pairs):
                term = tiles[a] * tiles[b]
                sums[p] = term if sums[p] is None else sums[p] + term
    ones = jnp.ones((8, Z), jnp.float32)
    lane = iota((8, Z), 1)
    rows = jnp.concatenate([jnp.sum(s, axis=0, keepdims=True) for s in sums], axis=0)
    pad = jnp.zeros((Z - len(pairs), Z), jnp.float32)
    out[...] = dot(ones, jnp.concatenate([rows, pad], axis=0), NT)


def ortho_kernel(count, cells, old, prev, slots, orth, proj, tri):
    M, X, Y, Z = old.shape
    J = prev.shape[0]
    if count <= 64:
        total = slots[0, pl.ds(6, 1)]
        for t in range(1, count):
            total = total + slots[t, pl.ds(6, 1)]
    else:
        total = lax.fori_loop(0, count, lambda t, s: s + slots[t, pl.ds(6, 1)], jnp.zeros((1, Z), jnp.float32))
    total = jnp.broadcast_to(total, (8, Z)) / cells
    value = {}
    p = 0
    for a in range(M + J):
        for b in range(a, M + J):
            one = jnp.broadcast_to(total[:, p : p + 1], (8, Z))
            value[a, b] = value[b, a] = one
            p += 1
    P_ = [[value[m, M + j] for j in range(J)] for m in range(M)]
    gram = {}
    for i in range(J):
        for j in range(i + 1):
            s = value[M + i, M + j]
            for m in range(M):
                inner = None
                for k in range(M):
                    term = value[m, k] * P_[k][j]
                    inner = term if inner is None else inner + term
                s = s - P_[m][i] * (P_[m][j] - inner) - P_[m][j] * P_[m][i]
            gram[i, j] = s
    L = {}
    for i in range(J):
        for j in range(i + 1):
            s = gram[i, j]
            for k in range(j):
                s = s - L[i, k] * L[j, k]
            L[i, j] = jnp.sqrt(s) if i == j else s / L[j, j]
    inv = {}
    for i in range(J):
        for j in range(i + 1):
            s = jnp.ones((8, Z), jnp.float32) if i == j else None
            for k in range(j, i):
                term = L[i, k] * inv[k, j]
                s = -term if s is None else s - term
            inv[i, j] = s / L[i, i]
    row, col = iota((M, J), 0), iota((M, J), 1)
    proj_v, tri_v = jnp.zeros((M, J), jnp.float32), jnp.zeros((J, J), jnp.float32)
    for m in range(M):
        for j in range(J):
            here = (row == m) & (col == j)
            proj_v = jnp.where(here, P_[m][j][0:M, 0:J], proj_v)
            if j >= m:
                tri_v = jnp.where(here, L[j, m][0:J, 0:J], tri_v)
    proj[...] = proj_v
    tri[...] = tri_v
    mix = {}
    for j in range(J):
        for m in range(M):
            s = None
            for i in range(j + 1):
                term = inv[j, i] * P_[m][i]
                s = term if s is None else s + term
            mix[j, m] = s
    for x in range(X):
        for y in range(0, Y, 8):
            olds = [old[m, x, y : y + 8] for m in range(M)]
            rem = []
            for i in range(J):
                r = prev[i, x, y : y + 8]
                for m in range(M):
                    r = r - P_[m][i] * olds[m]
                rem.append(r)
            for j in range(J):
                s = None
                for i in range(j + 1):
                    term = inv[j, i] * rem[i]
                    s = term if s is None else s + term
                orth[j, x, y : y + 8] = s


def run(kernel, shapes, args, scratch=(), name=None):
    fn = pl.pallas_call(
        kernel,
        out_shape=[jax.ShapeDtypeStruct(s, jnp.float32) for s in shapes],
        in_specs=[VM] * len(args),
        out_specs=[VM] * len(shapes),
        scratch_shapes=[pltpu.VMEM(s, jnp.float32) for s in scratch],
        name=name,
    )
    return fn(*args)


def shift(value, axis, step):
    n = lax.axis_size(axis)
    return lax.ppermute(value, axis, [(i, (i + step) % n) for i in range(n)])


def diagonal(counts, value, dx, dy):
    nx, ny = counts[:2]
    step = dy if dy else 1
    pairs = [(x * ny + y, (x + dx) % nx * ny + (y + step) % ny) for x in range(nx) for y in range(ny)]
    return lax.ppermute(value, ("gx", "gy"), pairs)


def swap(slots):
    return lax.all_to_all(slots, AXES, split_axis=0, concat_axis=0, tiled=True)


def wide_coarse(counts, parts_y, slots0, slots2):
    nx, ny, nz = counts
    Z = slots2.shape[2]
    width = Z // parts_y

    def whole(t, lead):
        t = t.reshape(nx, ny, nz, lead * 2, Z)
        parts = []
        for j in range(parts_y):
            part = t[..., j * width : (j + 1) * width].transpose(3, 0, 1, 2, 4)
            parts.append(part.reshape(lead * 2, nx, ny, nz * width))
        t = jnp.stack(parts, axis=3).reshape(lead, 2, nx, ny * parts_y, nz * width)
        return t.transpose(0, 2, 1, 3, 4).reshape(lead, nx * 2, ny * parts_y, nz * width)

    g2 = whole(slots2, 4)
    c2 = whole(jnp.stack([slots0[:, 3], slots0[:, 7]], axis=1), 1)

    def around(v):
        p = jnp.pad(v, ((0, 0), (1, 1), (1, 1), (1, 1)))
        m = slice(1, -1)
        return (
            p[:, 2:, m, m] + p[:, :-2, m, m] + p[:, m, 2:, m] + p[:, m, :-2, m] + p[:, m, m, 2:] + p[:, m, m, :-2]
        )

    def pairs(e):
        return onehot(iota((e, 2 * e), 0) == iota((e, 2 * e), 1) // 2)

    def shrink(v):
        d, a, b, e = v.shape
        v = v.reshape(d, a // 2, 2, b, e).sum(axis=2)
        v = v[:, :, 0::2] + v[:, :, 1::2]
        return dot(v.reshape(-1, e), pairs(e // 2).T * 0.125).reshape(d, a // 2, b // 2, e // 2)

    def grow(v):
        d, a, b, e = v.shape
        v = dot(v.reshape(-1, e), pairs(e)).reshape(d, a, b, 2 * e)
        return jnp.repeat(jnp.repeat(v, 2, axis=1), 2, axis=2)

    def cycle(g, c, level):
        if level == LEVELS - 1:
            v = OMEGA * g
            for _ in range(COARSE_SWEEPS - 1):
                v = KEEP * v + OMEGA * g + SIXTH * around(v)
            return v
        v = PRE_G * g + PRE_N * around(g)
        r = 0.25**level * c * (6.0 * (g - v) + around(v))
        down = shrink(c)
        v = v + grow(cycle(shrink(r) / (6.0 * 0.25 ** (level + 1) * down), down, level + 1))
        return KEEP * v + OMEGA * g + SIXTH * around(v)

    e = jnp.pad(cycle(g2, c2, 2), ((0, 0), (1, 1), (1, 1), (1, 1)))
    ix, iy, iz = (lax.axis_index(a) for a in AXES)
    e = lax.dynamic_slice(
        e, (jnp.int32(0), ix * 2, iy * parts_y, iz * width), (4, 4, parts_y + 2, width + 2)
    )
    e = jnp.repeat(e, 2, axis=3)
    e = jnp.concatenate(
        [e[..., 2:], jnp.zeros(e.shape[:3] + (Z - 2 * width - 4,), e.dtype), e[..., :2]], axis=3
    )
    pad = jnp.zeros((4, 4, 8 - parts_y - 2, Z), e.dtype)
    return jnp.concatenate([e[:, :, 1:], pad, e[:, :, :1]], axis=2)


def per_device(counts, old, prev, inc, c):
    V, X, Y, Z = inc.shape
    count = counts[0] * counts[1] * counts[2]
    merge_y = counts[1] == 2
    R = Y + 8
    X1, Y1 = X // 2, Y // 2
    y_shape = (V, X // 2, 8, Z)
    shapes = [(V, X, Y, Z), (V, H, Y, Z), (V, H, Y, Z), y_shape]
    shapes += [] if merge_y else [y_shape]
    shapes += [(count, 16, Z), (8, Z)]
    outs = run(functools.partial(first_kernel, counts, merge_y), shapes, (inc, c), name="first")
    g, xlo, xhi = outs[:3]
    slots0, c2p = outs[-2:]
    slots0 = swap(slots0)
    xl, xh = shift(xhi, "gx", 1), shift(xlo, "gx", -1)
    if merge_y:
        yl = yh = shift(outs[3], "gy", 1)
    else:
        yl, yh = shift(outs[4], "gy", 1), shift(outs[3], "gy", -1)
    (gram,) = run(gram_kernel, [(8, Z)], (old, prev), name="gram")
    ext0, ext1 = (V + 1, X + 2 * H, R, Z), (V, X1 + 2 * H, 2 * Y1, Z)
    G, S, p1, slots1, c1 = run(
        functools.partial(second_kernel, counts),
        [ext0, ext0, (V // 2, X1, Y1, Z), (count, 8, Z), (X1, Y1, Z)],
        (g, c, xl, xh, yl, yh, slots0, gram),
        [(V * X1 * Y, Z), (X1 * Y, Z)],
        name="second",
    )
    slots1 = swap(slots1)
    xl, xh = shift(p1, "gx", 1), shift(p1, "gx", -1)
    if merge_y:
        yl = yh = shift(p1, "gy", 1)
    else:
        yl, yh = shift(p1, "gy", 1), shift(p1, "gy", -1)
    steps = edge_steps(merge_y)
    G1, S1, slots2, *edges = run(
        functools.partial(third_kernel, counts, merge_y),
        [ext1, ext1, (count, 8, Z)] + [(16, Z)] * len(steps),
        (p1, c1, xl, xh, yl, yh, slots1, c2p),
        [(V * X1 // 2 * Y1, Z)],
        name="third",
    )
    slots2 = swap(slots2)
    edges = [diagonal(counts, e, dx, dy) for e, (dx, dy) in zip(edges, steps)]
    orth, proj, tri = run(
        functools.partial(ortho_kernel, count, float(count * X * Y * Z)),
        [(V, X, Y, Z), (4, 4), (4, 4)],
        (old, prev, slots1),
        name="ortho",
    )
    parts_y = Y // 4
    if counts[2] * (Z // parts_y) == Z and count <= 64:
        (e2,) = run(
            functools.partial(coarse_kernel, counts, parts_y),
            [(V, 4, 8, Z)],
            (slots0, slots2),
            [(counts[1] * parts_y, counts[0], 8, Z), (V, 4, 8, Z)],
            name="coarse",
        )
    else:
        e2 = wide_coarse(counts, parts_y, slots0, slots2)
    pre, op = run(
        functools.partial(last_kernel, counts, merge_y),
        [(V, X, Y, Z), (V, X, Y, Z)],
        (e2, G1, S1, G, S, c, *edges),
        [(V * X1 * 2 * Y1, Z), ext1, ((V + 1) * (X + 2) * R, Z), ext0],
        name="last",
    )
    return orth, proj, tri, pre, op


def solution(mesh):
    block = P(None, *AXES)
    counts = tuple(mesh.shape[a] for a in AXES)
    return jax.shard_map(
        functools.partial(per_device, counts),
        mesh=mesh,
        in_specs=(block, block, block, P(*AXES)),
        out_specs=(block, P(), P(), block, block),
        check_vma=False,
    )
```

```python
import functools

import jax
import jax.numpy as jnp
from jax import lax
from jax.experimental import pallas as pl
from jax.experimental.pallas import tpu as pltpu
from jax.sharding import PartitionSpec as P

LEVELS = 6
COARSE_SWEEPS = 4
OMEGA = 0.8
KEEP = 1.0 - OMEGA
SIXTH = OMEGA / 6.0
PRE_G = OMEGA * (2.0 - OMEGA)
PRE_N = OMEGA * OMEGA / 6.0
AXES = ("gx", "gy", "gz")
HIGH = lax.Precision.HIGHEST
H = 3
NN = (((1,), (0,)), ((), ()))
NT = (((1,), (1,)), ((), ()))
TN = (((0,), (0,)), ((), ()))
VM = pl.BlockSpec(memory_space=pltpu.VMEM)
HB = pl.BlockSpec(memory_space=pltpu.HBM)
EDGE = ((0, 0), (0, 1), (1, 0))
EDGE1 = EDGE + ((1, 1), (0, 2), (2, 0))
GRAM_ROW, C_ROW = 3, 4


def edge_steps(merge_y):
    return [(dx, dy) for dx in (1, -1) for dy in ((0,) if merge_y else (1, -1))]


def dot(a, b, dims=NN):
    return lax.dot_general(a, b, dims, precision=HIGH, preferred_element_type=jnp.float32)


def iota(shape, dim):
    return lax.broadcasted_iota(jnp.int32, shape, dim)


def onehot(cond, scale=1.0):
    return jnp.where(cond, jnp.float32(scale), jnp.float32(0.0))


def roll(a, shift, axis):
    size = a.shape[axis]
    shift = shift % size
    return a if shift == 0 else pltpu.roll(a, shift, axis)


class Place:
    def __init__(self, counts):
        self.counts = counts
        self.at = tuple(lax.axis_index(a) for a in AXES)
        self.me = self.linear(self.at)

    def linear(self, p):
        nx, ny, nz = self.counts
        return (p[0] * ny + p[1]) * nz + p[2]

    def lo(self, axis):
        return self.at[axis] > 0

    def hi(self, axis):
        return self.at[axis] < self.counts[axis] - 1

    def has(self, d):
        ok = None
        for axis in range(3):
            if d[axis]:
                one = self.hi(axis) if d[axis] > 0 else self.lo(axis)
                ok = one if ok is None else jnp.logical_and(ok, one)
        return ok

    def slot(self, d):
        there = self.linear(tuple(p + s for p, s in zip(self.at, d)))
        return jnp.where(self.has(d), there, self.me)


def f32(flag):
    return jnp.where(flag, jnp.float32(1.0), jnp.float32(0.0))


def keep(flag, a):
    return jnp.where(flag, a, jnp.zeros_like(a))


def fill_slots(ref, count, value, rows):
    if count <= 64:
        for t in range(count):
            ref[t, 0:rows] = value
    else:
        def body(t, carry):
            ref[t, 0:rows] = value
            return carry
        lax.fori_loop(0, count, body, 0)


def first_kernel(counts, merge_y, inc_hbm, c_hbm, *refs):
    if merge_y:
        g, xlo, xhi, ymsg, slots, inc, c, sems = refs
    else:
        g, xlo, xhi, ylo, yhi, slots, inc, c, sems = refs
    V, X, Y, Z = inc.shape
    place = Place(counts)
    copy_c = pltpu.make_async_copy(c_hbm, c, sems.at[V])
    copies = [pltpu.make_async_copy(inc_hbm.at[v], inc.at[v], sems.at[v]) for v in range(V)]
    copy_c.start()
    for copy in copies:
        copy.start()
    sub = iota((8, Z), 0)
    row, lane = iota((32, Z), 0), iota((32, Z), 1)
    layer = (row % 16) // 4
    wanted = jnp.where(row < 16, Z - H, 0) + layer
    copy_c.wait()
    scale = [1.0 / (6.0 * c[x]) for x in range(X)]
    faces = None
    for v in range(V):
        copies[v].wait()
        for x in range(X):
            value = inc[v, x] * scale[x]
            g[v, x] = value
            if x < H:
                xlo[v, x] = value
            if x >= X - H:
                xhi[v, x - (X - H)] = value
        pick = onehot((lane == wanted) & (layer < H) & (row % 4 == v))
        part = dot(pick, g[v].reshape(X * Y, Z), NT)
        faces = part if faces is None else faces + part
    up = [faces[4 * k : 4 * k + 4] for k in range(H)]
    down = [faces[16 + 4 * k : 20 + 4 * k] for k in range(H)]
    for dx in (-1, 0, 1):
        for dy in (-1, 0, 1):
            above, below = place.slot((dx, dy, 1)), place.slot((dx, dy, -1))
            for k in range(H):
                slots[above, k] = up[k]
                slots[below, k] = down[k]
            if dx and dy:
                t = place.slot((dx, dy, 0))
                for cell, (a, b) in enumerate(EDGE):
                    x = X - 1 - a if dx > 0 else a
                    y = Y - 1 - b if dy > 0 else b
                    for v in range(V):
                        slots[t, cell, pl.ds(v, 1)] = g[v, x, pl.ds(y, 1)]

    def packed(v, j, start, own):
        return jnp.where(own, g[v, 2 * j, pl.ds(start, 8)], roll(g[v, 2 * j + 1, pl.ds(start, 8)], 4, 0))

    for v in range(V):
        for j in range(X // 2):
            if merge_y:
                first = place.at[1] == 0
                start = pl.multiple_of(jnp.where(first, Y - 8, 0), 8)
                own = (sub + jnp.where(first, 0, 4)) % 8 >= 4
                ymsg[v, j] = packed(v, j, start, own)
            else:
                yhi[v, j] = packed(v, j, Y - 8, sub >= 4)
                ylo[v, j] = packed(v, j, 0, sub < 4)


def spread(cur, below, above, zl, zr):
    return below + above + roll(cur, 1, 0) + roll(cur, -1, 0) + zl + zr


def fine_sum(ref, v, i, V, lane):
    cur = ref[v, i]
    zl, zr = roll(cur, 1, 1), roll(cur, -1, 1)
    if v < V:
        rim = ref[V, i]
        last = lane.shape[1] - 1
        zl = jnp.where(lane == 0, roll(rim, -(16 * v + 2), 1), zl)
        zr = jnp.where(lane == last, roll(rim, last - (16 * v + 10), 1), zr)
    return spread(cur, ref[v, i - 1], ref[v, i + 1], zl, zr)


def fine_masks(place, Y, Z):
    R = Y + 8
    row = iota((R, Z), 0)
    ym = onehot(row < Y) + onehot((row >= Y) & (row < Y + H)) * f32(place.hi(1))
    ym = ym + onehot(row >= R - H) * f32(place.lo(1))
    lane = iota((R, Z), 1)
    k = lane % 8
    outside_lo = ((lane // 8) % 2 == 0) & (k < H)
    outside_hi = ((lane // 8) % 2 == 1) & (k >= 2)
    zm = jnp.where(outside_lo, f32(place.lo(2)), jnp.where(outside_hi, f32(place.hi(2)), jnp.float32(1.0)))
    return ym, ym * zm


def x_flag(place, i, X):
    if i < H:
        return f32(place.lo(0))
    if i >= H + X:
        return f32(place.hi(0))
    return None


def scaled(flag, mask):
    return mask if flag is None else mask * flag


def second_kernel(counts, merge_y, g, c, xl, xh, yl, yh, slots, gram, c2p, G, S, p1, slots1, c1, *refs):
    edges, (Q, QC) = refs[:-2], refs[-2:]
    V, X, Y, Z = g.shape
    R = Y + 8
    place = Place(counts)
    sub = iota((8, Z), 0)
    zero8 = jnp.zeros((8, Z), jnp.float32)
    zero_y = jnp.zeros((Y, Z), jnp.float32)
    has_yl, has_yh, has_xl, has_xh = place.lo(1), place.hi(1), place.lo(0), place.hi(0)
    m_hi = jnp.logical_and(sub < H, has_yh)
    m_lo = jnp.logical_and(sub >= 8 - H, has_yl)
    for v in range(V):
        for x in range(X):
            G[v, H + x, 0:Y] = g[v, x]
            hi, lo = yh[v, x // 2], yl[v, x // 2]
            if x % 2:
                hi, lo = roll(hi, 4, 0), roll(lo, 4, 0)
            G[v, H + x, Y:R] = jnp.where(m_hi, hi, jnp.where(m_lo, lo, zero8))
        for i in range(H):
            G[v, i, 0:Y] = keep(has_xl, xl[v, i])
            G[v, i, Y:R] = zero8
            G[v, H + X + i, 0:Y] = keep(has_xh, xh[v, i])
            G[v, H + X + i, Y:R] = zero8
    for dx in (-1, 1):
        for dy in (-1, 1):
            ok, t = place.has((dx, dy, 0)), place.slot((dx, dy, 0))
            for cell, (a, b) in enumerate(EDGE):
                i = H + X + a if dx > 0 else H - 1 - a
                r = Y + b if dy > 0 else R - 1 - b
                for v in range(V):
                    G[v, i, pl.ds(r, 1)] = keep(ok, slots[t, cell, pl.ds(v, 1)])
    row, lane24 = iota((8 * H, Z), 0), iota((8 * H, Z), 1)
    target = jnp.where(row < 4 * H, 0, 10 - H) + 16 * (row % 4) + row // 4
    place_lanes = onehot(lane24 == target)

    def layers(dx, dy, lanes):
        below, above = (dx, dy, -1), (dx, dy, 1)
        low, high = place.slot(below), place.slot(above)
        rows = [keep(place.has(below), slots[low, k]) for k in range(H)]
        rows += [keep(place.has(above), slots[high, k]) for k in range(H)]
        return dot(jnp.concatenate(rows, axis=0)[:, lanes], place_lanes, TN)

    everything = slice(0, X * Y)
    for i in (0, H + X + H - 1):
        G[V, i] = jnp.zeros((R, Z), jnp.float32)
    mid = layers(0, 0, everything)
    up = layers(0, 1, everything)
    down = layers(0, -1, everything)
    for x in range(X):
        G[V, H + x, 0:Y] = mid[x * Y : (x + 1) * Y]
        tile = jnp.where(sub < 2, up[x * Y : x * Y + 8], zero8)
        G[V, H + x, Y:R] = jnp.where(sub >= 6, down[(x + 1) * Y - 8 : (x + 1) * Y], tile)
    for dx in (-1, 1):
        first = slice(0, 2 * Y) if dx > 0 else slice((X - 2) * Y, X * Y)
        side = layers(dx, 0, first)
        base = H + X if dx > 0 else H - 2
        for a in range(2):
            G[V, base + a, 0:Y] = side[a * Y : (a + 1) * Y]
            G[V, base + a, Y:R] = zero8
        near = slice(0, Y) if dx > 0 else slice((X - 1) * Y, X * Y)
        up = layers(dx, 1, near)
        down = layers(dx, -1, near)
        tile = jnp.where(sub < 2, up[0:8], zero8)
        G[V, H + X if dx > 0 else H - 1, Y:R] = jnp.where(sub >= 6, down[Y - 8 : Y], tile)
    lane = iota((R, Z), 1)
    for i in range(1, 2 * H + X - 1):
        rim = G[V, i]
        for v in range(V):
            body = G[v, i]
            rim = jnp.where((lane == 16 * v + 3) | (lane == 16 * v + 4), roll(body, 16 * v + 3, 1), rim)
            rim = jnp.where((lane == 16 * v + 8) | (lane == 16 * v + 9), roll(body, 16 * v + 10, 1), rim)
        G[V, i] = rim
    ym, zm = fine_masks(place, Y, Z)
    for i in range(1, 2 * H + X - 1):
        flag = x_flag(place, i, X)
        for v in range(V + 1):
            mask = scaled(flag, ym if v < V else zm)
            S[v, i] = mask * (PRE_G * G[v, i] + PRE_N * fine_sum(G, v, i, V, lane))
    for x in range(X // 2):
        for v in range(V):
            total = None
            for i in (2 * x, 2 * x + 1):
                inner = 6.0 * (G[v, H + i] - S[v, H + i]) + fine_sum(S, v, H + i, V, lane)
                part = c[i] * inner[0:Y]
                total = part if total is None else total + part
            Q[pl.ds((v * (X // 2) + x) * Y, Y)] = total
        QC[pl.ds(x * Y, Y)] = c[2 * x] + c[2 * x + 1]
    li, lo = iota((Z, Z), 0), iota((Z, Z), 1)
    halve = onehot(lo == li // 2, 0.125)
    n, nc = V * X * Y // 4, X * Y // 4
    b1 = dot(Q[pl.ds(0, n, stride=2)] + Q[pl.ds(1, n, stride=2)], halve)
    cc = dot(QC[pl.ds(0, nc, stride=2)] + QC[pl.ds(1, nc, stride=2)], halve)
    c1[...] = cc.reshape(X // 2, Y // 2, Z)
    scale = 1.0 / (1.5 * jnp.where(iota((nc, Z), 1) < Z // 2, cc, jnp.float32(1.0)))
    U = jnp.concatenate([b1[v * nc : (v + 1) * nc] * scale for v in range(V)], axis=0)
    per = nc
    for vp in range(V // 2):
        both = U[2 * vp * per : (2 * vp + 1) * per] + roll(U[(2 * vp + 1) * per : (2 * vp + 2) * per], Z // 2, 1)
        p1[vp] = both.reshape(X // 2, Y // 2, Z)
    half = Z // 2
    row, lane16 = iota((16, Z), 0), iota((16, Z), 1)
    wanted = jnp.where(row < 8, half - H, 0) + row % 8
    faces = dot(onehot((lane16 == wanted) & (row % 8 < H)), U, NT)
    row = iota((8, Z), 0)
    base = jnp.where(row == GRAM_ROW, gram[0:1], zero8)
    base = jnp.where(row == C_ROW, c2p[0:1], jnp.where(row == C_ROW + 1, c2p[1:2], base))
    fill_slots(slots1, counts[0] * counts[1] * counts[2], base, 8)
    up, down = jnp.where(row < H, faces[0:8], base), jnp.where(row < H, faces[8:16], base)
    for dx in (-1, 0, 1):
        for dy in (-1, 0, 1):
            slots1[place.slot((dx, dy, 1))] = up
            slots1[place.slot((dx, dy, -1))] = down
    X1, Y1 = X // 2, Y // 2
    for ref, (dx, dy) in zip(edges, edge_steps(merge_y)):
        for cell, (a, b) in enumerate(EDGE1):
            x = X1 - 1 - a if dx > 0 else a
            if dy == 0:
                y = jnp.where(place.at[1] == 0, Y1 - 1 - b, b)
            else:
                y = Y1 - 1 - b if dy > 0 else b
            for vp in range(V // 2):
                ref[pl.ds(cell * (V // 2) + vp, 1)] = p1[vp, x, pl.ds(y, 1)]


def coarse_masks(place, R, Z):
    half = Z // 2
    row, lane = iota((R, Z), 0), iota((R, Z), 1)
    y = R // 2
    mask = onehot(row < y) + onehot((row >= y) & (row < y + H)) * f32(place.hi(1))
    mask = mask + onehot(row >= R - H) * f32(place.lo(1))
    lanes = onehot(lane < half) + onehot((lane >= half) & (lane < half + H)) * f32(place.hi(2))
    lanes = lanes + onehot(lane >= Z - H) * f32(place.lo(2))
    return mask * lanes


def level1_sum(get, i):
    cur = get(i)
    return spread(cur, get(i - 1), get(i + 1), roll(cur, 1, 1), roll(cur, -1, 1))


def third_kernel(counts, merge_y, p1, c1, xl, xh, yl, yh, slots, c2p, *refs):
    edges, (G1, S1, slots2, Q) = refs[:-4], refs[-4:]
    VP, X, Y, Z = p1.shape
    V, R, half = 2 * VP, 2 * Y, Z // 2
    place = Place(counts)
    row, lane = iota((Y, Z), 0), iota((Y, Z), 1)
    zero = jnp.zeros((Y, Z), jnp.float32)

    def unpack(tile, v):
        return jnp.where(lane < half, roll(tile, half, 1) if v % 2 else tile, zero)

    r16, l16 = iota((16, Z), 0), iota((16, Z), 1)
    target = jnp.where(r16 < 8, Z - H, half) + r16 % 8
    place_lanes = onehot((l16 == target) & (r16 % 8 < H))

    def layers(dx, dy):
        below, above = (dx, dy, -1), (dx, dy, 1)
        low = keep(place.has(below), slots[place.slot(below)])
        high = keep(place.has(above), slots[place.slot(above)])
        return dot(jnp.concatenate([low, high], axis=0), place_lanes, TN)

    mid, up, down = layers(0, 0), layers(0, 1), layers(0, -1)
    m_hi = jnp.logical_and(row < H, place.hi(1))
    m_lo = jnp.logical_and(row >= Y - H, place.lo(1))

    def tile_of(d, v, x):
        k = (v * X + x) * Y
        return d[k : k + Y]

    for v in range(V):
        for x in range(X):
            G1[v, H + x, 0:Y] = unpack(p1[v // 2, x], v) + tile_of(mid, v, x)
            hi = unpack(yh[v // 2, x], v) + tile_of(up, v, x)
            lo = unpack(yl[v // 2, x], v) + tile_of(down, v, x)
            G1[v, H + x, Y:R] = jnp.where(m_hi, hi, jnp.where(m_lo, lo, zero))
    for dx in (-1, 1):
        side, up, down = layers(dx, 0), layers(dx, 1), layers(dx, -1)
        src = xh if dx > 0 else xl
        ok = place.hi(0) if dx > 0 else place.lo(0)
        for v in range(V):
            for a in range(H):
                x = a if dx > 0 else X - 1 - a
                i = H + X + a if dx > 0 else H - 1 - a
                G1[v, i, 0:Y] = keep(ok, unpack(src[v // 2, x], v) + tile_of(side, v, x))
                tile = zero
                if a < 2:
                    tile = jnp.where(m_hi, tile_of(up, v, x), jnp.where(m_lo, tile_of(down, v, x), zero))
                G1[v, i, Y:R] = tile
    for ref, (sx, sy) in zip(edges, edge_steps(merge_y)):
        dx = -sx
        for dy in (-1, 1) if sy == 0 else (-sy,):
            ok = place.has((dx, dy, 0))
            for cell, (a, b) in enumerate(EDGE1):
                i = H + X + a if dx > 0 else H - 1 - a
                r = Y + b if dy > 0 else R - 1 - b
                for v in range(V):
                    line = ref[pl.ds(cell * VP + v // 2, 1)]
                    line = roll(line, half, 1) if v % 2 else line
                    use = jnp.logical_and(lane[0:1] < half, ok)
                    line = jnp.where(use, line, jnp.zeros((1, Z), jnp.float32))
                    G1[v, i, pl.ds(r, 1)] = G1[v, i, pl.ds(r, 1)] + line
    mask = coarse_masks(place, R, Z)
    for i in range(1, 2 * H + X - 1):
        m = scaled(x_flag(place, i, X), mask)
        for v in range(V):
            get = lambda j: G1[v, j]
            S1[v, i] = m * (PRE_G * G1[v, i] + PRE_N * level1_sum(get, i))
    for x in range(X // 2):
        for v in range(V):
            total = None
            for i in (2 * x, 2 * x + 1):
                get = lambda j: S1[v, j]
                inner = 6.0 * (G1[v, H + i] - S1[v, H + i]) + level1_sum(get, H + i)
                part = c1[i] * inner[0:Y]
                total = part if total is None else total + part
            Q[pl.ds((v * (X // 2) + x) * Y, Y)] = total
    li, lo = iota((Z, Z), 0), iota((Z, Z), 1)
    rows = V * X // 2
    msg = None
    for y in range(Y // 2):
        pair = Q[pl.ds(2 * y, rows, stride=Y)] + Q[pl.ds(2 * y + 1, rows, stride=Y)]
        part = dot(pair, onehot((lo == y * (half // 2) + li // 2) & (li < half), 0.25 * 0.125))
        msg = part if msg is None else msg + part
    msg = msg / (6.0 * 0.0625 * c2p[...])
    fill_slots(slots2, counts[0] * counts[1] * counts[2], msg, 8)


def grid_of(count_y, count_x, fn):
    return [[fn(y, x) for x in range(count_x)] for y in range(count_y)]


def assemble(counts, parts_y, tile, lane):
    nx, ny, nz = counts
    width = lane.shape[1] // parts_y

    def one(y, x):
        y, j = y // parts_y, y % parts_y
        acc = roll(tile[(x * ny + y) * nz], -width * j, 1)
        for z in range(1, nz):
            acc = jnp.where(lane // width == z, roll(tile[(x * ny + y) * nz + z], width * (z - j), 1), acc)
        return acc

    return grid_of(ny * parts_y, nx, one)


def combine(fn, *grids):
    return [[fn(*ts) for ts in zip(*lines)] for lines in zip(*grids)]


def add(*terms):
    total = None
    for term in terms:
        if term is not None:
            total = term if total is None else total + term
    return total


def shrink_tiles(v, level, odd, lane):
    step = 2 ** (level - 2)
    v = [[a + b for a, b in zip(v[2 * y], v[2 * y + 1])] for y in range(len(v) // 2)]
    if level == 2:
        v = combine(lambda t: t + jnp.where(odd, roll(t, 1, 0), roll(t, -1, 0)), v)
    else:
        v = [[line[2 * x] + line[2 * x + 1] for x in range(len(line) // 2)] for line in v]
    upper = (lane // step) % 2 == 1
    return combine(lambda t: 0.125 * (t + jnp.where(upper, roll(t, step, 1), roll(t, -step, 1))), v)


def weights_kernel(counts, parts_y, slots1, *outs):
    lane = iota((8, outs[0].shape[-1]), 1)
    odd = iota(lane.shape, 0) % 2 == 1
    count = counts[0] * counts[1] * counts[2]
    rows = [jnp.where(odd, slots1[t, pl.ds(C_ROW + 1, 1)], slots1[t, pl.ds(C_ROW, 1)]) for t in range(count)]
    c = assemble(counts, parts_y, rows, lane)
    level = 2
    refs = list(outs)
    while True:
        ref = refs.pop(0)
        for y in range(len(c)):
            for x in range(len(c[0])):
                ref[y, x] = (0.25**level) * c[y][x]
                if level > 2:
                    inverse[y, x] = 1.0 / ((6.0 * 0.25**level) * c[y][x])
        if level == LEVELS - 1:
            return
        c = shrink_tiles(c, level, odd, lane)
        level += 1
        inverse = refs.pop(0)


def coarse_kernel(counts, parts_y, slots2, *refs):
    *weights, out, W, pre = refs
    nx, ny, nz = counts
    Z = slots2.shape[2]
    place = Place(counts)
    width = Z // parts_y
    lane = iota((8, Z), 1)
    odd = iota((8, Z), 0) % 2 == 1
    zero = jnp.zeros((8, Z), jnp.float32)
    inverse = {3 + i: weights[1 + 2 * i] for i in range(LEVELS - 3)}
    scale = {2: weights[0], **{3 + i: weights[2 + 2 * i] for i in range(LEVELS - 3)}}

    def at(v, y, x):
        inside = 0 <= y < len(v) and 0 <= x < len(v[0])
        return v[y][x] if inside else None

    def neighbours(v, level):
        step = 2 ** (level - 2)
        ahead = [[roll(t, -1, 0) for t in line] for line in v] if level == 2 else None
        back = [[roll(t, 1, 0) for t in line] for line in v] if level == 2 else None

        def one(y, x):
            t = v[y][x]
            zs = jnp.where(lane < step, zero, roll(t, step, 1)) + jnp.where(lane >= Z - step, zero, roll(t, -step, 1))
            ys = add(zs, at(v, y - 1, x), at(v, y + 1, x))
            if level > 2:
                return add(ys, at(v, y, x - 1), at(v, y, x + 1))
            return ys + jnp.where(
                odd, add(back[y][x], at(back, y, x + 1)), add(ahead[y][x], at(ahead, y, x - 1))
            )

        return grid_of(len(v), len(v[0]), one)

    def grow(v, level):
        v = [line for line in v for _ in range(2)]
        return v if level == 2 else [[t for t in line for _ in range(2)] for line in v]

    def sweep(v, g, level):
        return combine(lambda a, b, s: KEEP * a + OMEGA * b + SIXTH * s, v, g, neighbours(v, level))

    def cycle(g, level):
        if level == LEVELS - 1:
            v = combine(lambda b: OMEGA * b, g)
            for _ in range(COARSE_SWEEPS - 1):
                v = sweep(v, g, level)
            return v
        v = combine(lambda b, s: PRE_G * b + PRE_N * s, g, neighbours(g, level))
        c = grid_of(len(g), len(g[0]), lambda y, x: scale[level][y, x])
        r = combine(lambda c, b, a, s: c * (6.0 * (b - a) + s), c, g, v, neighbours(v, level))
        down = shrink_tiles(r, level, odd, lane)
        down = grid_of(len(down), len(down[0]), lambda y, x: down[y][x] * inverse[level + 1][y, x])
        v = combine(lambda a, b: a + b, v, grow(cycle(down, level + 1), level))
        return sweep(v, g, level)

    count = nx * ny * nz
    v = cycle(assemble(counts, parts_y, [slots2[t] for t in range(count)], lane), 2)
    for y in range(len(v)):
        for x in range(nx):
            W[y, x] = v[y][x]
    pre[...] = jnp.zeros_like(pre)
    ix, iy, iz = place.at
    for xw in range(4):
        x = ix + (xw + 1) // 2 - 1
        x_ok = jnp.logical_and(x >= 0, x < nx)
        x = jnp.clip(x, 0, nx - 1)
        for j in range(-1, parts_y + 1):
            y = iy * parts_y + j
            ok = jnp.logical_and(x_ok, jnp.logical_and(y >= 0, y < ny * parts_y))
            y = jnp.clip(y, 0, ny * parts_y - 1)
            for vec in range(4):
                pre[vec, xw, pl.ds(j % 8, 1)] = keep(ok, W[y, x, pl.ds(vec * 2 + (xw + 1) % 2, 1)])
    li, lo = iota((Z, Z), 0), iota((Z, Z), 1)
    z1 = jnp.where(lo < 96, lo, lo - Z)
    window = onehot(li == iz * width + jnp.floor_divide(z1 + 2, 2) - 1)
    moved = dot(pre[...].reshape(4 * 4 * 8, Z), window)
    out[...] = moved.reshape(4, 4, 8, Z)


def last_kernel(counts, e2, G1, S1, G, S, c, pre_hbm, op_hbm, E1, C1, E0, C0, pre, op, sems):
    V, X1, Y1, Z = e2.shape[0], S1.shape[1] - 2 * H, S1.shape[2] // 2, S1.shape[3]
    X, Y = 2 * X1, 2 * Y1
    R1, R = 2 * Y1, Y + 8
    place = Place(counts)
    for v in range(V):
        for x in range(X1):
            k = (v * X1 + x) * R1
            tile = e2[v, x]
            E1[pl.ds(k, 8, stride=2)] = tile
            E1[pl.ds(k + 1, 8, stride=2)] = tile
    for v in range(V):
        for i in range(1, 2 * H + X1 - 1):
            C1[v, i] = S1[v, i] + E1[pl.ds((v * X1 + (i - 1) // 2) * R1, R1)]
    mask = coarse_masks(place, R1, Z)
    n = X1 + 2
    fine = []
    for v in range(V):
        tiles = []
        for i in range(H - 1, H + X1 + 1):
            m = scaled(x_flag(place, i, X1), mask)
            get = lambda j: C1[v, j]
            tiles.append(m * (KEEP * C1[v, i] + OMEGA * G1[v, i] + SIXTH * level1_sum(get, i)))
        fine.append(jnp.concatenate(tiles, axis=0))
    li, lo = iota((Z, Z), 0), iota((Z, Z), 1)
    double = onehot(li == lo // 2)
    half = Z // 2
    k = lo % 8
    low_side = (lo // 8) % 2 == 0
    source = jnp.where(low_side, jnp.where(k < H, Z - 1, 0), jnp.where(k < 2, half - 1, half))
    rim = None
    for v in range(V):
        part = dot(fine[v], onehot((li == source) & (lo // 16 == v)))
        rim = part if rim is None else rim + part
    sub = iota((8, Z), 0)
    zero8 = jnp.zeros((8, Z), jnp.float32)
    for v in range(V + 1):
        wide = dot(fine[v], double) if v < V else rim
        for i in range(n):
            base = (v * n + i) * R
            tile = wide[i * R1 : i * R1 + Y1]
            edge = wide[i * R1 + Y1 : (i + 1) * R1]
            E0[pl.ds(base, 8, stride=2)] = tile
            E0[pl.ds(base + 1, 8, stride=2)] = tile
            E0[pl.ds(base + Y, 8)] = jnp.where(sub < 2, edge[0:1], jnp.where(sub >= 6, edge[7:8], zero8))
    for v in range(V + 1):
        for i in range(1, 2 * H + X - 1):
            C0[v, i] = S[v, i] + E0[pl.ds((v * n + (i - 1) // 2) * R, R)]
    ym, zm = fine_masks(place, Y, Z)
    lane = iota((R, Z), 1)
    for i in range(H - 1, H + X + 1):
        flag = x_flag(place, i, X)
        for v in range(V + 1):
            m = scaled(flag, ym if v < V else zm)
            value = m * (KEEP * C0[v, i] + OMEGA * G[v, i] + SIXTH * fine_sum(C0, v, i, V, lane))
            E0[pl.ds((v * (X + 2) + i - H + 1) * R, R)] = value
            if v < V and H <= i < H + X:
                pre[v, i - H] = value[0:Y]
    copies = [pltpu.make_async_copy(pre, pre_hbm, sems.at[0])]
    copies[0].start()

    class View:
        def __getitem__(self, key):
            v, i = key
            return E0[pl.ds((v * (X + 2) + i - H + 1) * R, R)]

    view = View()
    for x in range(X):
        for v in range(V):
            around = fine_sum(view, v, H + x, V, lane)
            op[v, x] = c[x] * (6.0 * view[v, H + x][0:Y] - around[0:Y])
        if x % 2:
            part = slice(x - 1, x + 1)
            copies.append(pltpu.make_async_copy(op.at[:, part], op_hbm.at[:, part], sems.at[1 + x // 2]))
            copies[-1].start()
    for copy in copies:
        copy.wait()


def gram_kernel(old, prev, c, out, c2p):
    M, X, Y, Z = old.shape
    J = prev.shape[0]
    pairs = [(a, b) for a in range(M + J) for b in range(a, M + J)]
    sums = [None] * len(pairs)
    for x in range(X):
        for y in range(0, Y, 8):
            tiles = [old[m, x, y : y + 8] for m in range(M)] + [prev[j, x, y : y + 8] for j in range(J)]
            for p, (a, b) in enumerate(pairs):
                term = tiles[a] * tiles[b]
                sums[p] = term if sums[p] is None else sums[p] + term
    ones = jnp.ones((8, Z), jnp.float32)
    lane = iota((8, Z), 1)
    rows = jnp.concatenate([jnp.sum(s, axis=0, keepdims=True) for s in sums], axis=0)
    pad = jnp.zeros((Z - len(pairs), Z), jnp.float32)
    out[...] = dot(ones, jnp.concatenate([rows, pad], axis=0), NT)
    ny2, nz2 = Y // 4, Z // 4
    sub, li, lo = iota((8, Z), 0), iota((Z, Z), 0), iota((Z, Z), 1)
    total = None
    for y in range(ny2):
        sums = []
        for x in range(X // 4):
            quad = c[4 * x] + c[4 * x + 1] + c[4 * x + 2] + c[4 * x + 3]
            sums.append(jnp.sum(quad[4 * y : 4 * y + 4], axis=0, keepdims=True))
        rows = jnp.where(sub % 2 == 0, sums[0], sums[1])
        part = dot(rows, onehot(lo == y * nz2 + li // 4, 1.0 / 64.0))
        total = part if total is None else total + part
    c2p[...] = total


def ortho_kernel(count, cells, old, prev, slots, orth, proj, tri):
    M, X, Y, Z = old.shape
    J = prev.shape[0]
    if count <= 64:
        total = slots[0, pl.ds(GRAM_ROW, 1)]
        for t in range(1, count):
            total = total + slots[t, pl.ds(GRAM_ROW, 1)]
    else:
        total = lax.fori_loop(0, count, lambda t, s: s + slots[t, pl.ds(GRAM_ROW, 1)], jnp.zeros((1, Z), jnp.float32))
    total = jnp.broadcast_to(total, (8, Z)) / cells
    value = {}
    p = 0
    for a in range(M + J):
        for b in range(a, M + J):
            one = jnp.broadcast_to(total[:, p : p + 1], (8, Z))
            value[a, b] = value[b, a] = one
            p += 1
    P_ = [[value[m, M + j] for j in range(J)] for m in range(M)]
    gram = {}
    for i in range(J):
        for j in range(i + 1):
            s = value[M + i, M + j]
            for m in range(M):
                inner = None
                for k in range(M):
                    term = value[m, k] * P_[k][j]
                    inner = term if inner is None else inner + term
                s = s - P_[m][i] * (P_[m][j] - inner) - P_[m][j] * P_[m][i]
            gram[i, j] = s
    L = {}
    for i in range(J):
        for j in range(i + 1):
            s = gram[i, j]
            for k in range(j):
                s = s - L[i, k] * L[j, k]
            L[i, j] = jnp.sqrt(s) if i == j else s / L[j, j]
    inv = {}
    for i in range(J):
        for j in range(i + 1):
            s = jnp.ones((8, Z), jnp.float32) if i == j else None
            for k in range(j, i):
                term = L[i, k] * inv[k, j]
                s = -term if s is None else s - term
            inv[i, j] = s / L[i, i]
    row, col = iota((M, J), 0), iota((M, J), 1)
    proj_v, tri_v = jnp.zeros((M, J), jnp.float32), jnp.zeros((J, J), jnp.float32)
    for m in range(M):
        for j in range(J):
            here = (row == m) & (col == j)
            proj_v = jnp.where(here, P_[m][j][0:M, 0:J], proj_v)
            if j >= m:
                tri_v = jnp.where(here, L[j, m][0:J, 0:J], tri_v)
    proj[...] = proj_v
    tri[...] = tri_v
    mix = {}
    for j in range(J):
        for m in range(M):
            s = None
            for i in range(j + 1):
                term = inv[j, i] * P_[m][i]
                s = term if s is None else s + term
            mix[j, m] = s
    for x in range(X):
        for y in range(0, Y, 8):
            olds = [old[m, x, y : y + 8] for m in range(M)]
            rem = []
            for i in range(J):
                r = prev[i, x, y : y + 8]
                for m in range(M):
                    r = r - P_[m][i] * olds[m]
                rem.append(r)
            for j in range(J):
                s = None
                for i in range(j + 1):
                    term = inv[j, i] * rem[i]
                    s = term if s is None else s + term
                orth[j, x, y : y + 8] = s


def run(near, kernel, shapes, args, scratch=(), name=None, result=(), plain=(), sems=0, out_sems=0):
    outs = []
    for i, shape in enumerate(shapes):
        kind = jax.ShapeDtypeStruct if i in result or not near else pltpu.VMEM
        outs.append(kind(shape, jnp.float32))
    if near:
        spaces = [pltpu.HBM if sems else None if i in plain else pltpu.VMEM for i in range(len(args))]
        args = [pltpu.with_memory_space_constraint(a, m) if m else a for a, m in zip(args, spaces)]
    fn = pl.pallas_call(
        kernel,
        out_shape=outs,
        in_specs=[HB if sems else VM] * len(args),
        out_specs=[HB if out_sems and i in result else VM for i in range(len(shapes))],
        scratch_shapes=[pltpu.VMEM(s, jnp.float32) for s in scratch] + [pltpu.SemaphoreType.DMA((sems + out_sems,))] * (sems + out_sems > 0),
        compiler_params=pltpu.CompilerParams(vmem_limit_bytes=16 * 2**20) if near else None,
        name=name,
    )
    return fn(*args)


def shift(value, axis, step):
    n = lax.axis_size(axis)
    return lax.ppermute(value, axis, [(i, (i + step) % n) for i in range(n)])


def diagonal(counts, value, dx, dy):
    nx, ny = counts[:2]
    step = dy if dy else 1
    pairs = [(x * ny + y, (x + dx) % nx * ny + (y + step) % ny) for x in range(nx) for y in range(ny)]
    return lax.ppermute(value, ("gx", "gy"), pairs)


def swap(slots):
    return lax.all_to_all(slots, AXES, split_axis=0, concat_axis=0, tiled=True)


def wide_coarse(counts, parts_y, slots1, slots2):
    nx, ny, nz = counts
    Z = slots2.shape[2]
    width = Z // parts_y

    def whole(t, lead):
        t = t.reshape(nx, ny, nz, lead * 2, Z)
        parts = []
        for j in range(parts_y):
            part = t[..., j * width : (j + 1) * width].transpose(3, 0, 1, 2, 4)
            parts.append(part.reshape(lead * 2, nx, ny, nz * width))
        t = jnp.stack(parts, axis=3).reshape(lead, 2, nx, ny * parts_y, nz * width)
        return t.transpose(0, 2, 1, 3, 4).reshape(lead, nx * 2, ny * parts_y, nz * width)

    g2 = whole(slots2, 4)
    c2 = whole(slots1[:, C_ROW : C_ROW + 2], 1)

    def around(v):
        p = jnp.pad(v, ((0, 0), (1, 1), (1, 1), (1, 1)))
        m = slice(1, -1)
        return (
            p[:, 2:, m, m] + p[:, :-2, m, m] + p[:, m, 2:, m] + p[:, m, :-2, m] + p[:, m, m, 2:] + p[:, m, m, :-2]
        )

    def pairs(e):
        return onehot(iota((e, 2 * e), 0) == iota((e, 2 * e), 1) // 2)

    def shrink(v):
        d, a, b, e = v.shape
        v = v.reshape(d, a // 2, 2, b, e).sum(axis=2)
        v = v[:, :, 0::2] + v[:, :, 1::2]
        return dot(v.reshape(-1, e), pairs(e // 2).T * 0.125).reshape(d, a // 2, b // 2, e // 2)

    def grow(v):
        d, a, b, e = v.shape
        v = dot(v.reshape(-1, e), pairs(e)).reshape(d, a, b, 2 * e)
        return jnp.repeat(jnp.repeat(v, 2, axis=1), 2, axis=2)

    def cycle(g, c, level):
        if level == LEVELS - 1:
            v = OMEGA * g
            for _ in range(COARSE_SWEEPS - 1):
                v = KEEP * v + OMEGA * g + SIXTH * around(v)
            return v
        v = PRE_G * g + PRE_N * around(g)
        r = 0.25**level * c * (6.0 * (g - v) + around(v))
        down = shrink(c)
        v = v + grow(cycle(shrink(r) / (6.0 * 0.25 ** (level + 1) * down), down, level + 1))
        return KEEP * v + OMEGA * g + SIXTH * around(v)

    e = jnp.pad(cycle(g2, c2, 2), ((0, 0), (1, 1), (1, 1), (1, 1)))
    ix, iy, iz = (lax.axis_index(a) for a in AXES)
    e = lax.dynamic_slice(
        e, (jnp.int32(0), ix * 2, iy * parts_y, iz * width), (4, 4, parts_y + 2, width + 2)
    )
    e = jnp.repeat(e, 2, axis=3)
    e = jnp.concatenate(
        [e[..., 2:], jnp.zeros(e.shape[:3] + (Z - 2 * width - 4,), e.dtype), e[..., :2]], axis=3
    )
    pad = jnp.zeros((4, 4, 8 - parts_y - 2, Z), e.dtype)
    return jnp.concatenate([e[:, :, 1:], pad, e[:, :, :1]], axis=2)


def per_device(counts, old, prev, inc, c):
    V, X, Y, Z = inc.shape
    count = counts[0] * counts[1] * counts[2]
    merge_y = counts[1] == 2
    near = count <= 64
    R = Y + 8
    X1, Y1 = X // 2, Y // 2
    y_shape = (V, X // 2, 8, Z)
    shapes = [(V, X, Y, Z), (V, H, Y, Z), (V, H, Y, Z), y_shape]
    shapes += [] if merge_y else [y_shape]
    shapes += [(count, H, V, Z)]
    outs = run(near, functools.partial(first_kernel, counts, merge_y), shapes, (inc, c), [inc.shape, c.shape], name="first", plain=(0, 1), result=(len(shapes) - 1,), sems=V + 1)
    g, xlo, xhi = outs[:3]
    slots0 = swap(outs[-1])
    xl, xh = shift(xhi, "gx", 1), shift(xlo, "gx", -1)
    if merge_y:
        yl = yh = shift(outs[3], "gy", 1)
    else:
        yl, yh = shift(outs[4], "gy", 1), shift(outs[3], "gy", -1)
    gram, c2p = run(near, gram_kernel, [(8, Z), (8, Z)], (old, prev, c), name="gram", plain=(0, 1))
    ext0, ext1 = (V + 1, X + 2 * H, R, Z), (V, X1 + 2 * H, 2 * Y1, Z)
    steps = edge_steps(merge_y)
    G, S, p1, slots1, c1, *edges = run(
        near,
        functools.partial(second_kernel, counts, merge_y),
        [ext0, ext0, (V // 2, X1, Y1, Z), (count, 8, Z), (X1, Y1, Z)] + [(16, Z)] * len(steps),
        (g, c, xl, xh, yl, yh, slots0, gram, c2p),
        [(V * X1 * Y, Z), (X1 * Y, Z)],
        name="second",
        result=(3,),
    )
    slots1 = swap(slots1)
    edges = [diagonal(counts, e, dx, dy) for e, (dx, dy) in zip(edges, steps)]
    xl, xh = shift(p1, "gx", 1), shift(p1, "gx", -1)
    if merge_y:
        yl = yh = shift(p1, "gy", 1)
    else:
        yl, yh = shift(p1, "gy", 1), shift(p1, "gy", -1)
    G1, S1, slots2 = run(
        near,
        functools.partial(third_kernel, counts, merge_y),
        [ext1, ext1, (count, 8, Z)],
        (p1, c1, xl, xh, yl, yh, slots1, c2p, *edges),
        [(V * X1 // 2 * Y1, Z)],
        name="third",
        result=(2,),
    )
    slots2 = swap(slots2)
    orth, proj, tri = run(
        near,
        functools.partial(ortho_kernel, count, float(count * X * Y * Z)),
        [(V, X, Y, Z), (4, 4), (4, 4)],
        (old, prev, slots1),
        name="ortho",
        result=(0, 1, 2),
        plain=(0, 1),
    )
    parts_y = Y // 4
    if near and counts[2] * (Z // parts_y) == Z:
        sizes = [(counts[1] * parts_y, counts[0], 8, Z)]
        for level in range(3, LEVELS):
            y, x = sizes[-1][:2]
            sizes += [(y // 2, x if level == 3 else x // 2, 8, Z)] * 2
        weights = run(
            near, functools.partial(weights_kernel, counts, parts_y), sizes, (slots1,), name="weights"
        )
        (e2,) = run(
            near,
            functools.partial(coarse_kernel, counts, parts_y),
            [(V, 4, 8, Z)],
            (slots2, *weights),
            [sizes[0], (V, 4, 8, Z)],
            name="coarse",
        )
    else:
        e2 = wide_coarse(counts, parts_y, slots1, slots2)
    pre, op = run(
        near,
        functools.partial(last_kernel, counts),
        [(V, X, Y, Z), (V, X, Y, Z)],
        (e2, G1, S1, G, S, c),
        [(V * X1 * 2 * Y1, Z), ext1, ((V + 1) * (X + 2) * R, Z), ext0, (V, X, Y, Z), (V, X, Y, Z)],
        name="last",
        result=(0, 1),
        out_sems=1 + X // 2,
    )
    return orth, proj, tri, pre, op


def solution(mesh):
    block = P(None, *AXES)
    counts = tuple(mesh.shape[a] for a in AXES)
    return jax.shard_map(
        functools.partial(per_device, counts),
        mesh=mesh,
        in_specs=(block, block, block, P(*AXES)),
        out_specs=(block, P(), P(), block, block),
        check_vma=False,
    )
```

```python
import functools

import jax
import jax.numpy as jnp
from jax import lax
from jax.experimental import pallas as pl
from jax.experimental.pallas import tpu as pltpu
from jax.sharding import PartitionSpec as P

LEVELS = 6
COARSE_SWEEPS = 4
OMEGA = 0.8
KEEP = 1.0 - OMEGA
SIXTH = OMEGA / 6.0
PRE_G = OMEGA * (2.0 - OMEGA)
PRE_N = OMEGA * OMEGA / 6.0
AXES = ("gx", "gy", "gz")
HIGH = lax.Precision.HIGHEST
H = 3
NN = (((1,), (0,)), ((), ()))
NT = (((1,), (1,)), ((), ()))
TN = (((0,), (0,)), ((), ()))
VM = pl.BlockSpec(memory_space=pltpu.VMEM)
HB = pl.BlockSpec(memory_space=pltpu.HBM)
EDGE = ((0, 0), (0, 1), (1, 0))
EDGE1 = EDGE + ((1, 1), (0, 2), (2, 0))
TAIL = 4


def edge_steps(merge_y):
    return [(dx, dy) for dx in (1, -1) for dy in ((0,) if merge_y else (1, -1))]


def dot(a, b, dims=NN):
    return lax.dot_general(a, b, dims, precision=HIGH, preferred_element_type=jnp.float32)


def iota(shape, dim):
    return lax.broadcasted_iota(jnp.int32, shape, dim)


def onehot(cond, scale=1.0):
    return jnp.where(cond, jnp.float32(scale), jnp.float32(0.0))


def roll(a, shift, axis):
    size = a.shape[axis]
    shift = shift % size
    return a if shift == 0 else pltpu.roll(a, shift, axis)


class Place:
    def __init__(self, counts):
        self.counts = counts
        self.at = tuple(lax.axis_index(a) for a in AXES)
        self.me = self.linear(self.at)

    def linear(self, p):
        nx, ny, nz = self.counts
        return (p[0] * ny + p[1]) * nz + p[2]

    def lo(self, axis):
        return self.at[axis] > 0

    def hi(self, axis):
        return self.at[axis] < self.counts[axis] - 1

    def has(self, d):
        ok = None
        for axis in range(3):
            if d[axis]:
                one = self.hi(axis) if d[axis] > 0 else self.lo(axis)
                ok = one if ok is None else jnp.logical_and(ok, one)
        return ok

    def slot(self, d):
        there = self.linear(tuple(p + s for p, s in zip(self.at, d)))
        return jnp.where(self.has(d), there, self.me)


def f32(flag):
    return jnp.where(flag, jnp.float32(1.0), jnp.float32(0.0))


def keep(flag, a):
    return jnp.where(flag, a, jnp.zeros_like(a))


def fill_slots(ref, count, value, rows):
    if count <= 64:
        for t in range(count):
            ref[t, 0:rows] = value
    else:
        def body(t, carry):
            ref[t, 0:rows] = value
            return carry
        lax.fori_loop(0, count, body, 0)


def fill_tail(ref, count, k, value):
    if count <= 64:
        for t in range(count):
            ref[t, k] = value
    else:
        def body(t, carry):
            ref[t, k] = value
            return carry
        lax.fori_loop(0, count, body, 0)


def first_kernel(counts, merge_y, inc_hbm, c_hbm, *refs):
    if merge_y:
        g, xlo, xhi, ymsg, slots, c1, inc, c, QC, sems = refs
    else:
        g, xlo, xhi, ylo, yhi, slots, c1, inc, c, QC, sems = refs
    V, X, Y, Z = inc.shape
    place = Place(counts)
    copy_c = pltpu.make_async_copy(c_hbm, c, sems.at[V])
    copies = [pltpu.make_async_copy(inc_hbm.at[v], inc.at[v], sems.at[v]) for v in range(V)]
    copy_c.start()
    for copy in copies:
        copy.start()
    sub = iota((8, Z), 0)
    row, lane = iota((32, Z), 0), iota((32, Z), 1)
    layer = (row % 16) // 4
    wanted = jnp.where(row < 16, Z - H, 0) + layer
    copy_c.wait()
    X1, Y1, half = X // 2, Y // 2, Z // 2
    for x in range(X1):
        QC[pl.ds(x * Y, Y)] = c[2 * x] + c[2 * x + 1]
    li, lo = iota((Z, Z), 0), iota((Z, Z), 1)
    n = X1 * Y1
    cc = dot(QC[pl.ds(0, n, stride=2)] + QC[pl.ds(1, n, stride=2)], onehot(lo == li // 2, 0.125))
    c1[...] = cc.reshape(X1, Y1, Z)
    c2 = None
    for y in range(Y // 4):
        sums = []
        for x in range(X // 4):
            k = 2 * x * Y1 + 2 * y
            pair = cc[k : k + 2] + cc[k + Y1 : k + Y1 + 2]
            sums.append(pair[0:1] + pair[1:2])
        rows = jnp.where(sub % 2 == 0, sums[0], sums[1])
        part = dot(rows, onehot((lo == y * (half // 2) + li // 2) & (li < half), 0.125))
        c2 = part if c2 is None else c2 + part
    r8, l8, r4, l4 = iota((8, Z), 0), iota((8, Z), 1), iota((4, Z), 0), iota((4, Z), 1)
    rim = dot(onehot((l8 == jnp.where(r8 < 2, half - 1 - r8, r8 - 2)) & (r8 < 4)), jnp.concatenate([cc] * (Z // n), 0), NT)
    base = jnp.where(r4 < 2, c2[0:4], jnp.zeros((4, Z), jnp.float32))
    fill_tail(slots, counts[0] * counts[1] * counts[2], H, base)

    def tail(line):
        return jnp.where(r4 == 2, line, base)

    def rim_row(k):
        first, second = rim[k : k + 1], rim[k + 1 : k + 2]
        return jnp.where(l4 < n, first, jnp.where(l4 < 2 * n, second, jnp.zeros((4, Z), jnp.float32)))

    up_tail, down_tail = tail(rim_row(0)), tail(rim_row(2))
    wide8 = l8 < half
    xlo[V * H, 0:Y1] = jnp.where(wide8, c1[0], roll(c1[1], half, 1))
    xhi[V * H, 0:Y1] = jnp.where(wide8, c1[X1 - 1], roll(c1[X1 - 2], half, 1))
    ends = [(ymsg, jnp.where(place.at[1] == 0, 1, 0))] if merge_y else [(ylo, 0), (yhi, 1)]
    for ref, upper in ends:
        for x in range(X1):
            for b in range(2):
                y = jnp.where(upper == 1, Y1 - 1 - b, b)
                ref[V * (X // 2), pl.ds(2 * x + b, 1)] = c1[x, pl.ds(y, 1)]
    scale = [1.0 / (6.0 * c[x]) for x in range(X)]
    faces = None
    for v in range(V):
        copies[v].wait()
        for x in range(X):
            value = inc[v, x] * scale[x]
            g[v, x] = value
            if x < H:
                xlo[v * H + x] = value
            if x >= X - H:
                xhi[v * H + x - (X - H)] = value
        pick = onehot((lane == wanted) & (layer < H) & (row % 4 == v))
        part = dot(pick, g[v].reshape(X * Y, Z), NT)
        faces = part if faces is None else faces + part
    up = [faces[4 * k : 4 * k + 4] for k in range(H)]
    down = [faces[16 + 4 * k : 20 + 4 * k] for k in range(H)]
    for dx in (-1, 0, 1):
        for dy in (-1, 0, 1):
            above, below = place.slot((dx, dy, 1)), place.slot((dx, dy, -1))
            for k in range(H):
                slots[above, k] = up[k]
                slots[below, k] = down[k]
            slots[above, H] = up_tail
            slots[below, H] = down_tail
            if dx and dy:
                t = place.slot((dx, dy, 0))
                for cell, (a, b) in enumerate(EDGE):
                    x = X - 1 - a if dx > 0 else a
                    y = Y - 1 - b if dy > 0 else b
                    for v in range(V):
                        slots[t, cell, pl.ds(v, 1)] = g[v, x, pl.ds(y, 1)]
                slots[t, H] = tail(c1[X1 - 1 if dx > 0 else 0, Y1 - 1 if dy > 0 else 0][None])

    def packed(v, j, start, own):
        return jnp.where(own, g[v, 2 * j, pl.ds(start, 8)], roll(g[v, 2 * j + 1, pl.ds(start, 8)], 4, 0))

    for v in range(V):
        for j in range(X // 2):
            if merge_y:
                first = place.at[1] == 0
                start = pl.multiple_of(jnp.where(first, Y - 8, 0), 8)
                own = (sub + jnp.where(first, 0, 4)) % 8 >= 4
                ymsg[v * (X // 2) + j] = packed(v, j, start, own)
            else:
                yhi[v * (X // 2) + j] = packed(v, j, Y - 8, sub >= 4)
                ylo[v * (X // 2) + j] = packed(v, j, 0, sub < 4)


def spread(cur, below, above, zl, zr):
    return below + above + roll(cur, 1, 0) + roll(cur, -1, 0) + zl + zr


def fine_sum(ref, v, i, V, lane):
    cur = ref[v, i]
    zl, zr = roll(cur, 1, 1), roll(cur, -1, 1)
    if v < V:
        rim = ref[V, i]
        last = lane.shape[1] - 1
        zl = jnp.where(lane == 0, roll(rim, -(16 * v + 2), 1), zl)
        zr = jnp.where(lane == last, roll(rim, last - (16 * v + 10), 1), zr)
    return spread(cur, ref[v, i - 1], ref[v, i + 1], zl, zr)


def fine_masks(place, Y, Z):
    R = Y + 8
    row = iota((R, Z), 0)
    ym = onehot(row < Y) + onehot((row >= Y) & (row < Y + H)) * f32(place.hi(1))
    ym = ym + onehot(row >= R - H) * f32(place.lo(1))
    lane = iota((R, Z), 1)
    k = lane % 8
    outside_lo = ((lane // 8) % 2 == 0) & (k < H)
    outside_hi = ((lane // 8) % 2 == 1) & (k >= 2)
    zm = jnp.where(outside_lo, f32(place.lo(2)), jnp.where(outside_hi, f32(place.hi(2)), jnp.float32(1.0)))
    return ym, ym * zm


def x_flag(place, i, X):
    if i < H:
        return f32(place.lo(0))
    if i >= H + X:
        return f32(place.hi(0))
    return None


def scaled(flag, mask):
    return mask if flag is None else mask * flag


def second_kernel(counts, merge_y, g, c, c1, xl, xh, yl, yh, slots, gram, G, S, p1, slots1, c2s, *refs):
    edges, (Q, CE, GL, VL) = refs[:-4], refs[-4:]
    V, X, Y, Z = g.shape
    R = Y + 8
    place = Place(counts)
    sub = iota((8, Z), 0)
    zero8 = jnp.zeros((8, Z), jnp.float32)
    zero_y = jnp.zeros((Y, Z), jnp.float32)
    has_yl, has_yh, has_xl, has_xh = place.lo(1), place.hi(1), place.lo(0), place.hi(0)
    m_hi = jnp.logical_and(sub < H, has_yh)
    m_lo = jnp.logical_and(sub >= 8 - H, has_yl)
    for v in range(V):
        for x in range(X):
            G[v, H + x, 0:Y] = g[v, x]
            hi, lo = yh[v * (X // 2) + x // 2], yl[v * (X // 2) + x // 2]
            if x % 2:
                hi, lo = roll(hi, 4, 0), roll(lo, 4, 0)
            G[v, H + x, Y:R] = jnp.where(m_hi, hi, jnp.where(m_lo, lo, zero8))
        for i in range(H):
            G[v, i, 0:Y] = keep(has_xl, xl[v * H + i])
            G[v, i, Y:R] = zero8
            G[v, H + X + i, 0:Y] = keep(has_xh, xh[v * H + i])
            G[v, H + X + i, Y:R] = zero8
    for dx in (-1, 1):
        for dy in (-1, 1):
            ok, t = place.has((dx, dy, 0)), place.slot((dx, dy, 0))
            for cell, (a, b) in enumerate(EDGE):
                i = H + X + a if dx > 0 else H - 1 - a
                r = Y + b if dy > 0 else R - 1 - b
                for v in range(V):
                    G[v, i, pl.ds(r, 1)] = keep(ok, slots[t, cell, pl.ds(v, 1)])
    row, lane24 = iota((8 * H, Z), 0), iota((8 * H, Z), 1)
    target = jnp.where(row < 4 * H, 0, 10 - H) + 16 * (row % 4) + row // 4
    place_lanes = onehot(lane24 == target)

    def layers(dx, dy, lanes):
        below, above = (dx, dy, -1), (dx, dy, 1)
        low, high = place.slot(below), place.slot(above)
        rows = [keep(place.has(below), slots[low, k]) for k in range(H)]
        rows += [keep(place.has(above), slots[high, k]) for k in range(H)]
        return dot(jnp.concatenate(rows, axis=0)[:, lanes], place_lanes, TN)

    everything = slice(0, X * Y)
    for i in (0, H + X + H - 1):
        G[V, i] = jnp.zeros((R, Z), jnp.float32)
    mid = layers(0, 0, everything)
    up = layers(0, 1, everything)
    down = layers(0, -1, everything)
    for x in range(X):
        G[V, H + x, 0:Y] = mid[x * Y : (x + 1) * Y]
        tile = jnp.where(sub < 2, up[x * Y : x * Y + 8], zero8)
        G[V, H + x, Y:R] = jnp.where(sub >= 6, down[(x + 1) * Y - 8 : (x + 1) * Y], tile)
    for dx in (-1, 1):
        first = slice(0, 2 * Y) if dx > 0 else slice((X - 2) * Y, X * Y)
        side = layers(dx, 0, first)
        base = H + X if dx > 0 else H - 2
        for a in range(2):
            G[V, base + a, 0:Y] = side[a * Y : (a + 1) * Y]
            G[V, base + a, Y:R] = zero8
        near = slice(0, Y) if dx > 0 else slice((X - 1) * Y, X * Y)
        up = layers(dx, 1, near)
        down = layers(dx, -1, near)
        tile = jnp.where(sub < 2, up[0:8], zero8)
        G[V, H + X if dx > 0 else H - 1, Y:R] = jnp.where(sub >= 6, down[Y - 8 : Y], tile)
    lane = iota((R, Z), 1)
    for i in range(1, 2 * H + X - 1):
        rim = G[V, i]
        for v in range(V):
            body = G[v, i]
            rim = jnp.where((lane == 16 * v + 3) | (lane == 16 * v + 4), roll(body, 16 * v + 3, 1), rim)
            rim = jnp.where((lane == 16 * v + 8) | (lane == 16 * v + 9), roll(body, 16 * v + 10, 1), rim)
        G[V, i] = rim
    ym, zm = fine_masks(place, Y, Z)
    for i in range(1, 2 * H + X - 1):
        flag = x_flag(place, i, X)
        for v in range(V + 1):
            mask = scaled(flag, ym if v < V else zm)
            S[v, i] = mask * (PRE_G * G[v, i] + PRE_N * fine_sum(G, v, i, V, lane))
    for x in range(X // 2):
        for v in range(V):
            total = None
            for i in (2 * x, 2 * x + 1):
                inner = 6.0 * (G[v, H + i] - S[v, H + i]) + fine_sum(S, v, H + i, V, lane)
                part = c[i] * inner[0:Y]
                total = part if total is None else total + part
            Q[pl.ds((v * (X // 2) + x) * Y, Y)] = total
    li, lo = iota((Z, Z), 0), iota((Z, Z), 1)
    halve = onehot(lo == li // 2, 0.125)
    n, nc = V * X * Y // 4, X * Y // 4
    b1 = dot(Q[pl.ds(0, n, stride=2)] + Q[pl.ds(1, n, stride=2)], halve)
    cc = c1[...].reshape(nc, Z)
    scale = 1.0 / (1.5 * jnp.where(iota((nc, Z), 1) < Z // 2, cc, jnp.float32(1.0)))
    U = jnp.concatenate([b1[v * nc : (v + 1) * nc] * scale for v in range(V)], axis=0)
    per = nc
    for vp in range(V // 2):
        both = U[2 * vp * per : (2 * vp + 1) * per] + roll(U[(2 * vp + 1) * per : (2 * vp + 2) * per], Z // 2, 1)
        p1[vp] = both.reshape(X // 2, Y // 2, Z)
    half = Z // 2
    row, lane16 = iota((16, Z), 0), iota((16, Z), 1)
    wanted = jnp.where(row < 8, half - H, 0) + row % 8
    faces = dot(onehot((lane16 == wanted) & (row % 8 < H)), U, NT)
    X1, Y1 = X // 2, Y // 2
    if counts[0] * counts[1] * counts[2] <= 64:
        for t in range(counts[0] * counts[1] * counts[2]):
            c2s[t] = slots[t, H]
    else:
        c2s[...] = slots[:, H]
    around_c1(place, CE, c1, xl, xh, yl, yh, slots, V, X)
    gram_row = gram[0:1]
    tiles = contributions(place, U, gram_row, CE, GL, VL, Q, V)
    up, down = faces[0:4], faces[8:12]
    rest = counts[1] * counts[2]
    for x in range(counts[0]):
        for k, tile in enumerate(tiles[x % 2]):
            fill_tail(slots1.at[pl.ds(x * rest, rest)], rest, k, tile)
    for dx in (-1, 0, 1):
        for dy in (-1, 0, 1):
            slots1[place.slot((dx, dy, 1)), TAIL] = up
            slots1[place.slot((dx, dy, -1)), TAIL] = down
    for ref, (dx, dy) in zip(edges, edge_steps(merge_y)):
        for cell, (a, b) in enumerate(EDGE1):
            x = X1 - 1 - a if dx > 0 else a
            if dy == 0:
                y = jnp.where(place.at[1] == 0, Y1 - 1 - b, b)
            else:
                y = Y1 - 1 - b if dy > 0 else b
            for vp in range(V // 2):
                ref[pl.ds(cell * (V // 2) + vp, 1)] = p1[vp, x, pl.ds(y, 1)]


def around_c1(place, CE, c1, xl, xh, yl, yh, slots, V, X):
    X1, Y1, Z = c1.shape
    half, n = Z // 2, X1 * Y1
    sub, lane = iota((8, Z), 0), iota((8, Z), 1)
    zero = jnp.zeros((8, Z), jnp.float32)
    body = lane < half
    for i in range(1, 2 * H + X1 - 1):
        CE[i, Y1 : 2 * Y1] = zero
    for x in range(X1):
        CE[H + x, 0:Y1] = c1[x]
        for b in range(2):
            k = 2 * x + b
            hi, lo = yh[V * (X // 2), pl.ds(k, 1)], yl[V * (X // 2), pl.ds(k, 1)]
            CE[H + x, pl.ds(Y1 + b, 1)] = keep(place.hi(1), hi)
            CE[H + x, pl.ds(2 * Y1 - 1 - b, 1)] = keep(place.lo(1), lo)
    for ref, ok, near, far in ((xl, place.lo(0), H - 1, H - 2), (xh, place.hi(0), H + X1, H + X1 + 1)):
        tile = keep(ok, ref[V * H, 0:Y1])
        CE[near, 0:Y1] = jnp.where(body, tile, zero)
        CE[far, 0:Y1] = jnp.where(body, roll(tile, half, 1), zero)
    for dx in (-1, 1):
        for dy in (-1, 1):
            d = (dx, dy, 0)
            line = keep(place.has(d), slots[place.slot(d), H, pl.ds(2, 1)])
            CE[H + X1 if dx > 0 else H - 1, pl.ds(Y1 if dy > 0 else 2 * Y1 - 1, 1)] = line
    own = lane % Y1 == sub
    rows = []
    for dx, dy in ((0, 0), (-1, 0), (1, 0), (0, -1), (0, 1)):
        pair = []
        for dz in (-1, 1):
            d = (dx, dy, dz)
            line = keep(place.has(d), slots[place.slot(d), H, pl.ds(2, 1)])
            pair.append(jnp.where(own, line, zero))
        rows.append(jnp.concatenate(pair, axis=1))
    rows = jnp.concatenate(rows, axis=0)
    li, lo = iota((2 * Z, Z), 0), iota((2 * Z, Z), 1)
    l = li % Z
    k = l // n
    target = jnp.where(li < Z, Z - 1 - k, half + k)
    for x in range(X1):
        d = dot(rows, onehot((lo == target) & (k < 2) & ((l % n) // Y1 == x)))
        CE[H + x, 0:Y1] = CE[H + x, 0:Y1] + d[0:8]
        if x == X1 - 1:
            CE[H - 1, 0:Y1] = CE[H - 1, 0:Y1] + d[8:16]
        if x == 0:
            CE[H + X1, 0:Y1] = CE[H + X1, 0:Y1] + d[16:24]
        edge = jnp.where(sub == 7, d[24:32], jnp.where(sub == 0, d[32:40], zero))
        CE[H + x, Y1 : 2 * Y1] = CE[H + x, Y1 : 2 * Y1] + edge


def contributions(place, U, gram_row, CE, GL, VL, Q, V):
    X1, R1, Z = CE.shape[0] - 2 * H, CE.shape[1], CE.shape[2]
    Y1, half = R1 // 2, Z // 2
    zero = jnp.zeros((R1, Z), jnp.float32)
    n = X1 * Y1
    for v in range(V):
        for i in range(2 * H + X1):
            if H <= i < H + X1:
                k = v * n + (i - H) * Y1
                GL[v, i, 0:Y1] = U[k : k + Y1]
                GL[v, i, Y1:R1] = zero[0:Y1]
            else:
                GL[v, i] = zero
        for i in (0, 1, 2 * H + X1 - 2, 2 * H + X1 - 1):
            VL[v, i] = zero
    mask = coarse_masks(place, R1, Z)
    for i in range(H - 1, H + X1 + 1):
        m = scaled(x_flag(place, i, X1), mask)
        for v in range(V):
            get = lambda j: GL[v, j]
            VL[v, i] = m * (PRE_G * GL[v, i] + PRE_N * level1_sum(get, i))
    block = {1: 0, 2: 1, 3: 2 * V, 0: 2 * V + 1}
    for w in range(X1 // 2 + 2):
        for v in range(V):
            total = None
            for i in (H - 2 + 2 * w, H - 1 + 2 * w):
                get = lambda j: VL[v, j]
                part = CE[i] * (6.0 * (GL[v, i] - VL[v, i]) + level1_sum(get, i))
                total = part if total is None else total + part
            Q[pl.ds((block[w] + 2 * v) * R1, R1)] = total
    li, lo = iota((Z, 2 * Z), 0), iota((Z, 2 * Z), 1)
    width = half // 2
    out = None
    for j in range(-1, Y1 // 2 + 1):
        r = (2 * j) % R1
        rows = Q[pl.ds(r, 4 * V, stride=R1)] + Q[pl.ds(r + 1, 4 * V, stride=R1)]
        start = Z if j < 0 else Z + width if j == Y1 // 2 else j * width
        rim = Z + 2 * width + j + 1
        to = jnp.where(li < half, start + li // 2, jnp.where(li < half + 2, rim + 8, rim))
        used = (li < half + 2) | (li >= Z - 2)
        part = dot(rows, onehot((lo == to) & used, 0.25 * 0.125))
        out = part if out is None else out + part
    lane4 = iota((4, Z), 1)
    pairs = []
    for p in range(V // 2):
        r, q = 4 * p, 2 * V + 4 * p
        own, rim = out[r : r + 4, 0:Z], out[r : r + 4, Z:]
        beside, beside_rim = out[q : q + 4, 0:Z], out[q : q + 4, Z:]
        edges = jnp.where(lane4 < half, rim, roll(beside_rim, half, 1))
        ends = jnp.where(lane4 < half, gram_row, jnp.where(lane4 < half + 16, rim, roll(beside_rim, 16, 1)))
        pairs.append((own, edges, beside, ends))
    return pairs


def coarse_masks(place, R, Z):
    half = Z // 2
    row, lane = iota((R, Z), 0), iota((R, Z), 1)
    y = R // 2
    mask = onehot(row < y) + onehot((row >= y) & (row < y + H)) * f32(place.hi(1))
    mask = mask + onehot(row >= R - H) * f32(place.lo(1))
    lanes = onehot(lane < half) + onehot((lane >= half) & (lane < half + H)) * f32(place.hi(2))
    lanes = lanes + onehot(lane >= Z - H) * f32(place.lo(2))
    return mask * lanes


def level1_sum(get, i):
    cur = get(i)
    return spread(cur, get(i - 1), get(i + 1), roll(cur, 1, 1), roll(cur, -1, 1))


def third_kernel(counts, merge_y, p1, xl, xh, yl, yh, slots, *refs):
    edges, (G1, S1) = refs[:-2], refs[-2:]
    VP, X, Y, Z = p1.shape
    V, R, half = 2 * VP, 2 * Y, Z // 2
    place = Place(counts)
    row, lane = iota((Y, Z), 0), iota((Y, Z), 1)
    zero = jnp.zeros((Y, Z), jnp.float32)

    def unpack(tile, v):
        return jnp.where(lane < half, roll(tile, half, 1) if v % 2 else tile, zero)

    r8, l8 = iota((8, Z), 0), iota((8, Z), 1)
    target = jnp.where(r8 < 4, Z - H, half) + r8 % 4
    place_lanes = onehot((l8 == target) & (r8 % 4 < H))

    def layers(dx, dy):
        below, above = (dx, dy, -1), (dx, dy, 1)
        low = keep(place.has(below), slots[place.slot(below), TAIL])
        high = keep(place.has(above), slots[place.slot(above), TAIL])
        return dot(jnp.concatenate([low, high], axis=0), place_lanes, TN)

    mid, up, down = layers(0, 0), layers(0, 1), layers(0, -1)
    m_hi = jnp.logical_and(row < H, place.hi(1))
    m_lo = jnp.logical_and(row >= Y - H, place.lo(1))

    def tile_of(d, v, x):
        k = (v * X + x) * Y
        return d[k : k + Y]

    for v in range(V):
        for x in range(X):
            G1[v, H + x, 0:Y] = unpack(p1[v // 2, x], v) + tile_of(mid, v, x)
            hi = unpack(yh[v // 2, x], v) + tile_of(up, v, x)
            lo = unpack(yl[v // 2, x], v) + tile_of(down, v, x)
            G1[v, H + x, Y:R] = jnp.where(m_hi, hi, jnp.where(m_lo, lo, zero))
    for dx in (-1, 1):
        side, up, down = layers(dx, 0), layers(dx, 1), layers(dx, -1)
        src = xh if dx > 0 else xl
        ok = place.hi(0) if dx > 0 else place.lo(0)
        for v in range(V):
            for a in range(H):
                x = a if dx > 0 else X - 1 - a
                i = H + X + a if dx > 0 else H - 1 - a
                G1[v, i, 0:Y] = keep(ok, unpack(src[v // 2, x], v) + tile_of(side, v, x))
                tile = zero
                if a < 2:
                    tile = jnp.where(m_hi, tile_of(up, v, x), jnp.where(m_lo, tile_of(down, v, x), zero))
                G1[v, i, Y:R] = tile
    for ref, (sx, sy) in zip(edges, edge_steps(merge_y)):
        dx = -sx
        for dy in (-1, 1) if sy == 0 else (-sy,):
            ok = place.has((dx, dy, 0))
            for cell, (a, b) in enumerate(EDGE1):
                i = H + X + a if dx > 0 else H - 1 - a
                r = Y + b if dy > 0 else R - 1 - b
                for v in range(V):
                    line = ref[pl.ds(cell * VP + v // 2, 1)]
                    line = roll(line, half, 1) if v % 2 else line
                    use = jnp.logical_and(lane[0:1] < half, ok)
                    line = jnp.where(use, line, jnp.zeros((1, Z), jnp.float32))
                    G1[v, i, pl.ds(r, 1)] = G1[v, i, pl.ds(r, 1)] + line
    mask = coarse_masks(place, R, Z)
    for i in range(1, 2 * H + X - 1):
        m = scaled(x_flag(place, i, X), mask)
        for v in range(V):
            get = lambda j: G1[v, j]
            S1[v, i] = m * (PRE_G * G1[v, i] + PRE_N * level1_sum(get, i))


def grid_of(count_y, count_x, fn):
    return [[fn(y, x) for x in range(count_x)] for y in range(count_y)]


def assemble(counts, parts_y, tile, lane):
    nx, ny, nz = counts
    width = lane.shape[1] // parts_y

    def one(y, x):
        y, j = y // parts_y, y % parts_y
        acc = roll(tile[(x * ny + y) * nz], -width * j, 1)
        for z in range(1, nz):
            acc = jnp.where(lane // width == z, roll(tile[(x * ny + y) * nz + z], width * (z - j), 1), acc)
        return acc

    return grid_of(ny * parts_y, nx, one)


def gather_parts(counts, parts_y, slots, lane, odd):
    nx, ny, nz = counts
    width = lane.shape[1] // parts_y

    def tile(x, y, z, k):
        t = (x * ny + y) * nz + z
        return jnp.concatenate([slots[t, k], slots[t, k]], axis=0)

    def joined(own, beside, x, y, z):
        zero = jnp.zeros(lane.shape, jnp.float32)
        before = beside[x - 1, y, z] if x else zero
        after = beside[x + 1, y, z] if x < nx - 1 else zero
        return own[x, y, z] + jnp.where(odd, after, before)

    half = lane.shape[1] // 2
    every = [(x, y, z) for x in range(nx) for y in range(ny) for z in range(nz)]
    edges, ends = {p: tile(*p, 1) for p in every}, {p: tile(*p, 3) for p in every}
    own = {p: tile(*p, 0) for p in every}
    beside = {p: tile(*p, 2) for p in every}
    own_rim = {p: jnp.where(lane < half, edges[p], ends[p]) for p in every}
    beside_rim = {p: jnp.where(lane < half, roll(edges[p], half, 1), roll(ends[p], -16, 1)) for p in every}
    main = {p: joined(own, beside, *p) for p in every}
    rim = {p: joined(own_rim, beside_rim, *p) for p in every}

    def one(yy, x):
        y, j = yy // parts_y, yy % parts_y
        sources = [(main, y, j, j)]
        if j == 0 and y:
            sources.append((rim, y - 1, 1, parts_y))
        if j == parts_y - 1 and y < ny - 1:
            sources.append((rim, y + 1, 0, -1))
        total = None
        for grid, from_y, chunk, inner in sources:
            acc = roll(grid[x, from_y, 0], -width * chunk, 1)
            for z in range(1, nz):
                acc = jnp.where(lane // width == z, roll(grid[x, from_y, z], width * (z - chunk), 1), acc)
            for z in range(nz):
                at = 2 * width + inner + 1
                if z:
                    to = width * z - 1
                    acc = acc + jnp.where(lane == to, roll(rim[x, from_y, z], to - at, 1), jnp.zeros_like(acc))
                if z < nz - 1:
                    to = width * (z + 1)
                    acc = acc + jnp.where(lane == to, roll(rim[x, from_y, z], to - at - 8, 1), jnp.zeros_like(acc))
            total = acc if total is None else total + acc
        return total

    return grid_of(ny * parts_y, nx, one)


def combine(fn, *grids):
    return [[fn(*ts) for ts in zip(*lines)] for lines in zip(*grids)]


def add(*terms):
    total = None
    for term in terms:
        if term is not None:
            total = term if total is None else total + term
    return total


def shrink_tiles(v, level, odd, lane):
    step = 2 ** (level - 2)
    v = [[a + b for a, b in zip(v[2 * y], v[2 * y + 1])] for y in range(len(v) // 2)]
    if level == 2:
        v = combine(lambda t: t + jnp.where(odd, roll(t, 1, 0), roll(t, -1, 0)), v)
    else:
        v = [[line[2 * x] + line[2 * x + 1] for x in range(len(line) // 2)] for line in v]
    upper = (lane // step) % 2 == 1
    return combine(lambda t: 0.125 * (t + jnp.where(upper, roll(t, step, 1), roll(t, -step, 1))), v)


def weights_kernel(counts, parts_y, c2s, *outs):
    lane = iota((8, outs[0].shape[-1]), 1)
    odd = iota(lane.shape, 0) % 2 == 1
    count = counts[0] * counts[1] * counts[2]
    rows = [jnp.where(odd, c2s[t, pl.ds(1, 1)], c2s[t, pl.ds(0, 1)]) for t in range(count)]
    c = assemble(counts, parts_y, rows, lane)
    for level in range(2, LEVELS):
        for y in range(len(c)):
            for x in range(len(c[0])):
                outs[level - 2][y, x] = (0.25**level) * c[y][x]
        if level < LEVELS - 1:
            c = shrink_tiles(c, level, odd, lane)


def coarse_kernel(counts, parts_y, slots1, *refs):
    *weights, mine, other, W, pre = refs
    nx, ny, nz = counts
    Z = slots1.shape[3]
    place = Place(counts)
    width = Z // parts_y
    lane = iota((8, Z), 1)
    odd = iota((8, Z), 0) % 2 == 1
    zero = jnp.zeros((8, Z), jnp.float32)
    scale = {2 + i: ref for i, ref in enumerate(weights)}
    inverse = {}
    for level, ref in scale.items():
        inverse[level] = grid_of(ref.shape[0], ref.shape[1], lambda y, x: 1.0 / (6.0 * ref[y, x]))

    def at(v, y, x):
        inside = 0 <= y < len(v) and 0 <= x < len(v[0])
        return v[y][x] if inside else None

    def neighbours(v, level):
        step = 2 ** (level - 2)
        ahead = [[roll(t, -1, 0) for t in line] for line in v] if level == 2 else None
        back = [[roll(t, 1, 0) for t in line] for line in v] if level == 2 else None

        def one(y, x):
            t = v[y][x]
            zs = jnp.where(lane < step, zero, roll(t, step, 1)) + jnp.where(lane >= Z - step, zero, roll(t, -step, 1))
            ys = add(zs, at(v, y - 1, x), at(v, y + 1, x))
            if level > 2:
                return add(ys, at(v, y, x - 1), at(v, y, x + 1))
            return ys + jnp.where(
                odd, add(back[y][x], at(back, y, x + 1)), add(ahead[y][x], at(ahead, y, x - 1))
            )

        return grid_of(len(v), len(v[0]), one)

    def grow(v, level):
        v = [line for line in v for _ in range(2)]
        return v if level == 2 else [[t for t in line for _ in range(2)] for line in v]

    def sweep(v, g, level):
        return combine(lambda a, b, s: KEEP * a + OMEGA * b + SIXTH * s, v, g, neighbours(v, level))

    def cycle(g, level):
        if level == LEVELS - 1:
            v = combine(lambda b: OMEGA * b, g)
            for _ in range(COARSE_SWEEPS - 1):
                v = sweep(v, g, level)
            return v
        v = combine(lambda b, s: PRE_G * b + PRE_N * s, g, neighbours(g, level))
        c = grid_of(len(g), len(g[0]), lambda y, x: scale[level][y, x])
        r = combine(lambda c, b, a, s: c * (6.0 * (b - a) + s), c, g, v, neighbours(v, level))
        down = shrink_tiles(r, level, odd, lane)
        down = grid_of(len(down), len(down[0]), lambda y, x: down[y][x] * inverse[level + 1][y][x])
        v = combine(lambda a, b: a + b, v, grow(cycle(down, level + 1), level))
        return sweep(v, g, level)

    b2 = gather_parts(counts, parts_y, slots1, lane, odd)
    v = cycle(grid_of(len(b2), nx, lambda y, x: b2[y][x] * inverse[2][y][x]), 2)
    for y in range(len(v)):
        for x in range(nx):
            W[y, x] = v[y][x]
    pre[...] = jnp.zeros_like(pre)
    ix, iy, iz = place.at
    for side, dev in enumerate((ix, ix + 1 - 2 * (ix % 2))):
        for xw in range(4):
            x = dev + (xw + 1) // 2 - 1
            x_ok = jnp.logical_and(x >= 0, x < nx)
            x = jnp.clip(x, 0, nx - 1)
            for j in range(-1, parts_y + 1):
                y = iy * parts_y + j
                ok = jnp.logical_and(x_ok, jnp.logical_and(y >= 0, y < ny * parts_y))
                y = jnp.clip(y, 0, ny * parts_y - 1)
                for vec in range(2):
                    line = W[y, x, pl.ds(vec * 2 + (xw + 1) % 2, 1)]
                    pre[2 * side + vec, xw, pl.ds(j % 8, 1)] = keep(ok, line)
    li, lo = iota((Z, Z), 0), iota((Z, Z), 1)
    z1 = jnp.where(lo < 96, lo, lo - Z)
    window = onehot(li == iz * width + jnp.floor_divide(z1 + 2, 2) - 1)
    moved = dot(pre[...].reshape(4 * 4 * 8, Z), window).reshape(4, 4, 8, Z)
    mine[...] = moved[0:2]
    other[...] = moved[2:4]


def last_kernel(counts, mine, other, G1, S1, G, S, c, pre_hbm, op_hbm, E1, C1, E0, C0, pre, op, sems):
    V, X1, Y1, Z = S1.shape[0], S1.shape[1] - 2 * H, S1.shape[2] // 2, S1.shape[3]
    X, Y = 2 * X1, 2 * Y1
    R1, R = 2 * Y1, Y + 8
    place = Place(counts)
    for v in range(V):
        for x in range(X1):
            k = (v * X1 + x) * R1
            held = place.at[0] % 2 == v // 2
            tile = jnp.where(held, mine[v % 2, x], other[v % 2, x])
            E1[pl.ds(k, 8, stride=2)] = tile
            E1[pl.ds(k + 1, 8, stride=2)] = tile
    for v in range(V):
        for i in range(1, 2 * H + X1 - 1):
            C1[v, i] = S1[v, i] + E1[pl.ds((v * X1 + (i - 1) // 2) * R1, R1)]
    mask = coarse_masks(place, R1, Z)
    n = X1 + 2
    fine = []
    for v in range(V):
        tiles = []
        for i in range(H - 1, H + X1 + 1):
            m = scaled(x_flag(place, i, X1), mask)
            get = lambda j: C1[v, j]
            tiles.append(m * (KEEP * C1[v, i] + OMEGA * G1[v, i] + SIXTH * level1_sum(get, i)))
        fine.append(jnp.concatenate(tiles, axis=0))
    li, lo = iota((Z, Z), 0), iota((Z, Z), 1)
    double = onehot(li == lo // 2)
    half = Z // 2
    k = lo % 8
    low_side = (lo // 8) % 2 == 0
    source = jnp.where(low_side, jnp.where(k < H, Z - 1, 0), jnp.where(k < 2, half - 1, half))
    rim = None
    for v in range(V):
        part = dot(fine[v], onehot((li == source) & (lo // 16 == v)))
        rim = part if rim is None else rim + part
    sub = iota((8, Z), 0)
    zero8 = jnp.zeros((8, Z), jnp.float32)
    for v in range(V + 1):
        wide = dot(fine[v], double) if v < V else rim
        for i in range(n):
            base = (v * n + i) * R
            tile = wide[i * R1 : i * R1 + Y1]
            edge = wide[i * R1 + Y1 : (i + 1) * R1]
            E0[pl.ds(base, 8, stride=2)] = tile
            E0[pl.ds(base + 1, 8, stride=2)] = tile
            E0[pl.ds(base + Y, 8)] = jnp.where(sub < 2, edge[0:1], jnp.where(sub >= 6, edge[7:8], zero8))
    for v in range(V + 1):
        for i in range(1, 2 * H + X - 1):
            C0[v, i] = S[v, i] + E0[pl.ds((v * n + (i - 1) // 2) * R, R)]
    ym, zm = fine_masks(place, Y, Z)
    lane = iota((R, Z), 1)
    for i in range(H - 1, H + X + 1):
        flag = x_flag(place, i, X)
        for v in range(V + 1):
            m = scaled(flag, ym if v < V else zm)
            value = m * (KEEP * C0[v, i] + OMEGA * G[v, i] + SIXTH * fine_sum(C0, v, i, V, lane))
            E0[pl.ds((v * (X + 2) + i - H + 1) * R, R)] = value
            if v < V and H <= i < H + X:
                pre[v, i - H] = value[0:Y]
    copies = [pltpu.make_async_copy(pre, pre_hbm, sems.at[0])]
    copies[0].start()

    class View:
        def __getitem__(self, key):
            v, i = key
            return E0[pl.ds((v * (X + 2) + i - H + 1) * R, R)]

    view = View()
    for x in range(X):
        for v in range(V):
            around = fine_sum(view, v, H + x, V, lane)
            op[v, x] = c[x] * (6.0 * view[v, H + x][0:Y] - around[0:Y])
        if x % 2:
            part = slice(x - 1, x + 1)
            copies.append(pltpu.make_async_copy(op.at[:, part], op_hbm.at[:, part], sems.at[1 + x // 2]))
            copies[-1].start()
    for copy in copies:
        copy.wait()


def gram_kernel(old, prev, out):
    M, X, Y, Z = old.shape
    J = prev.shape[0]
    pairs = [(a, b) for a in range(M + J) for b in range(a, M + J)]
    sums = [None] * len(pairs)
    for x in range(X):
        for y in range(0, Y, 8):
            tiles = [old[m, x, y : y + 8] for m in range(M)] + [prev[j, x, y : y + 8] for j in range(J)]
            for p, (a, b) in enumerate(pairs):
                term = tiles[a] * tiles[b]
                sums[p] = term if sums[p] is None else sums[p] + term
    ones = jnp.ones((8, Z), jnp.float32)
    lane = iota((8, Z), 1)
    rows = jnp.concatenate([jnp.sum(s, axis=0, keepdims=True) for s in sums], axis=0)
    pad = jnp.zeros((Z - len(pairs), Z), jnp.float32)
    out[...] = dot(ones, jnp.concatenate([rows, pad], axis=0), NT)


def ortho_kernel(count, cells, old, prev, slots, orth, proj, tri):
    M, X, Y, Z = old.shape
    J = prev.shape[0]
    if count <= 64:
        total = slots[0, TAIL - 1, pl.ds(0, 1)]
        for t in range(1, count):
            total = total + slots[t, TAIL - 1, pl.ds(0, 1)]
    else:
        total = lax.fori_loop(0, count, lambda t, s: s + slots[t, TAIL - 1, pl.ds(0, 1)], jnp.zeros((1, Z), jnp.float32))
    total = jnp.broadcast_to(total, (8, Z)) / cells
    value = {}
    p = 0
    for a in range(M + J):
        for b in range(a, M + J):
            one = jnp.broadcast_to(total[:, p : p + 1], (8, Z))
            value[a, b] = value[b, a] = one
            p += 1
    P_ = [[value[m, M + j] for j in range(J)] for m in range(M)]
    gram = {}
    for i in range(J):
        for j in range(i + 1):
            s = value[M + i, M + j]
            for m in range(M):
                inner = None
                for k in range(M):
                    term = value[m, k] * P_[k][j]
                    inner = term if inner is None else inner + term
                s = s - P_[m][i] * (P_[m][j] - inner) - P_[m][j] * P_[m][i]
            gram[i, j] = s
    L = {}
    for i in range(J):
        for j in range(i + 1):
            s = gram[i, j]
            for k in range(j):
                s = s - L[i, k] * L[j, k]
            L[i, j] = jnp.sqrt(s) if i == j else s / L[j, j]
    inv = {}
    for i in range(J):
        for j in range(i + 1):
            s = jnp.ones((8, Z), jnp.float32) if i == j else None
            for k in range(j, i):
                term = L[i, k] * inv[k, j]
                s = -term if s is None else s - term
            inv[i, j] = s / L[i, i]
    row, col = iota((M, J), 0), iota((M, J), 1)
    proj_v, tri_v = jnp.zeros((M, J), jnp.float32), jnp.zeros((J, J), jnp.float32)
    for m in range(M):
        for j in range(J):
            here = (row == m) & (col == j)
            proj_v = jnp.where(here, P_[m][j][0:M, 0:J], proj_v)
            if j >= m:
                tri_v = jnp.where(here, L[j, m][0:J, 0:J], tri_v)
    proj[...] = proj_v
    tri[...] = tri_v
    mix = {}
    for j in range(J):
        for m in range(M):
            s = None
            for i in range(j + 1):
                term = inv[j, i] * P_[m][i]
                s = term if s is None else s + term
            mix[j, m] = s
    for x in range(X):
        for y in range(0, Y, 8):
            olds = [old[m, x, y : y + 8] for m in range(M)]
            rem = []
            for i in range(J):
                r = prev[i, x, y : y + 8]
                for m in range(M):
                    r = r - P_[m][i] * olds[m]
                rem.append(r)
            for j in range(J):
                s = None
                for i in range(j + 1):
                    term = inv[j, i] * rem[i]
                    s = term if s is None else s + term
                orth[j, x, y : y + 8] = s


def run(near, kernel, shapes, args, scratch=(), name=None, result=(), plain=(), sems=0, out_sems=0):
    outs = []
    for i, shape in enumerate(shapes):
        kind = jax.ShapeDtypeStruct if i in result or not near else pltpu.VMEM
        outs.append(kind(shape, jnp.float32))
    if near:
        spaces = [pltpu.HBM if sems else None if i in plain else pltpu.VMEM for i in range(len(args))]
        args = [pltpu.with_memory_space_constraint(a, m) if m else a for a, m in zip(args, spaces)]
    fn = pl.pallas_call(
        kernel,
        out_shape=outs,
        in_specs=[HB if sems else VM] * len(args),
        out_specs=[HB if out_sems and i in result else VM for i in range(len(shapes))],
        scratch_shapes=[pltpu.VMEM(s, jnp.float32) for s in scratch] + [pltpu.SemaphoreType.DMA((sems + out_sems,))] * (sems + out_sems > 0),
        compiler_params=pltpu.CompilerParams(vmem_limit_bytes=16 * 2**20) if near else None,
        name=name,
    )
    return fn(*args)


def shift(value, axis, step):
    n = lax.axis_size(axis)
    return lax.ppermute(value, axis, [(i, (i + step) % n) for i in range(n)])


def diagonal(counts, value, dx, dy):
    nx, ny = counts[:2]
    step = dy if dy else 1
    pairs = [(x * ny + y, (x + dx) % nx * ny + (y + step) % ny) for x in range(nx) for y in range(ny)]
    return lax.ppermute(value, ("gx", "gy"), pairs)


def swap(slots):
    return lax.all_to_all(slots, AXES, split_axis=0, concat_axis=0, tiled=True)


def wide_coarse(counts, parts_y, c2s, slots1):
    nx, ny, nz = counts
    Z = slots1.shape[3]
    width = Z // parts_y
    lead, half = 2, Z // 2

    def across_x(own, beside):
        own, beside = (
            t.reshape(nx, ny, nz, lead, 2, Z).transpose(3, 4, 0, 1, 2, 5) for t in (own, beside)
        )
        pad = ((0, 0), (1, 1), (0, 0), (0, 0), (0, 0))
        first = own[:, 0] + jnp.pad(beside[:, 0], pad)[:, 0:nx]
        last = own[:, 1] + jnp.pad(beside[:, 1], pad)[:, 2:]
        return jnp.stack([first, last], axis=2).reshape(lead, 2 * nx, ny, nz, Z)

    edges, ends = slots1[:, 1], slots1[:, 3]
    low = iota((1, 1, Z), 2) < half
    main = across_x(slots1[:, 0], slots1[:, 2])
    rim = across_x(
        jnp.where(low, edges, ends), jnp.where(low, jnp.roll(edges, half, 2), jnp.roll(ends, -16, 2))
    )

    def with_z(line, low, high):
        pad = ((0, 0), (0, 0), (0, 0), (1, 1))
        first = jnp.pad(high, pad)[..., 0:nz]
        last = jnp.pad(low, pad)[..., 2:]
        lanes = iota((1, width), 1)[0]
        line = line + jnp.where(lanes == 0, first[..., None], 0.0) + jnp.where(lanes == width - 1, last[..., None], 0.0)
        return line.reshape(lead, 2 * nx, ny, nz * width)

    lines = []
    for j in range(-1, parts_y + 1):
        source, start = (rim, 0) if j < 0 else (rim, width) if j == parts_y else (main, j * width)
        at = 2 * width + j + 1
        lines.append(with_z(source[..., start : start + width], rim[..., at], rim[..., at + 8]))
    pad = ((0, 0), (0, 0), (1, 1), (0, 0))
    lines[1] = lines[1] + jnp.pad(lines[-1], pad)[:, :, 0:ny]
    lines[parts_y] = lines[parts_y] + jnp.pad(lines[0], pad)[:, :, 2:]
    b2 = jnp.stack(lines[1:-1], axis=3).reshape(lead, 2 * nx, ny * parts_y, nz * width)

    def whole(t, lead):
        t = t.reshape(nx, ny, nz, lead * 2, Z)
        parts = []
        for j in range(parts_y):
            part = t[..., j * width : (j + 1) * width].transpose(3, 0, 1, 2, 4)
            parts.append(part.reshape(lead * 2, nx, ny, nz * width))
        t = jnp.stack(parts, axis=3).reshape(lead, 2, nx, ny * parts_y, nz * width)
        return t.transpose(0, 2, 1, 3, 4).reshape(lead, nx * 2, ny * parts_y, nz * width)

    c2 = whole(c2s[:, 0:2], 1)
    g2 = b2 / (6.0 * 0.0625 * c2)

    def around(v):
        p = jnp.pad(v, ((0, 0), (1, 1), (1, 1), (1, 1)))
        m = slice(1, -1)
        return (
            p[:, 2:, m, m] + p[:, :-2, m, m] + p[:, m, 2:, m] + p[:, m, :-2, m] + p[:, m, m, 2:] + p[:, m, m, :-2]
        )

    def pairs(e):
        return onehot(iota((e, 2 * e), 0) == iota((e, 2 * e), 1) // 2)

    def shrink(v):
        d, a, b, e = v.shape
        v = v.reshape(d, a // 2, 2, b, e).sum(axis=2)
        v = v[:, :, 0::2] + v[:, :, 1::2]
        return dot(v.reshape(-1, e), pairs(e // 2).T * 0.125).reshape(d, a // 2, b // 2, e // 2)

    def grow(v):
        d, a, b, e = v.shape
        v = dot(v.reshape(-1, e), pairs(e)).reshape(d, a, b, 2 * e)
        return jnp.repeat(jnp.repeat(v, 2, axis=1), 2, axis=2)

    def cycle(g, c, level):
        if level == LEVELS - 1:
            v = OMEGA * g
            for _ in range(COARSE_SWEEPS - 1):
                v = KEEP * v + OMEGA * g + SIXTH * around(v)
            return v
        v = PRE_G * g + PRE_N * around(g)
        r = 0.25**level * c * (6.0 * (g - v) + around(v))
        down = shrink(c)
        v = v + grow(cycle(shrink(r) / (6.0 * 0.25 ** (level + 1) * down), down, level + 1))
        return KEEP * v + OMEGA * g + SIXTH * around(v)

    e = jnp.pad(cycle(g2, c2, 2), ((0, 0), (1, 1), (1, 1), (1, 1)))
    ix, iy, iz = (lax.axis_index(a) for a in AXES)

    def window(x):
        w = lax.dynamic_slice(
            e, (jnp.int32(0), x * 2, iy * parts_y, iz * width), (lead, 4, parts_y + 2, width + 2)
        )
        w = jnp.repeat(w, 2, axis=3)
        gap = jnp.zeros(w.shape[:3] + (Z - 2 * width - 4,), w.dtype)
        w = jnp.concatenate([w[..., 2:], gap, w[..., :2]], axis=3)
        pad = jnp.zeros((lead, 4, 8 - parts_y - 2, Z), w.dtype)
        return jnp.concatenate([w[:, :, 1:], pad, w[:, :, :1]], axis=2)

    return window(ix), window(ix + 1 - 2 * (ix % 2))


def per_device(counts, old, prev, inc, c):
    V, X, Y, Z = inc.shape
    count = counts[0] * counts[1] * counts[2]
    merge_y = counts[1] == 2
    near = count <= 64
    R = Y + 8
    X1, Y1 = X // 2, Y // 2
    y_shape, x_shape = (V * (X // 2) + 1, 8, Z), (V * H + 1, Y, Z)
    shapes = [(V, X, Y, Z), x_shape, x_shape, y_shape]
    shapes += [] if merge_y else [y_shape]
    shapes += [(count, H + 1, V, Z), (X1, Y1, Z)]
    outs = run(
        near,
        functools.partial(first_kernel, counts, merge_y),
        shapes,
        (inc, c),
        [inc.shape, c.shape, (X1 * Y, Z)],
        name="first",
        result=(len(shapes) - 2,),
        sems=V + 1,
    )
    g, xlo, xhi = outs[:3]
    c1 = outs[-1]
    slots0 = swap(outs[-2])
    xl, xh = shift(xhi, "gx", 1), shift(xlo, "gx", -1)
    if merge_y:
        yl = yh = shift(outs[3], "gy", 1)
    else:
        yl, yh = shift(outs[4], "gy", 1), shift(outs[3], "gy", -1)
    (gram,) = run(near, gram_kernel, [(8, Z)], (old, prev), name="gram", plain=(0, 1))
    ext0, ext1 = (V + 1, X + 2 * H, R, Z), (V, X1 + 2 * H, 2 * Y1, Z)
    steps = edge_steps(merge_y)
    G, S, p1, slots1, c2s, *edges = run(
        near,
        functools.partial(second_kernel, counts, merge_y),
        [ext0, ext0, (V // 2, X1, Y1, Z), (count, TAIL + 1, V, Z), (count, V, Z)] + [(16, Z)] * len(steps),
        (g, c, c1, xl, xh, yl, yh, slots0, gram),
        [(V * X1 * Y, Z), ext1[1:], ext1, ext1],
        name="second",
        result=(3,),
    )
    slots1 = swap(slots1)
    edges = [diagonal(counts, e, dx, dy) for e, (dx, dy) in zip(edges, steps)]
    xl, xh = shift(p1, "gx", 1), shift(p1, "gx", -1)
    if merge_y:
        yl = yh = shift(p1, "gy", 1)
    else:
        yl, yh = shift(p1, "gy", 1), shift(p1, "gy", -1)
    slots1, xl, xh, yl, yh, *edges = lax.optimization_barrier((slots1, xl, xh, yl, yh, *edges))
    G1, S1 = run(
        near,
        functools.partial(third_kernel, counts, merge_y),
        [ext1, ext1],
        (p1, xl, xh, yl, yh, slots1, *edges),
        name="third",
    )
    orth, proj, tri = run(
        near,
        functools.partial(ortho_kernel, count, float(count * X * Y * Z)),
        [(V, X, Y, Z), (4, 4), (4, 4)],
        (old, prev, slots1),
        name="ortho",
        result=(0, 1, 2),
        plain=(0, 1),
    )
    parts_y = Y // 4
    if near and counts[2] * (Z // parts_y) == Z:
        sizes = [(counts[1] * parts_y, counts[0], 8, Z)]
        for level in range(3, LEVELS):
            y, x = sizes[-1][:2]
            sizes.append((y // 2, x if level == 3 else x // 2, 8, Z))
        weights = run(
            near, functools.partial(weights_kernel, counts, parts_y), sizes, (c2s,), name="weights"
        )
        e2, others = run(
            near,
            functools.partial(coarse_kernel, counts, parts_y),
            [(V // 2, 4, 8, Z)] * 2,
            (slots1, *weights),
            [sizes[0], (V, 4, 8, Z)],
            name="coarse",
        )
    else:
        e2, others = wide_coarse(counts, parts_y, c2s, slots1)
    others = lax.ppermute(others, "gx", [(i, i ^ 1) for i in range(counts[0])])
    pre, op = run(
        near,
        functools.partial(last_kernel, counts),
        [(V, X, Y, Z), (V, X, Y, Z)],
        (e2, others, G1, S1, G, S, c),
        [(V * X1 * 2 * Y1, Z), ext1, ((V + 1) * (X + 2) * R, Z), ext0, (V, X, Y, Z), (V, X, Y, Z)],
        name="last",
        result=(0, 1),
        out_sems=1 + X // 2,
    )
    return orth, proj, tri, pre, op


def solution(mesh):
    block = P(None, *AXES)
    counts = tuple(mesh.shape[a] for a in AXES)
    return jax.shard_map(
        functools.partial(per_device, counts),
        mesh=mesh,
        in_specs=(block, block, block, P(*AXES)),
        out_specs=(block, P(), P(), block, block),
        check_vma=False,
    )
```

```python
import functools

import jax
import jax.numpy as jnp
from jax import lax
from jax.experimental import pallas as pl
from jax.experimental.pallas import tpu as pltpu
from jax.sharding import PartitionSpec as P

LEVELS = 6
COARSE_SWEEPS = 4
OMEGA = 0.8
KEEP = 1.0 - OMEGA
SIXTH = OMEGA / 6.0
PRE_G = OMEGA * (2.0 - OMEGA)
PRE_N = OMEGA * OMEGA / 6.0
AXES = ("gx", "gy", "gz")
HIGH = lax.Precision.HIGHEST
H = 3
NN = (((1,), (0,)), ((), ()))
NT = (((1,), (1,)), ((), ()))
TN = (((0,), (0,)), ((), ()))
VM = pl.BlockSpec(memory_space=pltpu.VMEM)
HB = pl.BlockSpec(memory_space=pltpu.HBM)
EDGE = ((0, 0), (0, 1), (1, 0))
EDGE1 = EDGE + ((1, 1), (0, 2), (2, 0))
TAIL = 4


def edge_steps(merge_y):
    return [(dx, dy) for dx in (1, -1) for dy in ((0,) if merge_y else (1, -1))]


def dot(a, b, dims=NN):
    return lax.dot_general(a, b, dims, precision=HIGH, preferred_element_type=jnp.float32)


def iota(shape, dim):
    return lax.broadcasted_iota(jnp.int32, shape, dim)


def onehot(cond, scale=1.0):
    return jnp.where(cond, jnp.float32(scale), jnp.float32(0.0))


def roll(a, shift, axis):
    size = a.shape[axis]
    shift = shift % size
    return a if shift == 0 else pltpu.roll(a, shift, axis)


class Place:
    def __init__(self, counts):
        self.counts = counts
        self.at = tuple(lax.axis_index(a) for a in AXES)
        self.me = self.linear(self.at)

    def linear(self, p):
        nx, ny, nz = self.counts
        return (p[0] * ny + p[1]) * nz + p[2]

    def lo(self, axis):
        return self.at[axis] > 0

    def hi(self, axis):
        return self.at[axis] < self.counts[axis] - 1

    def has(self, d):
        ok = None
        for axis in range(3):
            if d[axis]:
                one = self.hi(axis) if d[axis] > 0 else self.lo(axis)
                ok = one if ok is None else jnp.logical_and(ok, one)
        return ok

    def slot(self, d):
        there = self.linear(tuple(p + s for p, s in zip(self.at, d)))
        return jnp.where(self.has(d), there, self.me)


def f32(flag):
    return jnp.where(flag, jnp.float32(1.0), jnp.float32(0.0))


def keep(flag, a):
    return jnp.where(flag, a, jnp.zeros_like(a))


def fill_slots(ref, count, value, rows):
    if count <= 64:
        for t in range(count):
            ref[t, 0:rows] = value
    else:
        def body(t, carry):
            ref[t, 0:rows] = value
            return carry
        lax.fori_loop(0, count, body, 0)


def fill_tail(ref, count, k, value):
    if count <= 64:
        for t in range(count):
            ref[t, k] = value
    else:
        def body(t, carry):
            ref[t, k] = value
            return carry
        lax.fori_loop(0, count, body, 0)


def first_kernel(counts, merge_y, inc_hbm, c_hbm, *refs):
    if merge_y:
        g, xlo, xhi, ymsg, slots, c1, inc, c, QC, sems = refs
    else:
        g, xlo, xhi, ylo, yhi, slots, c1, inc, c, QC, sems = refs
    V, X, Y, Z = inc.shape
    place = Place(counts)
    copy_c = pltpu.make_async_copy(c_hbm, c, sems.at[V])
    copies = [pltpu.make_async_copy(inc_hbm.at[v], inc.at[v], sems.at[v]) for v in range(V)]
    copy_c.start()
    for copy in copies:
        copy.start()
    sub = iota((8, Z), 0)
    lane = iota((8, Z), 1)
    copy_c.wait()
    X1, Y1, half = X // 2, Y // 2, Z // 2
    for x in range(X1):
        QC[pl.ds(x * Y, Y)] = c[2 * x] + c[2 * x + 1]
    li, lo = iota((Z, Z), 0), iota((Z, Z), 1)
    n = X1 * Y1
    cc = dot(QC[pl.ds(0, n, stride=2)] + QC[pl.ds(1, n, stride=2)], onehot(lo == li // 2, 0.125))
    c1[...] = cc.reshape(X1, Y1, Z)
    stack = []
    for y in range(Y // 4):
        sums = []
        for x in range(X // 4):
            k = 2 * x * Y1 + 2 * y
            pair = cc[k : k + 2] + cc[k + Y1 : k + Y1 + 2]
            sums.append(pair[0:1] + pair[1:2])
        stack.append(jnp.where(sub % 2 == 0, sums[0], sums[1]))
    stack = dot(jnp.concatenate(stack, axis=0), onehot((lo == li // 2) & (li < half), 0.125))
    c2 = stack[0:8]
    for y in range(1, Y // 4):
        c2 = c2 + roll(stack[8 * y : 8 * y + 8], y * (half // 2), 1)
    r4, l4 = iota((4, Z), 0), iota((4, Z), 1)
    zero4 = jnp.zeros((4, Z), jnp.float32)
    base = [jnp.where(r4 == H, c2[x : x + 1], zero4) for x in range(2)] + [zero4] * (V - 2)
    for v in range(2):
        fill_tail(slots, counts[0] * counts[1] * counts[2], v, base[v])

    wide8 = lane < half
    xlo[V * H, 0:Y1] = jnp.where(wide8, c1[0], roll(c1[1], half, 1))
    xhi[V * H, 0:Y1] = jnp.where(wide8, c1[X1 - 1], roll(c1[X1 - 2], half, 1))
    ends = [(ymsg, jnp.where(place.at[1] == 0, 1, 0))] if merge_y else [(ylo, 0), (yhi, 1)]
    for ref, upper in ends:
        for x in range(X1):
            for b in range(2):
                y = jnp.where(upper == 1, Y1 - 1 - b, b)
                ref[V * (X // 2), pl.ds(2 * x + b, 1)] = c1[x, pl.ds(y, 1)]
    scale = [1.0 / (6.0 * c[x]) for x in range(X)]
    for v in range(V):
        copies[v].wait()
        for x in range(X):
            value = inc[v, x] * scale[x]
            g[v, x] = value
            if x < H:
                xlo[v * H + x] = value
            if x >= X - H:
                xhi[v * H + x - (X - H)] = value
    faces = []
    for x in range(X):
        for y in range(0, Y, 8):
            acc = jnp.zeros((8, Z), jnp.float32)
            for v in range(V):
                acc = jnp.where(lane // 8 == v, roll(g[v, x, y : y + 8], 8 * v + H, 1), acc)
            m = len(faces)
            if m < X1:
                acc = jnp.where(lane // 2 == 4 * V, roll(c1[m], 8 * V - half + 2, 1), acc)
                acc = jnp.where(lane // 2 == 4 * V + 1, roll(c1[m], 8 * V + 2, 1), acc)
            faces.append(acc)
    faces = jnp.concatenate(faces, axis=0).T
    k = 8 * V
    c_up = jnp.where(l4 < n, faces[k + 1 : k + 2], roll(faces[k : k + 8], n, 1)[0:1])
    c_down = jnp.where(l4 < n, faces[k + 2 : k + 3], roll(faces[k : k + 8], n, 1)[3:4])
    rows_up = [jnp.where(r4 < H, faces[8 * v : 8 * v + 4], base[v]) for v in range(V)]
    rows_down = [jnp.where(r4 < H, faces[8 * v + H : 8 * v + H + 4], base[v]) for v in range(V)]
    rows_up[2] = jnp.where(r4 < H, rows_up[2], jnp.where(l4 < 2 * n, c_up, zero4))
    rows_down[2] = jnp.where(r4 < H, rows_down[2], jnp.where(l4 < 2 * n, c_down, zero4))
    for dx in (-1, 0, 1):
        for dy in (-1, 0, 1):
            above, below = place.slot((dx, dy, 1)), place.slot((dx, dy, -1))
            for v in range(V):
                slots[above, v] = rows_up[v]
                slots[below, v] = rows_down[v]
            if dx and dy:
                t = place.slot((dx, dy, 0))
                for cell, (a, b) in enumerate(EDGE):
                    x = X - 1 - a if dx > 0 else a
                    y = Y - 1 - b if dy > 0 else b
                    for v in range(V):
                        slots[t, v, pl.ds(cell, 1)] = g[v, x, pl.ds(y, 1)]
                corner = c1[X1 - 1 if dx > 0 else 0, pl.ds(Y1 - 1 if dy > 0 else 0, 1)]
                slots[t, 2, pl.ds(H, 1)] = corner

    def packed(v, j, start, own):
        return jnp.where(own, g[v, 2 * j, pl.ds(start, 8)], roll(g[v, 2 * j + 1, pl.ds(start, 8)], 4, 0))

    for v in range(V):
        for j in range(X // 2):
            if merge_y:
                first = place.at[1] == 0
                start = pl.multiple_of(jnp.where(first, Y - 8, 0), 8)
                own = (sub + jnp.where(first, 0, 4)) % 8 >= 4
                ymsg[v * (X // 2) + j] = packed(v, j, start, own)
            else:
                yhi[v * (X // 2) + j] = packed(v, j, Y - 8, sub >= 4)
                ylo[v * (X // 2) + j] = packed(v, j, 0, sub < 4)


def spread(cur, below, above, zl, zr):
    return below + above + roll(cur, 1, 0) + roll(cur, -1, 0) + zl + zr


def fine_sum(ref, v, i, V, lane):
    cur = ref[v, i]
    zl, zr = roll(cur, 1, 1), roll(cur, -1, 1)
    if v < V:
        rim = ref[V, i]
        last = lane.shape[1] - 1
        zl = jnp.where(lane == 0, roll(rim, -(16 * v + 2), 1), zl)
        zr = jnp.where(lane == last, roll(rim, last - (16 * v + 8), 1), zr)
    return spread(cur, ref[v, i - 1], ref[v, i + 1], zl, zr)


def fine_masks(place, Y, Z):
    R = Y + 8
    row = iota((R, Z), 0)
    ym = onehot(row < Y) + onehot((row >= Y) & (row < Y + H)) * f32(place.hi(1))
    ym = ym + onehot(row >= R - H) * f32(place.lo(1))
    lane = iota((R, Z), 1)
    outside_lo, outside_hi = lane % 16 < H, lane % 16 >= 8
    zm = jnp.where(outside_lo, f32(place.lo(2)), jnp.where(outside_hi, f32(place.hi(2)), jnp.float32(1.0)))
    return ym, ym * zm


def x_flag(place, i, X):
    if i < H:
        return f32(place.lo(0))
    if i >= H + X:
        return f32(place.hi(0))
    return None


def scaled(flag, mask):
    return mask if flag is None else mask * flag


def second_kernel(counts, merge_y, g, c, c1, xl, xh, yl, yh, slots, gram, G, S, p1, slots1, c2s, *refs):
    edges, (Q, CE, GL, VL) = refs[:-4], refs[-4:]
    V, X, Y, Z = g.shape
    R = Y + 8
    place = Place(counts)
    sub = iota((8, Z), 0)
    zero8 = jnp.zeros((8, Z), jnp.float32)
    zero_y = jnp.zeros((Y, Z), jnp.float32)
    has_yl, has_yh, has_xl, has_xh = place.lo(1), place.hi(1), place.lo(0), place.hi(0)
    m_hi = jnp.logical_and(sub < H, has_yh)
    m_lo = jnp.logical_and(sub >= 8 - H, has_yl)
    for v in range(V):
        for x in range(X):
            G[v, H + x, 0:Y] = g[v, x]
            hi, lo = yh[v * (X // 2) + x // 2], yl[v * (X // 2) + x // 2]
            if x % 2:
                hi, lo = roll(hi, 4, 0), roll(lo, 4, 0)
            G[v, H + x, Y:R] = jnp.where(m_hi, hi, jnp.where(m_lo, lo, zero8))
        for i in range(H):
            G[v, i, 0:Y] = keep(has_xl, xl[v * H + i])
            G[v, i, Y:R] = zero8
            G[v, H + X + i, 0:Y] = keep(has_xh, xh[v * H + i])
            G[v, H + X + i, Y:R] = zero8
    for dx in (-1, 1):
        for dy in (-1, 1):
            ok, t = place.has((dx, dy, 0)), place.slot((dx, dy, 0))
            for cell, (a, b) in enumerate(EDGE):
                i = H + X + a if dx > 0 else H - 1 - a
                r = Y + b if dy > 0 else R - 1 - b
                for v in range(V):
                    G[v, i, pl.ds(r, 1)] = keep(ok, slots[t, v, pl.ds(cell, 1)])
    r4 = iota((4, Z), 0)
    zero4 = jnp.zeros((4, Z), jnp.float32)

    def layers(dx, dy):
        tiles = []
        for v in range(V):
            for dz in (-1, 1):
                d = (dx, dy, dz)
                use = jnp.logical_and(r4 < H, place.has(d))
                tiles += [jnp.where(use, slots[place.slot(d), v], zero4), zero4]
        return jnp.concatenate(tiles, axis=0)

    wide = iota((16 * V, Z), 1)
    mid = layers(0, 0)
    sides = jnp.where(wide % Y < 8, layers(0, 1), layers(0, -1))
    first = jnp.concatenate([mid, sides], axis=0).T
    edges_x = jnp.where(wide < 2 * Y, layers(1, 0), layers(-1, 0))
    for d, start, to in (((1, 1), 0, 2), ((1, -1), 0, 3), ((-1, 1), X - 1, 4), ((-1, -1), X - 1, 5)):
        edges_x = jnp.where(wide // Y == to, roll(layers(*d), (to - start) * Y, 1), edges_x)
    second = jnp.concatenate([edges_x, jnp.zeros((Z - 16 * V, Z), jnp.float32)], axis=0).T
    lane_y, lane_8 = iota((Y, Z), 1) < 16 * V, iota((8, Z), 1) < 16 * V
    for i in (0, H + X + H - 1):
        G[V, i] = jnp.zeros((R, Z), jnp.float32)
    for x in range(X):
        tile = first[x * Y : (x + 1) * Y]
        G[V, H + x, 0:Y] = jnp.where(lane_y, tile, zero_y)
        other = roll(tile, Z - 16 * V, 1)
        edge = jnp.where(sub < 2, other[0:8], jnp.where(sub >= 6, other[Y - 8 : Y], zero8))
        G[V, H + x, Y:R] = jnp.where(lane_8, edge, zero8)
    for base, at in ((H + X, 0), (H - 2, X - 2)):
        for a in range(2):
            G[V, base + a, 0:Y] = second[(at + a) * Y : (at + a + 1) * Y]
            G[V, base + a, Y:R] = zero8
    for i, a in ((H + X, 2), (H - 1, 4)):
        up, down = second[a * Y : a * Y + 8], second[(a + 2) * Y - 8 : (a + 2) * Y]
        G[V, i, Y:R] = jnp.where(sub < 2, up, jnp.where(sub >= 6, down, zero8))
    lane = iota((R, Z), 1)
    for i in range(1, 2 * H + X - 1):
        rim = G[V, i]
        for v in range(V):
            body = G[v, i]
            rim = jnp.where((lane == 16 * v + 3) | (lane == 16 * v + 4), roll(body, 16 * v + 3, 1), rim)
            rim = jnp.where((lane == 16 * v + 6) | (lane == 16 * v + 7), roll(body, 16 * v + 8, 1), rim)
        G[V, i] = rim
    ym, zm = fine_masks(place, Y, Z)
    for i in range(1, 2 * H + X - 1):
        flag = x_flag(place, i, X)
        for v in range(V + 1):
            mask = scaled(flag, ym if v < V else zm)
            S[v, i] = mask * (PRE_G * G[v, i] + PRE_N * fine_sum(G, v, i, V, lane))
    for x in range(X // 2):
        for v in range(V):
            total = None
            for i in (2 * x, 2 * x + 1):
                inner = 6.0 * (G[v, H + i] - S[v, H + i]) + fine_sum(S, v, H + i, V, lane)
                part = c[i] * inner[0:Y]
                total = part if total is None else total + part
            Q[pl.ds((v * (X // 2) + x) * Y, Y)] = total
    li, lo = iota((Z, Z), 0), iota((Z, Z), 1)
    halve = onehot(lo == li // 2, 0.125)
    n, nc = V * X * Y // 4, X * Y // 4
    b1 = dot(Q[pl.ds(0, n, stride=2)] + Q[pl.ds(1, n, stride=2)], halve)
    cc = c1[...].reshape(nc, Z)
    scale = 1.0 / (1.5 * jnp.where(iota((nc, Z), 1) < Z // 2, cc, jnp.float32(1.0)))
    U = jnp.concatenate([b1[v * nc : (v + 1) * nc] * scale for v in range(V)], axis=0)
    per = nc
    for vp in range(V // 2):
        both = U[2 * vp * per : (2 * vp + 1) * per] + roll(U[(2 * vp + 1) * per : (2 * vp + 2) * per], Z // 2, 1)
        p1[vp] = both.reshape(X // 2, Y // 2, Z)
    half = Z // 2
    ends = jnp.where(iota(U.shape, 1) < 8, roll(U, H - half, 1), roll(U, 8, 1)).T
    faces = ends[0:16]
    X1, Y1 = X // 2, Y // 2
    if counts[0] * counts[1] * counts[2] <= 64:
        for t in range(counts[0] * counts[1] * counts[2]):
            for x in range(2):
                c2s[t, pl.ds(x, 1)] = slots[t, x, pl.ds(H, 1)]
    else:
        def move(t, carry):
            for x in range(2):
                c2s[t, pl.ds(x, 1)] = slots[t, x, pl.ds(H, 1)]
            return carry
        lax.fori_loop(0, c2s.shape[0], move, 0)
    around_c1(place, CE, c1, xl, xh, yl, yh, slots, V, X)
    gram_row = gram[0:1]
    tiles = contributions(place, U, gram_row, CE, GL, VL, Q, V)
    up, down = faces[0:4], faces[8:12]
    rest = counts[1] * counts[2]
    for x in range(counts[0]):
        for k, tile in enumerate(tiles[x % 2]):
            fill_tail(slots1.at[pl.ds(x * rest, rest)], rest, k, tile)
    for dx in (-1, 0, 1):
        for dy in (-1, 0, 1):
            slots1[place.slot((dx, dy, 1)), TAIL] = up
            slots1[place.slot((dx, dy, -1)), TAIL] = down
    for ref, (dx, dy) in zip(edges, edge_steps(merge_y)):
        for cell, (a, b) in enumerate(EDGE1):
            x = X1 - 1 - a if dx > 0 else a
            if dy == 0:
                y = jnp.where(place.at[1] == 0, Y1 - 1 - b, b)
            else:
                y = Y1 - 1 - b if dy > 0 else b
            for vp in range(V // 2):
                ref[pl.ds(cell * (V // 2) + vp, 1)] = p1[vp, x, pl.ds(y, 1)]


def around_c1(place, CE, c1, xl, xh, yl, yh, slots, V, X):
    X1, Y1, Z = c1.shape
    half, n = Z // 2, X1 * Y1
    sub, lane = iota((8, Z), 0), iota((8, Z), 1)
    zero = jnp.zeros((8, Z), jnp.float32)
    body = lane < half
    for i in range(1, 2 * H + X1 - 1):
        CE[i, Y1 : 2 * Y1] = zero
    for x in range(X1):
        CE[H + x, 0:Y1] = c1[x]
        for b in range(2):
            k = 2 * x + b
            hi, lo = yh[V * (X // 2), pl.ds(k, 1)], yl[V * (X // 2), pl.ds(k, 1)]
            CE[H + x, pl.ds(Y1 + b, 1)] = keep(place.hi(1), hi)
            CE[H + x, pl.ds(2 * Y1 - 1 - b, 1)] = keep(place.lo(1), lo)
    for ref, ok, near, far in ((xl, place.lo(0), H - 1, H - 2), (xh, place.hi(0), H + X1, H + X1 + 1)):
        tile = keep(ok, ref[V * H, 0:Y1])
        CE[near, 0:Y1] = jnp.where(body, tile, zero)
        CE[far, 0:Y1] = jnp.where(body, roll(tile, half, 1), zero)
    for dx in (-1, 1):
        for dy in (-1, 1):
            d = (dx, dy, 0)
            line = keep(place.has(d), slots[place.slot(d), 2, pl.ds(H, 1)])
            CE[H + X1 if dx > 0 else H - 1, pl.ds(Y1 if dy > 0 else 2 * Y1 - 1, 1)] = line
    rows = []
    steps = ((0, 0), (-1, 0), (1, 0), (0, -1), (0, 1))
    wanted = [range(X1), (X1 - 1,), (0,), range(X1), range(X1)]
    for (dx, dy), xs in zip(steps, wanted):
        pair = []
        for dz in (-1, 1):
            d = (dx, dy, dz)
            pair.append(keep(place.has(d), slots[place.slot(d), 2, pl.ds(H, 1)]))
        for x in xs:
            own = lane % n == x * Y1 + sub
            rows.append(jnp.concatenate([jnp.where(own, line, zero) for line in pair], axis=1))
    li, lo = iota((2 * Z, Z), 0), iota((2 * Z, Z), 1)
    l = li % Z
    target = jnp.where(li < Z, Z - 1 - l // n, half + l // n)
    d = dot(jnp.concatenate(rows, axis=0), onehot((lo == target) & (l < 2 * n)))
    d = [d[8 * m : 8 * m + 8] for m in range(len(rows))]
    CE[H - 1, 0:Y1] = CE[H - 1, 0:Y1] + d[X1]
    CE[H + X1, 0:Y1] = CE[H + X1, 0:Y1] + d[X1 + 1]
    for x in range(X1):
        CE[H + x, 0:Y1] = CE[H + x, 0:Y1] + d[x]
        edge = jnp.where(sub == 7, d[X1 + 2 + x], jnp.where(sub == 0, d[2 * X1 + 2 + x], zero))
        CE[H + x, Y1 : 2 * Y1] = CE[H + x, Y1 : 2 * Y1] + edge


def contributions(place, U, gram_row, CE, GL, VL, Q, V):
    X1, R1, Z = CE.shape[0] - 2 * H, CE.shape[1], CE.shape[2]
    Y1, half = R1 // 2, Z // 2
    zero = jnp.zeros((R1, Z), jnp.float32)
    n = X1 * Y1
    for v in range(V):
        for i in range(2 * H + X1):
            if H <= i < H + X1:
                k = v * n + (i - H) * Y1
                GL[v, i, 0:Y1] = U[k : k + Y1]
                GL[v, i, Y1:R1] = zero[0:Y1]
            else:
                GL[v, i] = zero
        for i in (0, 1, 2 * H + X1 - 2, 2 * H + X1 - 1):
            VL[v, i] = zero
    mask = coarse_masks(place, R1, Z)
    for i in range(H - 1, H + X1 + 1):
        m = scaled(x_flag(place, i, X1), mask)
        for v in range(V):
            get = lambda j: GL[v, j]
            VL[v, i] = m * (PRE_G * GL[v, i] + PRE_N * level1_sum(get, i))
    block = {1: 0, 2: 1, 3: 2 * V, 0: 2 * V + 1}
    for w in range(X1 // 2 + 2):
        for v in range(V):
            total = None
            for i in (H - 2 + 2 * w, H - 1 + 2 * w):
                get = lambda j: VL[v, j]
                part = CE[i] * (6.0 * (GL[v, i] - VL[v, i]) + level1_sum(get, i))
                total = part if total is None else total + part
            Q[pl.ds((block[w] + 2 * v) * R1, R1)] = total
    li, lo = iota((Z, Z), 0), iota((Z, Z), 1)
    width, m = half // 2, 4 * V
    stack = []
    for j in range(-1, Y1 // 2 + 1):
        r = (2 * j) % R1
        stack.append(Q[pl.ds(r, m, stride=R1)] + Q[pl.ds(r + 1, m, stride=R1)])
    to = jnp.where(li < half, li // 2, jnp.where(li < half + 2, width + 1, width))
    used = (li < half + 2) | (li >= Z - 2)
    small = dot(jnp.concatenate(stack, axis=0), onehot((lo == to) & used, 0.25 * 0.125))
    lane_m = iota((m, Z), 1)
    body, rims = jnp.zeros((m, Z), jnp.float32), jnp.zeros((m, Z), jnp.float32)
    for j in range(-1, Y1 // 2 + 1):
        piece = small[(j + 1) * m : (j + 2) * m]
        if 0 <= j < Y1 // 2:
            body = jnp.where(lane_m // width == j, roll(piece, j * width, 1), body)
        else:
            chunk = 0 if j < 0 else 1
            rims = jnp.where(lane_m // width == chunk, roll(piece, chunk * width, 1), rims)
        at = 2 * width + j + 1
        rims = jnp.where(lane_m == at, roll(piece, at - width, 1), rims)
        rims = jnp.where(lane_m == at + 8, roll(piece, at + 7 - width, 1), rims)
    lane4 = iota((4, Z), 1)
    pairs = []
    for p in range(V // 2):
        r, q = 4 * p, 2 * V + 4 * p
        own, rim = body[r : r + 4], rims[r : r + 4]
        beside, beside_rim = body[q : q + 4], rims[q : q + 4]
        edges = jnp.where(lane4 < half, rim, roll(beside_rim, half, 1))
        ends = jnp.where(lane4 < half, gram_row, jnp.where(lane4 < half + 16, rim, roll(beside_rim, 16, 1)))
        pairs.append((own, edges, beside, ends))
    return pairs


def coarse_masks(place, R, Z):
    half = Z // 2
    row, lane = iota((R, Z), 0), iota((R, Z), 1)
    y = R // 2
    mask = onehot(row < y) + onehot((row >= y) & (row < y + H)) * f32(place.hi(1))
    mask = mask + onehot(row >= R - H) * f32(place.lo(1))
    lanes = onehot(lane < half) + onehot((lane >= half) & (lane < half + H)) * f32(place.hi(2))
    lanes = lanes + onehot(lane >= Z - H) * f32(place.lo(2))
    return mask * lanes


def level1_sum(get, i):
    cur = get(i)
    return spread(cur, get(i - 1), get(i + 1), roll(cur, 1, 1), roll(cur, -1, 1))


def third_kernel(counts, merge_y, p1, xl, xh, yl, yh, slots, *refs):
    edges, (G1, S1) = refs[:-2], refs[-2:]
    VP, X, Y, Z = p1.shape
    V, R, half = 2 * VP, 2 * Y, Z // 2
    place = Place(counts)
    row, lane = iota((Y, Z), 0), iota((Y, Z), 1)
    zero = jnp.zeros((Y, Z), jnp.float32)

    def unpack(tile, v):
        return jnp.where(lane < half, roll(tile, half, 1) if v % 2 else tile, zero)

    r8, l8 = iota((8, Z), 0), iota((8, Z), 1)
    target = jnp.where(r8 < 4, Z - H, half) + r8 % 4
    place_lanes = onehot((l8 == target) & (r8 % 4 < H))

    def layers(dx, dy):
        below, above = (dx, dy, -1), (dx, dy, 1)
        low = keep(place.has(below), slots[place.slot(below), TAIL])
        high = keep(place.has(above), slots[place.slot(above), TAIL])
        return dot(jnp.concatenate([low, high], axis=0), place_lanes, TN)

    mid, up, down = layers(0, 0), layers(0, 1), layers(0, -1)
    m_hi = jnp.logical_and(row < H, place.hi(1))
    m_lo = jnp.logical_and(row >= Y - H, place.lo(1))

    def tile_of(d, v, x):
        k = (v * X + x) * Y
        return d[k : k + Y]

    for v in range(V):
        for x in range(X):
            G1[v, H + x, 0:Y] = unpack(p1[v // 2, x], v) + tile_of(mid, v, x)
            hi = unpack(yh[v // 2, x], v) + tile_of(up, v, x)
            lo = unpack(yl[v // 2, x], v) + tile_of(down, v, x)
            G1[v, H + x, Y:R] = jnp.where(m_hi, hi, jnp.where(m_lo, lo, zero))
    for dx in (-1, 1):
        side, up, down = layers(dx, 0), layers(dx, 1), layers(dx, -1)
        src = xh if dx > 0 else xl
        ok = place.hi(0) if dx > 0 else place.lo(0)
        for v in range(V):
            for a in range(H):
                x = a if dx > 0 else X - 1 - a
                i = H + X + a if dx > 0 else H - 1 - a
                G1[v, i, 0:Y] = keep(ok, unpack(src[v // 2, x], v) + tile_of(side, v, x))
                tile = zero
                if a < 2:
                    tile = jnp.where(m_hi, tile_of(up, v, x), jnp.where(m_lo, tile_of(down, v, x), zero))
                G1[v, i, Y:R] = tile
    for ref, (sx, sy) in zip(edges, edge_steps(merge_y)):
        dx = -sx
        for dy in (-1, 1) if sy == 0 else (-sy,):
            ok = place.has((dx, dy, 0))
            for cell, (a, b) in enumerate(EDGE1):
                i = H + X + a if dx > 0 else H - 1 - a
                r = Y + b if dy > 0 else R - 1 - b
                for v in range(V):
                    line = ref[pl.ds(cell * VP + v // 2, 1)]
                    line = roll(line, half, 1) if v % 2 else line
                    use = jnp.logical_and(lane[0:1] < half, ok)
                    line = jnp.where(use, line, jnp.zeros((1, Z), jnp.float32))
                    G1[v, i, pl.ds(r, 1)] = G1[v, i, pl.ds(r, 1)] + line
    mask = coarse_masks(place, R, Z)
    for i in range(1, 2 * H + X - 1):
        m = scaled(x_flag(place, i, X), mask)
        for v in range(V):
            get = lambda j: G1[v, j]
            S1[v, i] = m * (PRE_G * G1[v, i] + PRE_N * level1_sum(get, i))


def grid_of(count_y, count_x, fn):
    return [[fn(y, x) for x in range(count_x)] for y in range(count_y)]


def assemble(counts, parts_y, tile, lane):
    nx, ny, nz = counts
    width = lane.shape[1] // parts_y

    def one(y, x):
        y, j = y // parts_y, y % parts_y
        acc = roll(tile[(x * ny + y) * nz], -width * j, 1)
        for z in range(1, nz):
            acc = jnp.where(lane // width == z, roll(tile[(x * ny + y) * nz + z], width * (z - j), 1), acc)
        return acc

    return grid_of(ny * parts_y, nx, one)


def gather_parts(counts, parts_y, slots, lane, odd):
    nx, ny, nz = counts
    width = lane.shape[1] // parts_y

    def tile(x, y, z, k):
        t = (x * ny + y) * nz + z
        return jnp.concatenate([slots[t, k], slots[t, k]], axis=0)

    def joined(own, beside, x, y, z):
        zero = jnp.zeros(lane.shape, jnp.float32)
        before = beside[x - 1, y, z] if x else zero
        after = beside[x + 1, y, z] if x < nx - 1 else zero
        return own[x, y, z] + jnp.where(odd, after, before)

    half = lane.shape[1] // 2
    every = [(x, y, z) for x in range(nx) for y in range(ny) for z in range(nz)]
    edges, ends = {p: tile(*p, 1) for p in every}, {p: tile(*p, 3) for p in every}
    own = {p: tile(*p, 0) for p in every}
    beside = {p: tile(*p, 2) for p in every}
    own_rim = {p: jnp.where(lane < half, edges[p], ends[p]) for p in every}
    beside_rim = {p: jnp.where(lane < half, roll(edges[p], half, 1), roll(ends[p], -16, 1)) for p in every}
    main = {p: joined(own, beside, *p) for p in every}
    rim = {p: joined(own_rim, beside_rim, *p) for p in every}

    def one(yy, x):
        y, j = yy // parts_y, yy % parts_y
        sources = [(main, y, j, j)]
        if j == 0 and y:
            sources.append((rim, y - 1, 1, parts_y))
        if j == parts_y - 1 and y < ny - 1:
            sources.append((rim, y + 1, 0, -1))
        total = None
        for grid, from_y, chunk, inner in sources:
            acc = roll(grid[x, from_y, 0], -width * chunk, 1)
            for z in range(1, nz):
                acc = jnp.where(lane // width == z, roll(grid[x, from_y, z], width * (z - chunk), 1), acc)
            for z in range(nz):
                at = 2 * width + inner + 1
                if z:
                    to = width * z - 1
                    acc = acc + jnp.where(lane == to, roll(rim[x, from_y, z], to - at, 1), jnp.zeros_like(acc))
                if z < nz - 1:
                    to = width * (z + 1)
                    acc = acc + jnp.where(lane == to, roll(rim[x, from_y, z], to - at - 8, 1), jnp.zeros_like(acc))
            total = acc if total is None else total + acc
        return total

    return grid_of(ny * parts_y, nx, one)


def combine(fn, *grids):
    return [[fn(*ts) for ts in zip(*lines)] for lines in zip(*grids)]


def add(*terms):
    total = None
    for term in terms:
        if term is not None:
            total = term if total is None else total + term
    return total


def shrink_tiles(v, level, odd, lane):
    step = 2 ** (level - 2)
    v = [[a + b for a, b in zip(v[2 * y], v[2 * y + 1])] for y in range(len(v) // 2)]
    if level == 2:
        v = combine(lambda t: t + jnp.where(odd, roll(t, 1, 0), roll(t, -1, 0)), v)
    else:
        v = [[line[2 * x] + line[2 * x + 1] for x in range(len(line) // 2)] for line in v]
    upper = (lane // step) % 2 == 1
    return combine(lambda t: 0.125 * (t + jnp.where(upper, roll(t, step, 1), roll(t, -step, 1))), v)


def weights_kernel(counts, parts_y, c2s, *outs):
    lane = iota((8, outs[0].shape[-1]), 1)
    odd = iota(lane.shape, 0) % 2 == 1
    count = counts[0] * counts[1] * counts[2]
    rows = [jnp.where(odd, c2s[t, pl.ds(1, 1)], c2s[t, pl.ds(0, 1)]) for t in range(count)]
    c = assemble(counts, parts_y, rows, lane)
    for level in range(2, LEVELS):
        for y in range(len(c)):
            for x in range(len(c[0])):
                outs[level - 2][y, x] = (0.25**level) * c[y][x]
        if level < LEVELS - 1:
            c = shrink_tiles(c, level, odd, lane)


def coarse_kernel(counts, parts_y, slots1, *refs):
    *weights, mine, other, W, pre = refs
    nx, ny, nz = counts
    Z = slots1.shape[3]
    place = Place(counts)
    width = Z // parts_y
    lane = iota((8, Z), 1)
    odd = iota((8, Z), 0) % 2 == 1
    zero = jnp.zeros((8, Z), jnp.float32)
    scale = {2 + i: ref for i, ref in enumerate(weights)}
    inverse = {}
    for level, ref in scale.items():
        inverse[level] = grid_of(ref.shape[0], ref.shape[1], lambda y, x: 1.0 / (6.0 * ref[y, x]))

    def at(v, y, x):
        inside = 0 <= y < len(v) and 0 <= x < len(v[0])
        return v[y][x] if inside else None

    def neighbours(v, level):
        step = 2 ** (level - 2)
        ahead = [[roll(t, -1, 0) for t in line] for line in v] if level == 2 else None
        back = [[roll(t, 1, 0) for t in line] for line in v] if level == 2 else None

        def one(y, x):
            t = v[y][x]
            zs = jnp.where(lane < step, zero, roll(t, step, 1)) + jnp.where(lane >= Z - step, zero, roll(t, -step, 1))
            ys = add(zs, at(v, y - 1, x), at(v, y + 1, x))
            if level > 2:
                return add(ys, at(v, y, x - 1), at(v, y, x + 1))
            return ys + jnp.where(
                odd, add(back[y][x], at(back, y, x + 1)), add(ahead[y][x], at(ahead, y, x - 1))
            )

        return grid_of(len(v), len(v[0]), one)

    def grow(v, level):
        v = [line for line in v for _ in range(2)]
        return v if level == 2 else [[t for t in line for _ in range(2)] for line in v]

    def sweep(v, g, level):
        return combine(lambda a, b, s: KEEP * a + OMEGA * b + SIXTH * s, v, g, neighbours(v, level))

    def cycle(g, level):
        if level == LEVELS - 1:
            v = combine(lambda b: OMEGA * b, g)
            for _ in range(COARSE_SWEEPS - 1):
                v = sweep(v, g, level)
            return v
        v = combine(lambda b, s: PRE_G * b + PRE_N * s, g, neighbours(g, level))
        c = grid_of(len(g), len(g[0]), lambda y, x: scale[level][y, x])
        r = combine(lambda c, b, a, s: c * (6.0 * (b - a) + s), c, g, v, neighbours(v, level))
        down = shrink_tiles(r, level, odd, lane)
        down = grid_of(len(down), len(down[0]), lambda y, x: down[y][x] * inverse[level + 1][y][x])
        v = combine(lambda a, b: a + b, v, grow(cycle(down, level + 1), level))
        return sweep(v, g, level)

    b2 = gather_parts(counts, parts_y, slots1, lane, odd)
    v = cycle(grid_of(len(b2), nx, lambda y, x: b2[y][x] * inverse[2][y][x]), 2)
    for y in range(len(v)):
        for x in range(nx):
            W[y, x] = v[y][x]
    pre[...] = jnp.zeros_like(pre)
    ix, iy, iz = place.at
    for side, dev in enumerate((ix, ix + 1 - 2 * (ix % 2))):
        for xw in range(4):
            x = dev + (xw + 1) // 2 - 1
            x_ok = jnp.logical_and(x >= 0, x < nx)
            x = jnp.clip(x, 0, nx - 1)
            for j in range(-1, parts_y + 1):
                y = iy * parts_y + j
                ok = jnp.logical_and(x_ok, jnp.logical_and(y >= 0, y < ny * parts_y))
                y = jnp.clip(y, 0, ny * parts_y - 1)
                for vec in range(2):
                    line = W[y, x, pl.ds(vec * 2 + (xw + 1) % 2, 1)]
                    pre[2 * side + vec, xw, pl.ds(j % 8, 1)] = keep(ok, line)
    li, lo = iota((Z, Z), 0), iota((Z, Z), 1)
    z1 = jnp.where(lo < 96, lo, lo - Z)
    window = onehot(li == iz * width + jnp.floor_divide(z1 + 2, 2) - 1)
    moved = dot(pre[...].reshape(4 * 4 * 8, Z), window).reshape(4, 4, 8, Z)
    mine[...] = moved[0:2]
    other[...] = moved[2:4]


def last_kernel(counts, mine, other, G1, S1, G, S, c, pre_hbm, op_hbm, E1, C1, E0, C0, pre, op, sems):
    V, X1, Y1, Z = S1.shape[0], S1.shape[1] - 2 * H, S1.shape[2] // 2, S1.shape[3]
    X, Y = 2 * X1, 2 * Y1
    R1, R = 2 * Y1, Y + 8
    place = Place(counts)
    for v in range(V):
        for x in range(X1):
            k = (v * X1 + x) * R1
            held = place.at[0] % 2 == v // 2
            tile = jnp.where(held, mine[v % 2, x], other[v % 2, x])
            E1[pl.ds(k, 8, stride=2)] = tile
            E1[pl.ds(k + 1, 8, stride=2)] = tile
    for v in range(V):
        for i in range(1, 2 * H + X1 - 1):
            C1[v, i] = S1[v, i] + E1[pl.ds((v * X1 + (i - 1) // 2) * R1, R1)]
    mask = coarse_masks(place, R1, Z)
    n = X1 + 2
    fine = []
    for v in range(V):
        tiles = []
        for i in range(H - 1, H + X1 + 1):
            m = scaled(x_flag(place, i, X1), mask)
            get = lambda j: C1[v, j]
            tiles.append(m * (KEEP * C1[v, i] + OMEGA * G1[v, i] + SIXTH * level1_sum(get, i)))
        fine.append(jnp.concatenate(tiles, axis=0))
    li, lo = iota((Z, Z), 0), iota((Z, Z), 1)
    double = onehot(li == lo // 2)
    half = Z // 2
    k = lo % 16
    source = jnp.where(k < H, Z - 1, jnp.where(k < 6, 0, jnp.where(k < 8, half - 1, half)))
    rim = None
    for v in range(V):
        part = dot(fine[v], onehot((li == source) & (lo // 16 == v)))
        rim = part if rim is None else rim + part
    sub = iota((8, Z), 0)
    zero8 = jnp.zeros((8, Z), jnp.float32)
    for v in range(V + 1):
        wide = dot(fine[v], double) if v < V else rim
        for i in range(n):
            base = (v * n + i) * R
            tile = wide[i * R1 : i * R1 + Y1]
            edge = wide[i * R1 + Y1 : (i + 1) * R1]
            E0[pl.ds(base, 8, stride=2)] = tile
            E0[pl.ds(base + 1, 8, stride=2)] = tile
            E0[pl.ds(base + Y, 8)] = jnp.where(sub < 2, edge[0:1], jnp.where(sub >= 6, edge[7:8], zero8))
    for v in range(V + 1):
        for i in range(1, 2 * H + X - 1):
            C0[v, i] = S[v, i] + E0[pl.ds((v * n + (i - 1) // 2) * R, R)]
    ym, zm = fine_masks(place, Y, Z)
    lane = iota((R, Z), 1)
    for i in range(H - 1, H + X + 1):
        flag = x_flag(place, i, X)
        for v in range(V + 1):
            m = scaled(flag, ym if v < V else zm)
            value = m * (KEEP * C0[v, i] + OMEGA * G[v, i] + SIXTH * fine_sum(C0, v, i, V, lane))
            E0[pl.ds((v * (X + 2) + i - H + 1) * R, R)] = value
            if v < V and H <= i < H + X:
                pre[v, i - H] = value[0:Y]
    copies = [pltpu.make_async_copy(pre, pre_hbm, sems.at[0])]
    copies[0].start()

    class View:
        def __getitem__(self, key):
            v, i = key
            return E0[pl.ds((v * (X + 2) + i - H + 1) * R, R)]

    view = View()
    for x in range(X):
        for v in range(V):
            around = fine_sum(view, v, H + x, V, lane)
            op[v, x] = c[x] * (6.0 * view[v, H + x][0:Y] - around[0:Y])
        if x % 2:
            part = slice(x - 1, x + 1)
            copies.append(pltpu.make_async_copy(op.at[:, part], op_hbm.at[:, part], sems.at[1 + x // 2]))
            copies[-1].start()
    for copy in copies:
        copy.wait()


def gram_kernel(old, prev, out):
    M, X, Y, Z = old.shape
    J = prev.shape[0]
    pairs = [(a, b) for a in range(M + J) for b in range(a, M + J)]
    sums = [None] * len(pairs)
    for x in range(X):
        for y in range(0, Y, 8):
            tiles = [old[m, x, y : y + 8] for m in range(M)] + [prev[j, x, y : y + 8] for j in range(J)]
            for p, (a, b) in enumerate(pairs):
                term = tiles[a] * tiles[b]
                sums[p] = term if sums[p] is None else sums[p] + term
    ones = jnp.ones((8, Z), jnp.float32)
    lane = iota((8, Z), 1)
    rows = jnp.concatenate([jnp.sum(s, axis=0, keepdims=True) for s in sums], axis=0)
    pad = jnp.zeros((Z - len(pairs), Z), jnp.float32)
    out[...] = dot(ones, jnp.concatenate([rows, pad], axis=0), NT)


def ortho_kernel(count, cells, old, prev, slots, orth, proj, tri):
    M, X, Y, Z = old.shape
    J = prev.shape[0]
    if count <= 64:
        total = slots[0, TAIL - 1, pl.ds(0, 1)]
        for t in range(1, count):
            total = total + slots[t, TAIL - 1, pl.ds(0, 1)]
    else:
        total = lax.fori_loop(0, count, lambda t, s: s + slots[t, TAIL - 1, pl.ds(0, 1)], jnp.zeros((1, Z), jnp.float32))
    total = jnp.broadcast_to(total, (8, Z)) / cells
    value = {}
    p = 0
    for a in range(M + J):
        for b in range(a, M + J):
            one = jnp.broadcast_to(total[:, p : p + 1], (8, Z))
            value[a, b] = value[b, a] = one
            p += 1
    P_ = [[value[m, M + j] for j in range(J)] for m in range(M)]
    gram = {}
    for i in range(J):
        for j in range(i + 1):
            s = value[M + i, M + j]
            for m in range(M):
                inner = None
                for k in range(M):
                    term = value[m, k] * P_[k][j]
                    inner = term if inner is None else inner + term
                s = s - P_[m][i] * (P_[m][j] - inner) - P_[m][j] * P_[m][i]
            gram[i, j] = s
    L = {}
    for i in range(J):
        for j in range(i + 1):
            s = gram[i, j]
            for k in range(j):
                s = s - L[i, k] * L[j, k]
            L[i, j] = jnp.sqrt(s) if i == j else s / L[j, j]
    inv = {}
    for i in range(J):
        for j in range(i + 1):
            s = jnp.ones((8, Z), jnp.float32) if i == j else None
            for k in range(j, i):
                term = L[i, k] * inv[k, j]
                s = -term if s is None else s - term
            inv[i, j] = s / L[i, i]
    row, col = iota((M, J), 0), iota((M, J), 1)
    proj_v, tri_v = jnp.zeros((M, J), jnp.float32), jnp.zeros((J, J), jnp.float32)
    for m in range(M):
        for j in range(J):
            here = (row == m) & (col == j)
            proj_v = jnp.where(here, P_[m][j][0:M, 0:J], proj_v)
            if j >= m:
                tri_v = jnp.where(here, L[j, m][0:J, 0:J], tri_v)
    proj[...] = proj_v
    tri[...] = tri_v
    mix = {}
    for j in range(J):
        for m in range(M):
            s = None
            for i in range(j + 1):
                term = inv[j, i] * P_[m][i]
                s = term if s is None else s + term
            mix[j, m] = s
    for x in range(X):
        for y in range(0, Y, 8):
            olds = [old[m, x, y : y + 8] for m in range(M)]
            rem = []
            for i in range(J):
                r = prev[i, x, y : y + 8]
                for m in range(M):
                    r = r - P_[m][i] * olds[m]
                rem.append(r)
            for j in range(J):
                s = None
                for i in range(j + 1):
                    term = inv[j, i] * rem[i]
                    s = term if s is None else s + term
                orth[j, x, y : y + 8] = s


def run(near, kernel, shapes, args, scratch=(), name=None, result=(), plain=(), sems=0, out_sems=0):
    outs = []
    for i, shape in enumerate(shapes):
        kind = jax.ShapeDtypeStruct if i in result or not near else pltpu.VMEM
        outs.append(kind(shape, jnp.float32))
    if near:
        spaces = [pltpu.HBM if sems else None if i in plain else pltpu.VMEM for i in range(len(args))]
        args = [pltpu.with_memory_space_constraint(a, m) if m else a for a, m in zip(args, spaces)]
    fn = pl.pallas_call(
        kernel,
        out_shape=outs,
        in_specs=[HB if sems else VM] * len(args),
        out_specs=[HB if out_sems and i in result else VM for i in range(len(shapes))],
        scratch_shapes=[pltpu.VMEM(s, jnp.float32) for s in scratch] + [pltpu.SemaphoreType.DMA((sems + out_sems,))] * (sems + out_sems > 0),
        compiler_params=pltpu.CompilerParams(vmem_limit_bytes=16 * 2**20) if near else None,
        name=name,
    )
    return fn(*args)


def shift(value, axis, step):
    n = lax.axis_size(axis)
    return lax.ppermute(value, axis, [(i, (i + step) % n) for i in range(n)])


def diagonal(counts, value, dx, dy):
    nx, ny = counts[:2]
    step = dy if dy else 1
    pairs = [(x * ny + y, (x + dx) % nx * ny + (y + step) % ny) for x in range(nx) for y in range(ny)]
    return lax.ppermute(value, ("gx", "gy"), pairs)


def swap(slots):
    return lax.all_to_all(slots, AXES, split_axis=0, concat_axis=0, tiled=True)


def wide_coarse(counts, parts_y, c2s, slots1):
    nx, ny, nz = counts
    Z = slots1.shape[3]
    width = Z // parts_y
    lead, half = 2, Z // 2

    def across_x(own, beside):
        own, beside = (
            t.reshape(nx, ny, nz, lead, 2, Z).transpose(3, 4, 0, 1, 2, 5) for t in (own, beside)
        )
        pad = ((0, 0), (1, 1), (0, 0), (0, 0), (0, 0))
        first = own[:, 0] + jnp.pad(beside[:, 0], pad)[:, 0:nx]
        last = own[:, 1] + jnp.pad(beside[:, 1], pad)[:, 2:]
        return jnp.stack([first, last], axis=2).reshape(lead, 2 * nx, ny, nz, Z)

    edges, ends = slots1[:, 1], slots1[:, 3]
    low = iota((1, 1, Z), 2) < half
    main = across_x(slots1[:, 0], slots1[:, 2])
    rim = across_x(
        jnp.where(low, edges, ends), jnp.where(low, jnp.roll(edges, half, 2), jnp.roll(ends, -16, 2))
    )

    def with_z(line, low, high):
        pad = ((0, 0), (0, 0), (0, 0), (1, 1))
        first = jnp.pad(high, pad)[..., 0:nz]
        last = jnp.pad(low, pad)[..., 2:]
        lanes = iota((1, width), 1)[0]
        line = line + jnp.where(lanes == 0, first[..., None], 0.0) + jnp.where(lanes == width - 1, last[..., None], 0.0)
        return line.reshape(lead, 2 * nx, ny, nz * width)

    lines = []
    for j in range(-1, parts_y + 1):
        source, start = (rim, 0) if j < 0 else (rim, width) if j == parts_y else (main, j * width)
        at = 2 * width + j + 1
        lines.append(with_z(source[..., start : start + width], rim[..., at], rim[..., at + 8]))
    pad = ((0, 0), (0, 0), (1, 1), (0, 0))
    lines[1] = lines[1] + jnp.pad(lines[-1], pad)[:, :, 0:ny]
    lines[parts_y] = lines[parts_y] + jnp.pad(lines[0], pad)[:, :, 2:]
    b2 = jnp.stack(lines[1:-1], axis=3).reshape(lead, 2 * nx, ny * parts_y, nz * width)

    def whole(t, lead):
        t = t.reshape(nx, ny, nz, lead * 2, Z)
        parts = []
        for j in range(parts_y):
            part = t[..., j * width : (j + 1) * width].transpose(3, 0, 1, 2, 4)
            parts.append(part.reshape(lead * 2, nx, ny, nz * width))
        t = jnp.stack(parts, axis=3).reshape(lead, 2, nx, ny * parts_y, nz * width)
        return t.transpose(0, 2, 1, 3, 4).reshape(lead, nx * 2, ny * parts_y, nz * width)

    c2 = whole(c2s[:, 0:2], 1)
    g2 = b2 / (6.0 * 0.0625 * c2)

    def around(v):
        p = jnp.pad(v, ((0, 0), (1, 1), (1, 1), (1, 1)))
        m = slice(1, -1)
        return (
            p[:, 2:, m, m] + p[:, :-2, m, m] + p[:, m, 2:, m] + p[:, m, :-2, m] + p[:, m, m, 2:] + p[:, m, m, :-2]
        )

    def pairs(e):
        return onehot(iota((e, 2 * e), 0) == iota((e, 2 * e), 1) // 2)

    def shrink(v):
        d, a, b, e = v.shape
        v = v.reshape(d, a // 2, 2, b, e).sum(axis=2)
        v = v[:, :, 0::2] + v[:, :, 1::2]
        return dot(v.reshape(-1, e), pairs(e // 2).T * 0.125).reshape(d, a // 2, b // 2, e // 2)

    def grow(v):
        d, a, b, e = v.shape
        v = dot(v.reshape(-1, e), pairs(e)).reshape(d, a, b, 2 * e)
        return jnp.repeat(jnp.repeat(v, 2, axis=1), 2, axis=2)

    def cycle(g, c, level):
        if level == LEVELS - 1:
            v = OMEGA * g
            for _ in range(COARSE_SWEEPS - 1):
                v = KEEP * v + OMEGA * g + SIXTH * around(v)
            return v
        v = PRE_G * g + PRE_N * around(g)
        r = 0.25**level * c * (6.0 * (g - v) + around(v))
        down = shrink(c)
        v = v + grow(cycle(shrink(r) / (6.0 * 0.25 ** (level + 1) * down), down, level + 1))
        return KEEP * v + OMEGA * g + SIXTH * around(v)

    e = jnp.pad(cycle(g2, c2, 2), ((0, 0), (1, 1), (1, 1), (1, 1)))
    ix, iy, iz = (lax.axis_index(a) for a in AXES)

    def window(x):
        w = lax.dynamic_slice(
            e, (jnp.int32(0), x * 2, iy * parts_y, iz * width), (lead, 4, parts_y + 2, width + 2)
        )
        w = jnp.repeat(w, 2, axis=3)
        gap = jnp.zeros(w.shape[:3] + (Z - 2 * width - 4,), w.dtype)
        w = jnp.concatenate([w[..., 2:], gap, w[..., :2]], axis=3)
        pad = jnp.zeros((lead, 4, 8 - parts_y - 2, Z), w.dtype)
        return jnp.concatenate([w[:, :, 1:], pad, w[:, :, :1]], axis=2)

    return window(ix), window(ix + 1 - 2 * (ix % 2))


def per_device(counts, old, prev, inc, c):
    V, X, Y, Z = inc.shape
    count = counts[0] * counts[1] * counts[2]
    merge_y = counts[1] == 2
    near = count <= 64
    R = Y + 8
    X1, Y1 = X // 2, Y // 2
    y_shape, x_shape = (V * (X // 2) + 1, 8, Z), (V * H + 1, Y, Z)
    shapes = [(V, X, Y, Z), x_shape, x_shape, y_shape]
    shapes += [] if merge_y else [y_shape]
    shapes += [(count, V, H + 1, Z), (X1, Y1, Z)]
    outs = run(
        near,
        functools.partial(first_kernel, counts, merge_y),
        shapes,
        (inc, c),
        [inc.shape, c.shape, (X1 * Y, Z)],
        name="first",
        result=(len(shapes) - 2,),
        sems=V + 1,
    )
    g, xlo, xhi = outs[:3]
    c1 = outs[-1]
    slots0 = swap(outs[-2])
    xl, xh = shift(xhi, "gx", 1), shift(xlo, "gx", -1)
    if merge_y:
        yl = yh = shift(outs[3], "gy", 1)
    else:
        yl, yh = shift(outs[4], "gy", 1), shift(outs[3], "gy", -1)
    (gram,) = run(near, gram_kernel, [(8, Z)], (old, prev), name="gram", plain=(0, 1))
    ext0, ext1 = (V + 1, X + 2 * H, R, Z), (V, X1 + 2 * H, 2 * Y1, Z)
    steps = edge_steps(merge_y)
    G, S, p1, slots1, c2s, *edges = run(
        near,
        functools.partial(second_kernel, counts, merge_y),
        [ext0, ext0, (V // 2, X1, Y1, Z), (count, TAIL + 1, V, Z), (count, V, Z)] + [(16, Z)] * len(steps),
        (g, c, c1, xl, xh, yl, yh, slots0, gram),
        [(V * X1 * Y, Z), ext1[1:], ext1, ext1],
        name="second",
        result=(3,),
    )
    slots1 = swap(slots1)
    edges = [diagonal(counts, e, dx, dy) for e, (dx, dy) in zip(edges, steps)]
    xl, xh = shift(p1, "gx", 1), shift(p1, "gx", -1)
    if merge_y:
        yl = yh = shift(p1, "gy", 1)
    else:
        yl, yh = shift(p1, "gy", 1), shift(p1, "gy", -1)
    slots1, xl, xh, yl, yh, *edges = lax.optimization_barrier((slots1, xl, xh, yl, yh, *edges))
    G1, S1 = run(
        near,
        functools.partial(third_kernel, counts, merge_y),
        [ext1, ext1],
        (p1, xl, xh, yl, yh, slots1, *edges),
        name="third",
    )
    orth, proj, tri = run(
        near,
        functools.partial(ortho_kernel, count, float(count * X * Y * Z)),
        [(V, X, Y, Z), (4, 4), (4, 4)],
        (old, prev, slots1),
        name="ortho",
        result=(0, 1, 2),
        plain=(0, 1),
    )
    parts_y = Y // 4
    if near and counts[2] * (Z // parts_y) == Z:
        sizes = [(counts[1] * parts_y, counts[0], 8, Z)]
        for level in range(3, LEVELS):
            y, x = sizes[-1][:2]
            sizes.append((y // 2, x if level == 3 else x // 2, 8, Z))
        weights = run(
            near, functools.partial(weights_kernel, counts, parts_y), sizes, (c2s,), name="weights"
        )
        e2, others = run(
            near,
            functools.partial(coarse_kernel, counts, parts_y),
            [(V // 2, 4, 8, Z)] * 2,
            (slots1, *weights),
            [sizes[0], (V, 4, 8, Z)],
            name="coarse",
        )
    else:
        e2, others = wide_coarse(counts, parts_y, c2s, slots1)
    others = lax.ppermute(others, "gx", [(i, i ^ 1) for i in range(counts[0])])
    pre, op = run(
        near,
        functools.partial(last_kernel, counts),
        [(V, X, Y, Z), (V, X, Y, Z)],
        (e2, others, G1, S1, G, S, c),
        [(V * X1 * 2 * Y1, Z), ext1, ((V + 1) * (X + 2) * R, Z), ext0, (V, X, Y, Z), (V, X, Y, Z)],
        name="last",
        result=(0, 1),
        out_sems=1 + X // 2,
    )
    return orth, proj, tri, pre, op


def solution(mesh):
    block = P(None, *AXES)
    counts = tuple(mesh.shape[a] for a in AXES)
    return jax.shard_map(
        functools.partial(per_device, counts),
        mesh=mesh,
        in_specs=(block, block, block, P(*AXES)),
        out_specs=(block, P(), P(), block, block),
        check_vma=False,
    )
```

```python
import functools

import jax
import jax.numpy as jnp
from jax import lax
from jax.experimental import pallas as pl
from jax.experimental.pallas import tpu as pltpu
from jax.sharding import PartitionSpec as P

LEVELS = 6
COARSE_SWEEPS = 4
OMEGA = 0.8
KEEP = 1.0 - OMEGA
SIXTH = OMEGA / 6.0
PRE_G = OMEGA * (2.0 - OMEGA)
PRE_N = OMEGA * OMEGA / 6.0
AXES = ("gx", "gy", "gz")
HIGH = lax.Precision.HIGHEST
H = 3
NN = (((1,), (0,)), ((), ()))
NT = (((1,), (1,)), ((), ()))
TN = (((0,), (0,)), ((), ()))
VM = pl.BlockSpec(memory_space=pltpu.VMEM)
HB = pl.BlockSpec(memory_space=pltpu.HBM)
EDGE = ((0, 0), (0, 1), (1, 0))
EDGE1 = EDGE + ((1, 1), (0, 2), (2, 0))
TAIL = 4


def edge_steps(merge_y):
    return [(dx, dy) for dx in (1, -1) for dy in ((0,) if merge_y else (1, -1))]


def dot(a, b, dims=NN):
    return lax.dot_general(a, b, dims, precision=HIGH, preferred_element_type=jnp.float32)


def iota(shape, dim):
    return lax.broadcasted_iota(jnp.int32, shape, dim)


def onehot(cond, scale=1.0):
    return jnp.where(cond, jnp.float32(scale), jnp.float32(0.0))


def roll(a, shift, axis):
    size = a.shape[axis]
    shift = shift % size
    return a if shift == 0 else pltpu.roll(a, shift, axis)


class Place:
    def __init__(self, counts):
        self.counts = counts
        self.at = tuple(lax.axis_index(a) for a in AXES)
        self.me = self.linear(self.at)

    def linear(self, p):
        nx, ny, nz = self.counts
        return (p[0] * ny + p[1]) * nz + p[2]

    def lo(self, axis):
        return self.at[axis] > 0

    def hi(self, axis):
        return self.at[axis] < self.counts[axis] - 1

    def has(self, d):
        ok = None
        for axis in range(3):
            if d[axis]:
                one = self.hi(axis) if d[axis] > 0 else self.lo(axis)
                ok = one if ok is None else jnp.logical_and(ok, one)
        return ok

    def slot(self, d):
        there = self.linear(tuple(p + s for p, s in zip(self.at, d)))
        return jnp.where(self.has(d), there, self.me)


def f32(flag):
    return jnp.where(flag, jnp.float32(1.0), jnp.float32(0.0))


def keep(flag, a):
    return jnp.where(flag, a, jnp.zeros_like(a))


def fill_slots(ref, count, value, rows):
    if count <= 64:
        for t in range(count):
            ref[t, 0:rows] = value
    else:
        def body(t, carry):
            ref[t, 0:rows] = value
            return carry
        lax.fori_loop(0, count, body, 0)


def fill_tail(ref, count, k, value):
    if count <= 64:
        for t in range(count):
            ref[t, k] = value
    else:
        def body(t, carry):
            ref[t, k] = value
            return carry
        lax.fori_loop(0, count, body, 0)


def first_kernel(counts, merge_y, inc_hbm, c_hbm, *refs):
    if merge_y:
        g, xlo, xhi, ymsg, slots, c1, inc, c, QC, sems = refs
    else:
        g, xlo, xhi, ylo, yhi, slots, c1, inc, c, QC, sems = refs
    V, X, Y, Z = inc.shape
    place = Place(counts)
    copy_c = pltpu.make_async_copy(c_hbm, c, sems.at[V])
    copies = [pltpu.make_async_copy(inc_hbm.at[v], inc.at[v], sems.at[v]) for v in range(V)]
    copy_c.start()
    for copy in copies:
        copy.start()
    sub = iota((8, Z), 0)
    lane = iota((8, Z), 1)
    copy_c.wait()
    X1, Y1, half = X // 2, Y // 2, Z // 2
    for x in range(X1):
        QC[pl.ds(x * Y, Y)] = c[2 * x] + c[2 * x + 1]
    li, lo = iota((Z, Z), 0), iota((Z, Z), 1)
    n = X1 * Y1
    cc = dot(QC[pl.ds(0, n, stride=2)] + QC[pl.ds(1, n, stride=2)], onehot(lo == li // 2, 0.125))
    c1[...] = cc.reshape(X1, Y1, Z)
    stack = []
    for y in range(Y // 4):
        sums = []
        for x in range(X // 4):
            k = 2 * x * Y1 + 2 * y
            pair = cc[k : k + 2] + cc[k + Y1 : k + Y1 + 2]
            sums.append(pair[0:1] + pair[1:2])
        stack.append(jnp.where(sub % 2 == 0, sums[0], sums[1]))
    stack = dot(jnp.concatenate(stack, axis=0), onehot((lo == li // 2) & (li < half), 0.125))
    c2 = stack[0:8]
    for y in range(1, Y // 4):
        c2 = c2 + roll(stack[8 * y : 8 * y + 8], y * (half // 2), 1)
    r4, l4 = iota((4, Z), 0), iota((4, Z), 1)
    zero4 = jnp.zeros((4, Z), jnp.float32)
    base = [jnp.where(r4 == H, c2[x : x + 1], zero4) for x in range(2)] + [zero4] * (V - 2)
    for v in range(2):
        fill_tail(slots, counts[0] * counts[1] * counts[2], v, base[v])

    wide8 = lane < half
    xlo[V * H, 0:Y1] = jnp.where(wide8, c1[0], roll(c1[1], half, 1))
    xhi[V * H, 0:Y1] = jnp.where(wide8, c1[X1 - 1], roll(c1[X1 - 2], half, 1))
    ends = [(ymsg, jnp.where(place.at[1] == 0, 1, 0))] if merge_y else [(ylo, 0), (yhi, 1)]
    for ref, upper in ends:
        for x in range(X1):
            for b in range(2):
                y = jnp.where(upper == 1, Y1 - 1 - b, b)
                ref[V * (X // 2), pl.ds(2 * x + b, 1)] = c1[x, pl.ds(y, 1)]
    scale = [1.0 / (6.0 * c[x]) for x in range(X)]
    for v in range(V):
        copies[v].wait()
        for x in range(X):
            value = inc[v, x] * scale[x]
            g[v, x] = value
            if x < H:
                xlo[v * H + x] = value
            if x >= X - H:
                xhi[v * H + x - (X - H)] = value
    faces = []
    for x in range(X):
        for y in range(0, Y, 8):
            acc = jnp.zeros((8, Z), jnp.float32)
            for v in range(V):
                acc = jnp.where(lane // 8 == v, roll(g[v, x, y : y + 8], 8 * v + H, 1), acc)
            m = len(faces)
            if m < X1:
                acc = jnp.where(lane // 2 == 4 * V, roll(c1[m], 8 * V - half + 2, 1), acc)
                acc = jnp.where(lane // 2 == 4 * V + 1, roll(c1[m], 8 * V + 2, 1), acc)
            faces.append(acc)
    faces = jnp.concatenate(faces, axis=0).T
    k = 8 * V
    c_up = jnp.where(l4 < n, faces[k + 1 : k + 2], roll(faces[k : k + 8], n, 1)[0:1])
    c_down = jnp.where(l4 < n, faces[k + 2 : k + 3], roll(faces[k : k + 8], n, 1)[3:4])
    rows_up = [jnp.where(r4 < H, faces[8 * v : 8 * v + 4], base[v]) for v in range(V)]
    rows_down = [jnp.where(r4 < H, faces[8 * v + H : 8 * v + H + 4], base[v]) for v in range(V)]
    rows_up[2] = jnp.where(r4 < H, rows_up[2], jnp.where(l4 < 2 * n, c_up, zero4))
    rows_down[2] = jnp.where(r4 < H, rows_down[2], jnp.where(l4 < 2 * n, c_down, zero4))
    for dx in (-1, 0, 1):
        for dy in (-1, 0, 1):
            above, below = place.slot((dx, dy, 1)), place.slot((dx, dy, -1))
            for v in range(V):
                slots[above, v] = rows_up[v]
                slots[below, v] = rows_down[v]
            if dx and dy:
                t = place.slot((dx, dy, 0))
                for cell, (a, b) in enumerate(EDGE):
                    x = X - 1 - a if dx > 0 else a
                    y = Y - 1 - b if dy > 0 else b
                    for v in range(V):
                        slots[t, v, pl.ds(cell, 1)] = g[v, x, pl.ds(y, 1)]
                corner = c1[X1 - 1 if dx > 0 else 0, pl.ds(Y1 - 1 if dy > 0 else 0, 1)]
                slots[t, 2, pl.ds(H, 1)] = corner

    def packed(v, j, start, own):
        return jnp.where(own, g[v, 2 * j, pl.ds(start, 8)], roll(g[v, 2 * j + 1, pl.ds(start, 8)], 4, 0))

    for v in range(V):
        for j in range(X // 2):
            if merge_y:
                first = place.at[1] == 0
                start = pl.multiple_of(jnp.where(first, Y - 8, 0), 8)
                own = (sub + jnp.where(first, 0, 4)) % 8 >= 4
                ymsg[v * (X // 2) + j] = packed(v, j, start, own)
            else:
                yhi[v * (X // 2) + j] = packed(v, j, Y - 8, sub >= 4)
                ylo[v * (X // 2) + j] = packed(v, j, 0, sub < 4)


def spread(cur, below, above, zl, zr):
    return below + above + roll(cur, 1, 0) + roll(cur, -1, 0) + zl + zr


def fine_sum(ref, v, i, V, lane):
    cur = ref[v, i]
    zl, zr = roll(cur, 1, 1), roll(cur, -1, 1)
    if v < V:
        rim = ref[V, i]
        last = lane.shape[1] - 1
        zl = jnp.where(lane == 0, roll(rim, -(16 * v + 2), 1), zl)
        zr = jnp.where(lane == last, roll(rim, last - (16 * v + 8), 1), zr)
    return spread(cur, ref[v, i - 1], ref[v, i + 1], zl, zr)


def fine_masks(place, Y, Z):
    R = Y + 8
    row = iota((R, Z), 0)
    ym = onehot(row < Y) + onehot((row >= Y) & (row < Y + H)) * f32(place.hi(1))
    ym = ym + onehot(row >= R - H) * f32(place.lo(1))
    lane = iota((R, Z), 1)
    outside_lo, outside_hi = lane % 16 < H, lane % 16 >= 8
    zm = jnp.where(outside_lo, f32(place.lo(2)), jnp.where(outside_hi, f32(place.hi(2)), jnp.float32(1.0)))
    return ym, ym * zm


def x_flag(place, i, X):
    if i < H:
        return f32(place.lo(0))
    if i >= H + X:
        return f32(place.hi(0))
    return None


def scaled(flag, mask):
    return mask if flag is None else mask * flag


def second_kernel(counts, merge_y, g, c, c1, xl, xh, yl, yh, slots, gram, G, S, p1, slots1, c2s, *refs):
    edges, (Q, CE, GL, VL) = refs[:-4], refs[-4:]
    V, X, Y, Z = g.shape
    R = Y + 8
    place = Place(counts)
    sub = iota((8, Z), 0)
    zero8 = jnp.zeros((8, Z), jnp.float32)
    zero_y = jnp.zeros((Y, Z), jnp.float32)
    has_yl, has_yh, has_xl, has_xh = place.lo(1), place.hi(1), place.lo(0), place.hi(0)
    m_hi = jnp.logical_and(sub < H, has_yh)
    m_lo = jnp.logical_and(sub >= 8 - H, has_yl)
    for v in range(V):
        for x in range(X):
            G[v, H + x, 0:Y] = g[v, x]
            hi, lo = yh[v * (X // 2) + x // 2], yl[v * (X // 2) + x // 2]
            if x % 2:
                hi, lo = roll(hi, 4, 0), roll(lo, 4, 0)
            G[v, H + x, Y:R] = jnp.where(m_hi, hi, jnp.where(m_lo, lo, zero8))
        for i in range(H):
            G[v, i, 0:Y] = keep(has_xl, xl[v * H + i])
            G[v, i, Y:R] = zero8
            G[v, H + X + i, 0:Y] = keep(has_xh, xh[v * H + i])
            G[v, H + X + i, Y:R] = zero8
    for dx in (-1, 1):
        for dy in (-1, 1):
            ok, t = place.has((dx, dy, 0)), place.slot((dx, dy, 0))
            for cell, (a, b) in enumerate(EDGE):
                i = H + X + a if dx > 0 else H - 1 - a
                r = Y + b if dy > 0 else R - 1 - b
                for v in range(V):
                    G[v, i, pl.ds(r, 1)] = keep(ok, slots[t, v, pl.ds(cell, 1)])
    r4 = iota((4, Z), 0)
    zero4 = jnp.zeros((4, Z), jnp.float32)

    def layers(dx, dy):
        tiles = []
        for v in range(V):
            for dz in (-1, 1):
                d = (dx, dy, dz)
                use = jnp.logical_and(r4 < H, place.has(d))
                tiles += [jnp.where(use, slots[place.slot(d), v], zero4), zero4]
        return jnp.concatenate(tiles, axis=0)

    wide = iota((16 * V, Z), 1)
    mid = layers(0, 0)
    sides = jnp.where(wide % Y < 8, layers(0, 1), layers(0, -1))
    first = jnp.concatenate([mid, sides], axis=0).T
    edges_x = jnp.where(wide < 2 * Y, layers(1, 0), layers(-1, 0))
    for d, start, to in (((1, 1), 0, 2), ((1, -1), 0, 3), ((-1, 1), X - 1, 4), ((-1, -1), X - 1, 5)):
        edges_x = jnp.where(wide // Y == to, roll(layers(*d), (to - start) * Y, 1), edges_x)
    second = jnp.concatenate([edges_x, jnp.zeros((Z - 16 * V, Z), jnp.float32)], axis=0).T
    lane_y, lane_8 = iota((Y, Z), 1) < 16 * V, iota((8, Z), 1) < 16 * V
    for i in (0, H + X + H - 1):
        G[V, i] = jnp.zeros((R, Z), jnp.float32)
    for x in range(X):
        tile = first[x * Y : (x + 1) * Y]
        G[V, H + x, 0:Y] = jnp.where(lane_y, tile, zero_y)
        other = roll(tile, Z - 16 * V, 1)
        edge = jnp.where(sub < 2, other[0:8], jnp.where(sub >= 6, other[Y - 8 : Y], zero8))
        G[V, H + x, Y:R] = jnp.where(lane_8, edge, zero8)
    for base, at in ((H + X, 0), (H - 2, X - 2)):
        for a in range(2):
            G[V, base + a, 0:Y] = second[(at + a) * Y : (at + a + 1) * Y]
            G[V, base + a, Y:R] = zero8
    for i, a in ((H + X, 2), (H - 1, 4)):
        up, down = second[a * Y : a * Y + 8], second[(a + 2) * Y - 8 : (a + 2) * Y]
        G[V, i, Y:R] = jnp.where(sub < 2, up, jnp.where(sub >= 6, down, zero8))
    lane = iota((R, Z), 1)
    for i in range(1, 2 * H + X - 1):
        rim = G[V, i]
        for v in range(V):
            body = G[v, i]
            rim = jnp.where((lane == 16 * v + 3) | (lane == 16 * v + 4), roll(body, 16 * v + 3, 1), rim)
            rim = jnp.where((lane == 16 * v + 6) | (lane == 16 * v + 7), roll(body, 16 * v + 8, 1), rim)
        G[V, i] = rim
    ym, zm = fine_masks(place, Y, Z)
    for i in range(1, 2 * H + X - 1):
        flag = x_flag(place, i, X)
        for v in range(V + 1):
            mask = scaled(flag, ym if v < V else zm)
            S[v, i] = mask * (PRE_G * G[v, i] + PRE_N * fine_sum(G, v, i, V, lane))
    for x in range(X // 2):
        for v in range(V):
            total = None
            for i in (2 * x, 2 * x + 1):
                inner = 6.0 * (G[v, H + i] - S[v, H + i]) + fine_sum(S, v, H + i, V, lane)
                part = c[i] * inner[0:Y]
                total = part if total is None else total + part
            Q[pl.ds((v * (X // 2) + x) * Y, Y)] = total
    li, lo = iota((Z, Z), 0), iota((Z, Z), 1)
    halve = onehot(lo == li // 2, 0.125)
    n, nc = V * X * Y // 4, X * Y // 4
    b1 = dot(Q[pl.ds(0, n, stride=2)] + Q[pl.ds(1, n, stride=2)], halve)
    cc = c1[...].reshape(nc, Z)
    scale = 1.0 / (1.5 * jnp.where(iota((nc, Z), 1) < Z // 2, cc, jnp.float32(1.0)))
    U = jnp.concatenate([b1[v * nc : (v + 1) * nc] * scale for v in range(V)], axis=0)
    per = nc
    for vp in range(V // 2):
        both = U[2 * vp * per : (2 * vp + 1) * per] + roll(U[(2 * vp + 1) * per : (2 * vp + 2) * per], Z // 2, 1)
        p1[vp] = both.reshape(X // 2, Y // 2, Z)
    half = Z // 2
    ends = jnp.where(iota(U.shape, 1) < 8, roll(U, H - half, 1), roll(U, 8, 1)).T
    faces = ends[0:16]
    X1, Y1 = X // 2, Y // 2
    if counts[0] * counts[1] * counts[2] <= 64:
        for t in range(counts[0] * counts[1] * counts[2]):
            for x in range(2):
                c2s[t, pl.ds(x, 1)] = slots[t, x, pl.ds(H, 1)]
    else:
        def move(t, carry):
            for x in range(2):
                c2s[t, pl.ds(x, 1)] = slots[t, x, pl.ds(H, 1)]
            return carry
        lax.fori_loop(0, c2s.shape[0], move, 0)
    around_c1(place, CE, c1, xl, xh, yl, yh, slots, V, X)
    gram_row = gram[0:1]
    tiles = contributions(place, U, gram_row, CE, GL, VL, Q, V)
    up, down = faces[0:4], faces[8:12]
    rest = counts[1] * counts[2]
    for x in range(counts[0]):
        for k, tile in enumerate(tiles[x % 2]):
            fill_tail(slots1.at[pl.ds(x * rest, rest)], rest, k, tile)
    for dx in (-1, 0, 1):
        for dy in (-1, 0, 1):
            slots1[place.slot((dx, dy, 1)), TAIL] = up
            slots1[place.slot((dx, dy, -1)), TAIL] = down
    for ref, (dx, dy) in zip(edges, edge_steps(merge_y)):
        for cell, (a, b) in enumerate(EDGE1):
            x = X1 - 1 - a if dx > 0 else a
            if dy == 0:
                y = jnp.where(place.at[1] == 0, Y1 - 1 - b, b)
            else:
                y = Y1 - 1 - b if dy > 0 else b
            for vp in range(V // 2):
                ref[pl.ds(cell * (V // 2) + vp, 1)] = p1[vp, x, pl.ds(y, 1)]


def around_c1(place, CE, c1, xl, xh, yl, yh, slots, V, X):
    X1, Y1, Z = c1.shape
    half, n = Z // 2, X1 * Y1
    sub, lane = iota((8, Z), 0), iota((8, Z), 1)
    zero = jnp.zeros((8, Z), jnp.float32)
    body = lane < half
    for i in range(1, 2 * H + X1 - 1):
        CE[i, Y1 : 2 * Y1] = zero
    for x in range(X1):
        CE[H + x, 0:Y1] = c1[x]
        for b in range(2):
            k = 2 * x + b
            hi, lo = yh[V * (X // 2), pl.ds(k, 1)], yl[V * (X // 2), pl.ds(k, 1)]
            CE[H + x, pl.ds(Y1 + b, 1)] = keep(place.hi(1), hi)
            CE[H + x, pl.ds(2 * Y1 - 1 - b, 1)] = keep(place.lo(1), lo)
    for ref, ok, near, far in ((xl, place.lo(0), H - 1, H - 2), (xh, place.hi(0), H + X1, H + X1 + 1)):
        tile = keep(ok, ref[V * H, 0:Y1])
        CE[near, 0:Y1] = jnp.where(body, tile, zero)
        CE[far, 0:Y1] = jnp.where(body, roll(tile, half, 1), zero)
    for dx in (-1, 1):
        for dy in (-1, 1):
            d = (dx, dy, 0)
            line = keep(place.has(d), slots[place.slot(d), 2, pl.ds(H, 1)])
            CE[H + X1 if dx > 0 else H - 1, pl.ds(Y1 if dy > 0 else 2 * Y1 - 1, 1)] = line
    rows = []
    steps = ((0, 0), (-1, 0), (1, 0), (0, -1), (0, 1))
    wanted = [range(X1), (X1 - 1,), (0,), range(X1), range(X1)]
    for (dx, dy), xs in zip(steps, wanted):
        pair = []
        for dz in (-1, 1):
            d = (dx, dy, dz)
            pair.append(keep(place.has(d), slots[place.slot(d), 2, pl.ds(H, 1)]))
        for x in xs:
            own = lane % n == x * Y1 + sub
            rows.append(jnp.concatenate([jnp.where(own, line, zero) for line in pair], axis=1))
    li, lo = iota((2 * Z, Z), 0), iota((2 * Z, Z), 1)
    l = li % Z
    target = jnp.where(li < Z, Z - 1 - l // n, half + l // n)
    d = dot(jnp.concatenate(rows, axis=0), onehot((lo == target) & (l < 2 * n)))
    d = [d[8 * m : 8 * m + 8] for m in range(len(rows))]
    CE[H - 1, 0:Y1] = CE[H - 1, 0:Y1] + d[X1]
    CE[H + X1, 0:Y1] = CE[H + X1, 0:Y1] + d[X1 + 1]
    for x in range(X1):
        CE[H + x, 0:Y1] = CE[H + x, 0:Y1] + d[x]
        edge = jnp.where(sub == 7, d[X1 + 2 + x], jnp.where(sub == 0, d[2 * X1 + 2 + x], zero))
        CE[H + x, Y1 : 2 * Y1] = CE[H + x, Y1 : 2 * Y1] + edge


def contributions(place, U, gram_row, CE, GL, VL, Q, V):
    X1, R1, Z = CE.shape[0] - 2 * H, CE.shape[1], CE.shape[2]
    Y1, half = R1 // 2, Z // 2
    zero = jnp.zeros((R1, Z), jnp.float32)
    n = X1 * Y1
    for v in range(V):
        for i in range(2 * H + X1):
            if H <= i < H + X1:
                k = v * n + (i - H) * Y1
                GL[v, i, 0:Y1] = U[k : k + Y1]
                GL[v, i, Y1:R1] = zero[0:Y1]
            else:
                GL[v, i] = zero
        for i in (0, 1, 2 * H + X1 - 2, 2 * H + X1 - 1):
            VL[v, i] = zero
    mask = coarse_masks(place, R1, Z)
    for i in range(H - 1, H + X1 + 1):
        m = scaled(x_flag(place, i, X1), mask)
        for v in range(V):
            get = lambda j: GL[v, j]
            if H <= i < H + X1:
                VL[v, i] = m * (PRE_G * GL[v, i] + PRE_N * level1_sum(get, i))
            else:
                VL[v, i] = m * (PRE_N * GL[v, i + 1 if i < H else i - 1])
    block = {1: 0, 2: 2, 3: 2 * V, 0: 2 * V + 2}
    for w in range(X1 // 2 + 2):
        for v in range(V):
            total = None
            for i in (H - 2 + 2 * w, H - 1 + 2 * w):
                get = lambda j: VL[v, j]
                if i == H - 2 or i == H + X1 + 1:
                    part = CE[i] * VL[v, i + 1 if i < H else i - 1]
                elif H <= i < H + X1:
                    part = CE[i] * (6.0 * (GL[v, i] - VL[v, i]) + level1_sum(get, i))
                else:
                    part = CE[i] * (level1_sum(get, i) - 6.0 * VL[v, i])
                total = part if total is None else total + part
            Q[pl.ds((block[w] + 4 * (v // 2) + v % 2) * R1, R1)] = total
    li, lo = iota((Z, Z), 0), iota((Z, Z), 1)
    width, m = half // 2, 4 * V
    stack = []
    for j in range(-1, Y1 // 2 + 1):
        r = (2 * j) % R1
        stack.append(Q[pl.ds(r, m, stride=R1)] + Q[pl.ds(r + 1, m, stride=R1)])
    to = jnp.where(li < half, li // 2, jnp.where(li < half + 2, width + 1, width))
    used = (li < half + 2) | (li >= Z - 2)
    small = dot(jnp.concatenate(stack, axis=0), onehot((lo == to) & used, 0.25 * 0.125))
    lane_m = iota((m, Z), 1)
    body, rims = jnp.zeros((m, Z), jnp.float32), jnp.zeros((m, Z), jnp.float32)
    for j in range(-1, Y1 // 2 + 1):
        piece = small[(j + 1) * m : (j + 2) * m]
        if 0 <= j < Y1 // 2:
            body = jnp.where(lane_m // width == j, roll(piece, j * width, 1), body)
        else:
            chunk = 0 if j < 0 else 1
            rims = jnp.where(lane_m // width == chunk, roll(piece, chunk * width, 1), rims)
        at = 2 * width + j + 1
        rims = jnp.where(lane_m == at, roll(piece, at - width, 1), rims)
        rims = jnp.where(lane_m == at + 8, roll(piece, at + 7 - width, 1), rims)
    lane4 = iota((4, Z), 1)
    pairs = []
    for p in range(V // 2):
        r, q = 4 * p, 2 * V + 4 * p
        own, rim = body[r : r + 4], rims[r : r + 4]
        beside, beside_rim = body[q : q + 4], rims[q : q + 4]
        edges = jnp.where(lane4 < half, rim, roll(beside_rim, half, 1))
        ends = jnp.where(lane4 < half, gram_row, jnp.where(lane4 < half + 16, rim, roll(beside_rim, 16, 1)))
        pairs.append((own, edges, beside, ends))
    return pairs


def coarse_masks(place, R, Z):
    half = Z // 2
    row, lane = iota((R, Z), 0), iota((R, Z), 1)
    y = R // 2
    mask = onehot(row < y) + onehot((row >= y) & (row < y + H)) * f32(place.hi(1))
    mask = mask + onehot(row >= R - H) * f32(place.lo(1))
    lanes = onehot(lane < half) + onehot((lane >= half) & (lane < half + H)) * f32(place.hi(2))
    lanes = lanes + onehot(lane >= Z - H) * f32(place.lo(2))
    return mask * lanes


def level1_sum(get, i):
    cur = get(i)
    return spread(cur, get(i - 1), get(i + 1), roll(cur, 1, 1), roll(cur, -1, 1))


def third_kernel(counts, merge_y, p1, xl, xh, yl, yh, slots, *refs):
    edges, (G1, S1) = refs[:-2], refs[-2:]
    VP, X, Y, Z = p1.shape
    V, R, half = 2 * VP, 2 * Y, Z // 2
    place = Place(counts)
    row, lane = iota((Y, Z), 0), iota((Y, Z), 1)
    zero = jnp.zeros((Y, Z), jnp.float32)

    def unpack(tile, v):
        return jnp.where(lane < half, roll(tile, half, 1) if v % 2 else tile, zero)

    r8, l8 = iota((8, Z), 0), iota((8, Z), 1)
    target = jnp.where(r8 < 4, Z - H, half) + r8 % 4
    place_lanes = onehot((l8 == target) & (r8 % 4 < H))

    def layers(dx, dy):
        below, above = (dx, dy, -1), (dx, dy, 1)
        low = keep(place.has(below), slots[place.slot(below), TAIL])
        high = keep(place.has(above), slots[place.slot(above), TAIL])
        return dot(jnp.concatenate([low, high], axis=0), place_lanes, TN)

    mid, up, down = layers(0, 0), layers(0, 1), layers(0, -1)
    m_hi = jnp.logical_and(row < H, place.hi(1))
    m_lo = jnp.logical_and(row >= Y - H, place.lo(1))

    def tile_of(d, v, x):
        k = (v * X + x) * Y
        return d[k : k + Y]

    for v in range(V):
        for x in range(X):
            G1[v, H + x, 0:Y] = unpack(p1[v // 2, x], v) + tile_of(mid, v, x)
            hi = unpack(yh[v // 2, x], v) + tile_of(up, v, x)
            lo = unpack(yl[v // 2, x], v) + tile_of(down, v, x)
            G1[v, H + x, Y:R] = jnp.where(m_hi, hi, jnp.where(m_lo, lo, zero))
    for dx in (-1, 1):
        side, up, down = layers(dx, 0), layers(dx, 1), layers(dx, -1)
        src = xh if dx > 0 else xl
        ok = place.hi(0) if dx > 0 else place.lo(0)
        for v in range(V):
            for a in range(H):
                x = a if dx > 0 else X - 1 - a
                i = H + X + a if dx > 0 else H - 1 - a
                G1[v, i, 0:Y] = keep(ok, unpack(src[v // 2, x], v) + tile_of(side, v, x))
                tile = zero
                if a < 2:
                    tile = jnp.where(m_hi, tile_of(up, v, x), jnp.where(m_lo, tile_of(down, v, x), zero))
                G1[v, i, Y:R] = tile
    for ref, (sx, sy) in zip(edges, edge_steps(merge_y)):
        dx = -sx
        for dy in (-1, 1) if sy == 0 else (-sy,):
            ok = place.has((dx, dy, 0))
            for cell, (a, b) in enumerate(EDGE1):
                i = H + X + a if dx > 0 else H - 1 - a
                r = Y + b if dy > 0 else R - 1 - b
                for v in range(V):
                    line = ref[pl.ds(cell * VP + v // 2, 1)]
                    line = roll(line, half, 1) if v % 2 else line
                    use = jnp.logical_and(lane[0:1] < half, ok)
                    line = jnp.where(use, line, jnp.zeros((1, Z), jnp.float32))
                    G1[v, i, pl.ds(r, 1)] = G1[v, i, pl.ds(r, 1)] + line
    mask = coarse_masks(place, R, Z)
    for i in range(1, 2 * H + X - 1):
        m = scaled(x_flag(place, i, X), mask)
        for v in range(V):
            get = lambda j: G1[v, j]
            S1[v, i] = m * (PRE_G * G1[v, i] + PRE_N * level1_sum(get, i))


def grid_of(count_y, count_x, fn):
    return [[fn(y, x) for x in range(count_x)] for y in range(count_y)]


def assemble(counts, parts_y, tile, lane):
    nx, ny, nz = counts
    width = lane.shape[1] // parts_y

    def one(y, x):
        y, j = y // parts_y, y % parts_y
        acc = roll(tile[x, y, 0], -width * j, 1)
        for z in range(1, nz):
            acc = jnp.where(lane // width == z, roll(tile[x, y, z], width * (z - j), 1), acc)
        return acc

    return grid_of(ny * parts_y, nx // 2, one)


def gather_parts(counts, parts_y, slots, lane, row):
    nx, ny, nz = counts
    width = lane.shape[1] // parts_y

    half = lane.shape[1] // 2

    def tile(x, y, z, k):
        t = (2 * x * ny + y) * nz + z
        return jnp.concatenate([slots[t, k], slots[t + ny * nz, k]], axis=0)

    every = [(x, y, z) for x in range(nx // 2) for y in range(ny) for z in range(nz)]
    edges, ends = {p: tile(*p, 1) for p in every}, {p: tile(*p, 3) for p in every}
    own = {p: tile(*p, 0) for p in every}
    beside = {p: roll(tile(*p, 2), 4, 0) for p in every}
    own_rim = {p: jnp.where(lane < half, edges[p], ends[p]) for p in every}
    beside_rim = {
        p: roll(jnp.where(lane < half, roll(edges[p], half, 1), roll(ends[p], -16, 1)), 4, 0) for p in every
    }
    zero = jnp.zeros(lane.shape, jnp.float32)

    def joined(own, beside, x, y, z):
        before = beside[x - 1, y, z] if x else zero
        after = beside[x + 1, y, z] if x < nx // 2 - 1 else zero
        return own[x, y, z] + jnp.where(row < 2, before, jnp.where(row >= 6, after, beside[x, y, z]))

    main = {p: joined(own, beside, *p) for p in every}
    rim = {p: joined(own_rim, beside_rim, *p) for p in every}

    def one(yy, x):
        y, j = yy // parts_y, yy % parts_y
        sources = [(main, y, j, j)]
        if j == 0 and y:
            sources.append((rim, y - 1, 1, parts_y))
        if j == parts_y - 1 and y < ny - 1:
            sources.append((rim, y + 1, 0, -1))
        total = None
        for grid, from_y, chunk, inner in sources:
            acc = roll(grid[x, from_y, 0], -width * chunk, 1)
            for z in range(1, nz):
                acc = jnp.where(lane // width == z, roll(grid[x, from_y, z], width * (z - chunk), 1), acc)
            for z in range(nz):
                at = 2 * width + inner + 1
                if z:
                    to = width * z - 1
                    acc = acc + jnp.where(lane == to, roll(rim[x, from_y, z], to - at, 1), jnp.zeros_like(acc))
                if z < nz - 1:
                    to = width * (z + 1)
                    acc = acc + jnp.where(lane == to, roll(rim[x, from_y, z], to - at - 8, 1), jnp.zeros_like(acc))
            total = acc if total is None else total + acc
        return total

    return grid_of(ny * parts_y, nx // 2, one)


def combine(fn, *grids):
    return [[fn(*ts) for ts in zip(*lines)] for lines in zip(*grids)]


def add(*terms):
    total = None
    for term in terms:
        if term is not None:
            total = term if total is None else total + term
    return total


def shrink_tiles(v, level, row, lane):
    step = 2 ** (level - 2)
    v = [[a + b for a, b in zip(v[2 * y], v[2 * y + 1])] for y in range(len(v) // 2)]
    if level == 2:
        v = combine(lambda t: t + jnp.where((row // 2) % 2 == 1, roll(t, 2, 0), roll(t, -2, 0)), v)
    elif level == 3:
        v = combine(lambda t: t + roll(t, 4, 0), v)
    else:
        v = [[line[2 * x] + line[2 * x + 1] for x in range(len(line) // 2)] for line in v]
    upper = (lane // step) % 2 == 1
    return combine(lambda t: 0.125 * (t + jnp.where(upper, roll(t, step, 1), roll(t, -step, 1))), v)


def weights_kernel(counts, parts_y, c2s, *outs):
    lane = iota((8, outs[0].shape[-1]), 1)
    row = iota(lane.shape, 0)
    nx, ny, nz = counts

    def tile(x, y, z):
        t = (2 * x * ny + y) * nz + z
        u = t + ny * nz
        low = jnp.where(row < 2, c2s[t, pl.ds(0, 1)], c2s[t, pl.ds(1, 1)])
        return jnp.where(row < 4, low, jnp.where(row < 6, c2s[u, pl.ds(0, 1)], c2s[u, pl.ds(1, 1)]))

    every = [(x, y, z) for x in range(nx // 2) for y in range(ny) for z in range(nz)]
    c = assemble(counts, parts_y, {p: tile(*p) for p in every}, lane)
    for level in range(2, LEVELS):
        for y in range(len(c)):
            for x in range(len(c[0])):
                outs[level - 2][y, x] = (0.25**level) * c[y][x]
        if level < LEVELS - 1:
            c = shrink_tiles(c, level, row, lane)


def coarse_kernel(counts, parts_y, slots1, *refs):
    *weights, mine, other, W, pre = refs
    nx, ny, nz = counts
    Z = slots1.shape[3]
    place = Place(counts)
    width = Z // parts_y
    lane = iota((8, Z), 1)
    row = iota((8, Z), 0)
    zero = jnp.zeros((8, Z), jnp.float32)
    scale = {2 + i: ref for i, ref in enumerate(weights)}
    inverse = {}
    for level, ref in scale.items():
        inverse[level] = grid_of(ref.shape[0], ref.shape[1], lambda y, x: 1.0 / (6.0 * ref[y, x]))

    def at(v, y, x):
        inside = 0 <= y < len(v) and 0 <= x < len(v[0])
        return v[y][x] if inside else None

    def neighbours(v, level):
        step = 2 ** (level - 2)
        shift = {2: 2, 3: 4}.get(level)
        ahead = combine(lambda t: roll(t, -shift, 0), v) if shift else v
        back = combine(lambda t: roll(t, shift, 0), v) if level == 2 else ahead

        def one(y, x):
            t = v[y][x]
            zs = jnp.where(lane < step, zero, roll(t, step, 1)) + jnp.where(lane >= Z - step, zero, roll(t, -step, 1))
            ys = add(zs, at(v, y - 1, x), at(v, y + 1, x))
            if not shift:
                return add(ys, at(v, y, x - 1), at(v, y, x + 1))
            after, before = at(ahead, y, x + 1), at(back, y, x - 1)
            after, before = zero if after is None else after, zero if before is None else before
            up = jnp.where(row >= 8 - shift, after, ahead[y][x])
            return ys + up + jnp.where(row < shift, before, back[y][x])

        return grid_of(len(v), len(v[0]), one)

    def grow(v, level):
        v = [line for line in v for _ in range(2)]
        return v if level < 4 else [[t for t in line for _ in range(2)] for line in v]

    def sweep(v, g, level):
        return combine(lambda a, b, s: KEEP * a + OMEGA * b + SIXTH * s, v, g, neighbours(v, level))

    def cycle(g, level):
        if level == LEVELS - 1:
            v = combine(lambda b: OMEGA * b, g)
            for _ in range(COARSE_SWEEPS - 1):
                v = sweep(v, g, level)
            return v
        v = combine(lambda b, s: PRE_G * b + PRE_N * s, g, neighbours(g, level))
        c = grid_of(len(g), len(g[0]), lambda y, x: scale[level][y, x])
        r = combine(lambda c, b, a, s: c * (6.0 * (b - a) + s), c, g, v, neighbours(v, level))
        down = shrink_tiles(r, level, row, lane)
        down = grid_of(len(down), len(down[0]), lambda y, x: down[y][x] * inverse[level + 1][y][x])
        v = combine(lambda a, b: a + b, v, grow(cycle(down, level + 1), level))
        return sweep(v, g, level)

    b2 = gather_parts(counts, parts_y, slots1, lane, row)
    v = cycle(grid_of(len(b2), nx // 2, lambda y, x: b2[y][x] * inverse[2][y][x]), 2)
    for y in range(len(v)):
        for x in range(nx // 2):
            W[y, x] = v[y][x]
    pre[...] = jnp.zeros_like(pre)
    ix, iy, iz = place.at
    for side, dev in enumerate((ix, ix + 1 - 2 * (ix % 2))):
        for xw in range(4):
            x = 2 * dev + xw - 1
            x_ok = jnp.logical_and(x >= 0, x < 2 * nx)
            x = jnp.clip(x, 0, 2 * nx - 1)
            for j in range(-1, parts_y + 1):
                y = iy * parts_y + j
                ok = jnp.logical_and(x_ok, jnp.logical_and(y >= 0, y < ny * parts_y))
                y = jnp.clip(y, 0, ny * parts_y - 1)
                for vec in range(2):
                    line = W[y, x // 4, pl.ds(2 * (x % 4) + vec, 1)]
                    pre[2 * side + vec, xw, pl.ds(j % 8, 1)] = keep(ok, line)
    li, lo = iota((Z, Z), 0), iota((Z, Z), 1)
    z1 = jnp.where(lo < 96, lo, lo - Z)
    window = onehot(li == iz * width + jnp.floor_divide(z1 + 2, 2) - 1)
    moved = dot(pre[...].reshape(4 * 4 * 8, Z), window).reshape(4, 4, 8, Z)
    mine[...] = moved[0:2]
    other[...] = moved[2:4]


def last_kernel(counts, mine, other, G1, S1, G, S, c, pre_hbm, op_hbm, E1, C1, E0, C0, pre, op, sems):
    V, X1, Y1, Z = S1.shape[0], S1.shape[1] - 2 * H, S1.shape[2] // 2, S1.shape[3]
    X, Y = 2 * X1, 2 * Y1
    R1, R = 2 * Y1, Y + 8
    place = Place(counts)
    for v in range(V):
        for x in range(X1):
            k = (v * X1 + x) * R1
            held = place.at[0] % 2 == v // 2
            tile = jnp.where(held, mine[v % 2, x], other[v % 2, x])
            E1[pl.ds(k, 8, stride=2)] = tile
            E1[pl.ds(k + 1, 8, stride=2)] = tile
    for v in range(V):
        for i in range(1, 2 * H + X1 - 1):
            C1[v, i] = S1[v, i] + E1[pl.ds((v * X1 + (i - 1) // 2) * R1, R1)]
    mask = coarse_masks(place, R1, Z)
    n = X1 + 2
    fine = []
    for v in range(V):
        tiles = []
        for i in range(H - 1, H + X1 + 1):
            m = scaled(x_flag(place, i, X1), mask)
            get = lambda j: C1[v, j]
            tiles.append(m * (KEEP * C1[v, i] + OMEGA * G1[v, i] + SIXTH * level1_sum(get, i)))
        fine.append(jnp.concatenate(tiles, axis=0))
    li, lo = iota((Z, 2 * Z), 0), iota((Z, 2 * Z), 1)
    half = Z // 2
    k = lo % 16
    source = jnp.where(k < H, Z - 1, jnp.where(k < 6, 0, jnp.where(k < 8, half - 1, half)))
    group = (lo - Z) // 16
    rim, doubled = None, []
    for v in range(V):
        both = dot(fine[v], onehot(((lo < Z) & (li == lo // 2)) | ((lo >= Z) & (li == source) & (group == v))))
        doubled.append(both[:, 0:Z])
        rim = both[:, Z:] if rim is None else rim + both[:, Z:]
    sub = iota((8, Z), 0)
    zero8 = jnp.zeros((8, Z), jnp.float32)
    for v in range(V + 1):
        wide = doubled[v] if v < V else rim
        for i in range(n):
            base = (v * n + i) * R
            tile = wide[i * R1 : i * R1 + Y1]
            edge = wide[i * R1 + Y1 : (i + 1) * R1]
            E0[pl.ds(base, 8, stride=2)] = tile
            E0[pl.ds(base + 1, 8, stride=2)] = tile
            E0[pl.ds(base + Y, 8)] = jnp.where(sub < 2, edge[0:1], jnp.where(sub >= 6, edge[7:8], zero8))
    for v in range(V + 1):
        for i in range(1, 2 * H + X - 1):
            C0[v, i] = S[v, i] + E0[pl.ds((v * n + (i - 1) // 2) * R, R)]
    ym, zm = fine_masks(place, Y, Z)
    lane = iota((R, Z), 1)
    for i in range(H - 1, H + X + 1):
        flag = x_flag(place, i, X)
        for v in range(V + 1):
            m = scaled(flag, ym if v < V else zm)
            value = m * (KEEP * C0[v, i] + OMEGA * G[v, i] + SIXTH * fine_sum(C0, v, i, V, lane))
            E0[pl.ds((v * (X + 2) + i - H + 1) * R, R)] = value
            if v < V and H <= i < H + X:
                pre[v, i - H] = value[0:Y]
    copies = [pltpu.make_async_copy(pre, pre_hbm, sems.at[0])]
    copies[0].start()

    class View:
        def __getitem__(self, key):
            v, i = key
            return E0[pl.ds((v * (X + 2) + i - H + 1) * R, R)]

    view = View()
    for x in range(X):
        for v in range(V):
            around = fine_sum(view, v, H + x, V, lane)
            op[v, x] = c[x] * (6.0 * view[v, H + x][0:Y] - around[0:Y])
        if x % 2:
            part = slice(x - 1, x + 1)
            copies.append(pltpu.make_async_copy(op.at[:, part], op_hbm.at[:, part], sems.at[1 + x // 2]))
            copies[-1].start()
    for copy in copies:
        copy.wait()


def gram_kernel(old, prev, out):
    M, X, Y, Z = old.shape
    J = prev.shape[0]
    pairs = [(a, b) for a in range(M + J) for b in range(a, M + J)]
    sums = [None] * len(pairs)
    for x in range(X):
        for y in range(0, Y, 8):
            tiles = [old[m, x, y : y + 8] for m in range(M)] + [prev[j, x, y : y + 8] for j in range(J)]
            for p, (a, b) in enumerate(pairs):
                term = tiles[a] * tiles[b]
                sums[p] = term if sums[p] is None else sums[p] + term
    ones = jnp.ones((8, Z), jnp.float32)
    lane = iota((8, Z), 1)
    rows = jnp.concatenate([jnp.sum(s, axis=0, keepdims=True) for s in sums], axis=0)
    pad = jnp.zeros((Z - len(pairs), Z), jnp.float32)
    out[...] = dot(ones, jnp.concatenate([rows, pad], axis=0), NT)


def ortho_kernel(count, cells, old, prev, slots, orth, proj, tri):
    M, X, Y, Z = old.shape
    J = prev.shape[0]
    if count <= 64:
        total = slots[0, TAIL - 1, pl.ds(0, 1)]
        for t in range(1, count):
            total = total + slots[t, TAIL - 1, pl.ds(0, 1)]
    else:
        total = lax.fori_loop(0, count, lambda t, s: s + slots[t, TAIL - 1, pl.ds(0, 1)], jnp.zeros((1, Z), jnp.float32))
    total = jnp.broadcast_to(total, (8, Z)) / cells
    value = {}
    p = 0
    for a in range(M + J):
        for b in range(a, M + J):
            one = jnp.broadcast_to(total[:, p : p + 1], (8, Z))
            value[a, b] = value[b, a] = one
            p += 1
    P_ = [[value[m, M + j] for j in range(J)] for m in range(M)]
    gram = {}
    for i in range(J):
        for j in range(i + 1):
            s = value[M + i, M + j]
            for m in range(M):
                inner = None
                for k in range(M):
                    term = value[m, k] * P_[k][j]
                    inner = term if inner is None else inner + term
                s = s - P_[m][i] * (P_[m][j] - inner) - P_[m][j] * P_[m][i]
            gram[i, j] = s
    L = {}
    for i in range(J):
        for j in range(i + 1):
            s = gram[i, j]
            for k in range(j):
                s = s - L[i, k] * L[j, k]
            L[i, j] = jnp.sqrt(s) if i == j else s / L[j, j]
    inv = {}
    for i in range(J):
        for j in range(i + 1):
            s = jnp.ones((8, Z), jnp.float32) if i == j else None
            for k in range(j, i):
                term = L[i, k] * inv[k, j]
                s = -term if s is None else s - term
            inv[i, j] = s / L[i, i]
    row, col = iota((M, J), 0), iota((M, J), 1)
    proj_v, tri_v = jnp.zeros((M, J), jnp.float32), jnp.zeros((J, J), jnp.float32)
    for m in range(M):
        for j in range(J):
            here = (row == m) & (col == j)
            proj_v = jnp.where(here, P_[m][j][0:M, 0:J], proj_v)
            if j >= m:
                tri_v = jnp.where(here, L[j, m][0:J, 0:J], tri_v)
    proj[...] = proj_v
    tri[...] = tri_v
    mix = {}
    for j in range(J):
        for m in range(M):
            s = None
            for i in range(j + 1):
                term = inv[j, i] * P_[m][i]
                s = term if s is None else s + term
            mix[j, m] = s
    for x in range(X):
        for y in range(0, Y, 8):
            olds = [old[m, x, y : y + 8] for m in range(M)]
            rem = []
            for i in range(J):
                r = prev[i, x, y : y + 8]
                for m in range(M):
                    r = r - P_[m][i] * olds[m]
                rem.append(r)
            for j in range(J):
                s = None
                for i in range(j + 1):
                    term = inv[j, i] * rem[i]
                    s = term if s is None else s + term
                orth[j, x, y : y + 8] = s


def run(near, kernel, shapes, args, scratch=(), name=None, result=(), plain=(), sems=0, out_sems=0):
    outs = []
    for i, shape in enumerate(shapes):
        kind = jax.ShapeDtypeStruct if i in result or not near else pltpu.VMEM
        outs.append(kind(shape, jnp.float32))
    if near:
        spaces = [pltpu.HBM if sems else None if i in plain else pltpu.VMEM for i in range(len(args))]
        args = [pltpu.with_memory_space_constraint(a, m) if m else a for a, m in zip(args, spaces)]
    fn = pl.pallas_call(
        kernel,
        out_shape=outs,
        in_specs=[HB if sems else VM] * len(args),
        out_specs=[HB if out_sems and i in result else VM for i in range(len(shapes))],
        scratch_shapes=[pltpu.VMEM(s, jnp.float32) for s in scratch] + [pltpu.SemaphoreType.DMA((sems + out_sems,))] * (sems + out_sems > 0),
        compiler_params=pltpu.CompilerParams(vmem_limit_bytes=16 * 2**20) if near else None,
        name=name,
    )
    return fn(*args)


def shift(value, axis, step):
    n = lax.axis_size(axis)
    return lax.ppermute(value, axis, [(i, (i + step) % n) for i in range(n)])


def diagonal(counts, value, dx, dy):
    nx, ny = counts[:2]
    step = dy if dy else 1
    pairs = [(x * ny + y, (x + dx) % nx * ny + (y + step) % ny) for x in range(nx) for y in range(ny)]
    return lax.ppermute(value, ("gx", "gy"), pairs)


def swap(slots):
    return lax.all_to_all(slots, AXES, split_axis=0, concat_axis=0, tiled=True)


def wide_coarse(counts, parts_y, c2s, slots1):
    nx, ny, nz = counts
    Z = slots1.shape[3]
    width = Z // parts_y
    lead, half = 2, Z // 2

    def across_x(own, beside):
        own, beside = (
            t.reshape(nx, ny, nz, 2, lead, Z).transpose(4, 3, 0, 1, 2, 5) for t in (own, beside)
        )
        pad = ((0, 0), (1, 1), (0, 0), (0, 0), (0, 0))
        first = own[:, 0] + jnp.pad(beside[:, 0], pad)[:, 0:nx]
        last = own[:, 1] + jnp.pad(beside[:, 1], pad)[:, 2:]
        return jnp.stack([first, last], axis=2).reshape(lead, 2 * nx, ny, nz, Z)

    edges, ends = slots1[:, 1], slots1[:, 3]
    low = iota((1, 1, Z), 2) < half
    main = across_x(slots1[:, 0], slots1[:, 2])
    rim = across_x(
        jnp.where(low, edges, ends), jnp.where(low, jnp.roll(edges, half, 2), jnp.roll(ends, -16, 2))
    )

    def with_z(line, low, high):
        pad = ((0, 0), (0, 0), (0, 0), (1, 1))
        first = jnp.pad(high, pad)[..., 0:nz]
        last = jnp.pad(low, pad)[..., 2:]
        lanes = iota((1, width), 1)[0]
        line = line + jnp.where(lanes == 0, first[..., None], 0.0) + jnp.where(lanes == width - 1, last[..., None], 0.0)
        return line.reshape(lead, 2 * nx, ny, nz * width)

    lines = []
    for j in range(-1, parts_y + 1):
        source, start = (rim, 0) if j < 0 else (rim, width) if j == parts_y else (main, j * width)
        at = 2 * width + j + 1
        lines.append(with_z(source[..., start : start + width], rim[..., at], rim[..., at + 8]))
    pad = ((0, 0), (0, 0), (1, 1), (0, 0))
    lines[1] = lines[1] + jnp.pad(lines[-1], pad)[:, :, 0:ny]
    lines[parts_y] = lines[parts_y] + jnp.pad(lines[0], pad)[:, :, 2:]
    b2 = jnp.stack(lines[1:-1], axis=3).reshape(lead, 2 * nx, ny * parts_y, nz * width)

    def whole(t, lead):
        t = t.reshape(nx, ny, nz, lead * 2, Z)
        parts = []
        for j in range(parts_y):
            part = t[..., j * width : (j + 1) * width].transpose(3, 0, 1, 2, 4)
            parts.append(part.reshape(lead * 2, nx, ny, nz * width))
        t = jnp.stack(parts, axis=3).reshape(lead, 2, nx, ny * parts_y, nz * width)
        return t.transpose(0, 2, 1, 3, 4).reshape(lead, nx * 2, ny * parts_y, nz * width)

    c2 = whole(c2s[:, 0:2], 1)
    g2 = b2 / (6.0 * 0.0625 * c2)

    def around(v):
        p = jnp.pad(v, ((0, 0), (1, 1), (1, 1), (1, 1)))
        m = slice(1, -1)
        return (
            p[:, 2:, m, m] + p[:, :-2, m, m] + p[:, m, 2:, m] + p[:, m, :-2, m] + p[:, m, m, 2:] + p[:, m, m, :-2]
        )

    def pairs(e):
        return onehot(iota((e, 2 * e), 0) == iota((e, 2 * e), 1) // 2)

    def shrink(v):
        d, a, b, e = v.shape
        v = v.reshape(d, a // 2, 2, b, e).sum(axis=2)
        v = v[:, :, 0::2] + v[:, :, 1::2]
        return dot(v.reshape(-1, e), pairs(e // 2).T * 0.125).reshape(d, a // 2, b // 2, e // 2)

    def grow(v):
        d, a, b, e = v.shape
        v = dot(v.reshape(-1, e), pairs(e)).reshape(d, a, b, 2 * e)
        return jnp.repeat(jnp.repeat(v, 2, axis=1), 2, axis=2)

    def cycle(g, c, level):
        if level == LEVELS - 1:
            v = OMEGA * g
            for _ in range(COARSE_SWEEPS - 1):
                v = KEEP * v + OMEGA * g + SIXTH * around(v)
            return v
        v = PRE_G * g + PRE_N * around(g)
        r = 0.25**level * c * (6.0 * (g - v) + around(v))
        down = shrink(c)
        v = v + grow(cycle(shrink(r) / (6.0 * 0.25 ** (level + 1) * down), down, level + 1))
        return KEEP * v + OMEGA * g + SIXTH * around(v)

    e = jnp.pad(cycle(g2, c2, 2), ((0, 0), (1, 1), (1, 1), (1, 1)))
    ix, iy, iz = (lax.axis_index(a) for a in AXES)

    def window(x):
        w = lax.dynamic_slice(
            e, (jnp.int32(0), x * 2, iy * parts_y, iz * width), (lead, 4, parts_y + 2, width + 2)
        )
        w = jnp.repeat(w, 2, axis=3)
        gap = jnp.zeros(w.shape[:3] + (Z - 2 * width - 4,), w.dtype)
        w = jnp.concatenate([w[..., 2:], gap, w[..., :2]], axis=3)
        pad = jnp.zeros((lead, 4, 8 - parts_y - 2, Z), w.dtype)
        return jnp.concatenate([w[:, :, 1:], pad, w[:, :, :1]], axis=2)

    return window(ix), window(ix + 1 - 2 * (ix % 2))


def per_device(counts, old, prev, inc, c):
    V, X, Y, Z = inc.shape
    count = counts[0] * counts[1] * counts[2]
    merge_y = counts[1] == 2
    near = count <= 64
    R = Y + 8
    X1, Y1 = X // 2, Y // 2
    y_shape, x_shape = (V * (X // 2) + 1, 8, Z), (V * H + 1, Y, Z)
    shapes = [(V, X, Y, Z), x_shape, x_shape, y_shape]
    shapes += [] if merge_y else [y_shape]
    shapes += [(count, V, H + 1, Z), (X1, Y1, Z)]
    outs = run(
        near,
        functools.partial(first_kernel, counts, merge_y),
        shapes,
        (inc, c),
        [inc.shape, c.shape, (X1 * Y, Z)],
        name="first",
        result=(len(shapes) - 2,),
        sems=V + 1,
    )
    g, xlo, xhi = outs[:3]
    c1 = outs[-1]
    slots0 = swap(outs[-2])
    xl, xh = shift(xhi, "gx", 1), shift(xlo, "gx", -1)
    if merge_y:
        yl = yh = shift(outs[3], "gy", 1)
    else:
        yl, yh = shift(outs[4], "gy", 1), shift(outs[3], "gy", -1)
    (gram,) = run(near, gram_kernel, [(8, Z)], (old, prev), name="gram", plain=(0, 1))
    ext0, ext1 = (V + 1, X + 2 * H, R, Z), (V, X1 + 2 * H, 2 * Y1, Z)
    steps = edge_steps(merge_y)
    G, S, p1, slots1, c2s, *edges = run(
        near,
        functools.partial(second_kernel, counts, merge_y),
        [ext0, ext0, (V // 2, X1, Y1, Z), (count, TAIL + 1, V, Z), (count, V, Z)] + [(16, Z)] * len(steps),
        (g, c, c1, xl, xh, yl, yh, slots0, gram),
        [(V * X1 * Y, Z), ext1[1:], ext1, ext1],
        name="second",
        result=(3,),
    )
    slots1 = swap(slots1)
    edges = [diagonal(counts, e, dx, dy) for e, (dx, dy) in zip(edges, steps)]
    xl, xh = shift(p1, "gx", 1), shift(p1, "gx", -1)
    if merge_y:
        yl = yh = shift(p1, "gy", 1)
    else:
        yl, yh = shift(p1, "gy", 1), shift(p1, "gy", -1)
    slots1, xl, xh, yl, yh, *edges = lax.optimization_barrier((slots1, xl, xh, yl, yh, *edges))
    G1, S1 = run(
        near,
        functools.partial(third_kernel, counts, merge_y),
        [ext1, ext1],
        (p1, xl, xh, yl, yh, slots1, *edges),
        name="third",
    )
    orth, proj, tri = run(
        near,
        functools.partial(ortho_kernel, count, float(count * X * Y * Z)),
        [(V, X, Y, Z), (4, 4), (4, 4)],
        (old, prev, slots1),
        name="ortho",
        result=(0, 1, 2),
        plain=(0, 1),
    )
    parts_y = Y // 4
    if near and counts[2] * (Z // parts_y) == Z and counts[0] % 4 == 0:
        sizes = [(counts[1] * parts_y, counts[0] // 2, 8, Z)]
        for level in range(3, LEVELS):
            y, x = sizes[-1][:2]
            sizes.append((y // 2, x if level < 5 else x // 2, 8, Z))
        weights = run(
            near, functools.partial(weights_kernel, counts, parts_y), sizes, (c2s,), name="weights"
        )
        e2, others = run(
            near,
            functools.partial(coarse_kernel, counts, parts_y),
            [(V // 2, 4, 8, Z)] * 2,
            (slots1, *weights),
            [sizes[0], (V, 4, 8, Z)],
            name="coarse",
        )
    else:
        e2, others = wide_coarse(counts, parts_y, c2s, slots1)
    others = lax.ppermute(others, "gx", [(i, i ^ 1) for i in range(counts[0])])
    pre, op = run(
        near,
        functools.partial(last_kernel, counts),
        [(V, X, Y, Z), (V, X, Y, Z)],
        (e2, others, G1, S1, G, S, c),
        [(V * X1 * 2 * Y1, Z), ext1, ((V + 1) * (X + 2) * R, Z), ext0, (V, X, Y, Z), (V, X, Y, Z)],
        name="last",
        result=(0, 1),
        out_sems=1 + X // 2,
    )
    return orth, proj, tri, pre, op


def solution(mesh):
    block = P(None, *AXES)
    counts = tuple(mesh.shape[a] for a in AXES)
    return jax.shard_map(
        functools.partial(per_device, counts),
        mesh=mesh,
        in_specs=(block, block, block, P(*AXES)),
        out_specs=(block, P(), P(), block, block),
        check_vma=False,
    )
```

```python
import functools

import jax
import jax.numpy as jnp
from jax import lax
from jax.experimental import pallas as pl
from jax.experimental.pallas import tpu as pltpu
from jax.sharding import PartitionSpec as P

LEVELS = 6
COARSE_SWEEPS = 4
OMEGA = 0.8
KEEP = 1.0 - OMEGA
SIXTH = OMEGA / 6.0
PRE_G = OMEGA * (2.0 - OMEGA)
PRE_N = OMEGA * OMEGA / 6.0
AXES = ("gx", "gy", "gz")
HIGH = lax.Precision.HIGHEST
H = 3
NN = (((1,), (0,)), ((), ()))
NT = (((1,), (1,)), ((), ()))
TN = (((0,), (0,)), ((), ()))
VM = pl.BlockSpec(memory_space=pltpu.VMEM)
HB = pl.BlockSpec(memory_space=pltpu.HBM)
EDGE = ((0, 0), (0, 1), (1, 0))
EDGE1 = EDGE + ((1, 1), (0, 2), (2, 0))
TAIL = 3
CHUNKS = (0, 1, 3)


def edge_steps(merge_y):
    return [(dx, dy) for dx in (1, -1) for dy in ((0,) if merge_y else (1, -1))]


def dot(a, b, dims=NN):
    return lax.dot_general(a, b, dims, precision=HIGH, preferred_element_type=jnp.float32)


def iota(shape, dim):
    return lax.broadcasted_iota(jnp.int32, shape, dim)


def onehot(cond, scale=1.0):
    return jnp.where(cond, jnp.float32(scale), jnp.float32(0.0))


def roll(a, shift, axis):
    size = a.shape[axis]
    shift = shift % size
    return a if shift == 0 else pltpu.roll(a, shift, axis)


class Place:
    def __init__(self, counts):
        self.counts = counts
        self.at = tuple(lax.axis_index(a) for a in AXES)
        self.me = self.linear(self.at)

    def linear(self, p):
        nx, ny, nz = self.counts
        return (p[0] * ny + p[1]) * nz + p[2]

    def lo(self, axis):
        return self.at[axis] > 0

    def hi(self, axis):
        return self.at[axis] < self.counts[axis] - 1

    def has(self, d):
        ok = None
        for axis in range(3):
            if d[axis]:
                one = self.hi(axis) if d[axis] > 0 else self.lo(axis)
                ok = one if ok is None else jnp.logical_and(ok, one)
        return ok

    def slot(self, d):
        there = self.linear(tuple(p + s for p, s in zip(self.at, d)))
        return jnp.where(self.has(d), there, self.me)


def f32(flag):
    return jnp.where(flag, jnp.float32(1.0), jnp.float32(0.0))


def keep(flag, a):
    return jnp.where(flag, a, jnp.zeros_like(a))


def fill_slots(ref, count, value, rows):
    if count <= 64:
        for t in range(count):
            ref[t, 0:rows] = value
    else:
        def body(t, carry):
            ref[t, 0:rows] = value
            return carry
        lax.fori_loop(0, count, body, 0)


def fill_tail(ref, count, k, value):
    if count <= 64:
        for t in range(count):
            ref[t, k] = value
    else:
        def body(t, carry):
            ref[t, k] = value
            return carry
        lax.fori_loop(0, count, body, 0)


def first_kernel(counts, merge_y, inc_hbm, c_hbm, old_hbm, prev_hbm, *refs):
    if merge_y:
        g, xlo, xhi, ymsg, slots, c1, inc, c, QC, old, prev, sems = refs
    else:
        g, xlo, xhi, ylo, yhi, slots, c1, inc, c, QC, old, prev, sems = refs
    V, X, Y, Z = inc.shape
    place = Place(counts)
    copy_c = pltpu.make_async_copy(c_hbm, c, sems.at[V])
    copies = [pltpu.make_async_copy(inc_hbm.at[v], inc.at[v], sems.at[v]) for v in range(V)]
    basis = [pltpu.make_async_copy(a, b, sems.at[V + 1 + i]) for i, (a, b) in enumerate(((old_hbm, old), (prev_hbm, prev)))]
    for copy in [copy_c] + copies + basis:
        copy.start()
    sub = iota((8, Z), 0)
    lane = iota((8, Z), 1)
    copy_c.wait()
    X1, Y1, half = X // 2, Y // 2, Z // 2
    for x in range(X1):
        QC[pl.ds(x * Y, Y)] = c[2 * x] + c[2 * x + 1]
    li, lo = iota((Z, Z), 0), iota((Z, Z), 1)
    n = X1 * Y1
    cc = dot(QC[pl.ds(0, n, stride=2)] + QC[pl.ds(1, n, stride=2)], onehot(lo == li // 2, 0.125))
    c1[...] = cc.reshape(X1, Y1, Z)
    stack = []
    for y in range(Y // 4):
        sums = []
        for x in range(X // 4):
            k = 2 * x * Y1 + 2 * y
            pair = cc[k : k + 2] + cc[k + Y1 : k + Y1 + 2]
            sums.append(pair[0:1] + pair[1:2])
        stack.append(jnp.where(sub % 2 == 0, sums[0], sums[1]))
    stack = dot(jnp.concatenate(stack, axis=0), onehot((lo == li // 2) & (li < half), 0.125))
    c2 = stack[0:8]
    for y in range(1, Y // 4):
        c2 = c2 + roll(stack[8 * y : 8 * y + 8], y * (half // 2), 1)
    r4, l4 = iota((4, Z), 0), iota((4, Z), 1)
    zero4 = jnp.zeros((4, Z), jnp.float32)
    base = [jnp.where(r4 == H, c2[x : x + 1], zero4) for x in range(2)] + [zero4] * (V - 2)
    for v in range(2):
        fill_tail(slots, counts[0] * counts[1] * counts[2], v, base[v])

    wide8 = lane < half
    xlo[V * H, 0:Y1] = jnp.where(wide8, c1[0], roll(c1[1], half, 1))
    xhi[V * H, 0:Y1] = jnp.where(wide8, c1[X1 - 1], roll(c1[X1 - 2], half, 1))
    ends = [(ymsg, jnp.where(place.at[1] == 0, 1, 0))] if merge_y else [(ylo, 0), (yhi, 1)]
    for ref, upper in ends:
        for x in range(X1):
            for b in range(2):
                y = jnp.where(upper == 1, Y1 - 1 - b, b)
                ref[V * (X // 2), pl.ds(2 * x + b, 1)] = c1[x, pl.ds(y, 1)]
    scale = [1.0 / (6.0 * c[x]) for x in range(X)]
    for v in range(V):
        copies[v].wait()
        for x in range(X):
            value = inc[v, x] * scale[x]
            g[v, x] = value
            if x < H:
                xlo[v * H + x] = value
            if x >= X - H:
                xhi[v * H + x - (X - H)] = value
    faces = []
    for x in range(X):
        for y in range(0, Y, 8):
            acc = jnp.zeros((8, Z), jnp.float32)
            for v in range(V):
                acc = jnp.where(lane // 8 == v, roll(g[v, x, y : y + 8], 8 * v + H, 1), acc)
            m = len(faces)
            if m < X1:
                acc = jnp.where(lane // 2 == 4 * V, roll(c1[m], 8 * V - half + 2, 1), acc)
                acc = jnp.where(lane // 2 == 4 * V + 1, roll(c1[m], 8 * V + 2, 1), acc)
            faces.append(acc)
    faces = jnp.concatenate(faces, axis=0).T
    k = 8 * V
    c_up = jnp.where(l4 < n, faces[k + 1 : k + 2], roll(faces[k : k + 8], n, 1)[0:1])
    c_down = jnp.where(l4 < n, faces[k + 2 : k + 3], roll(faces[k : k + 8], n, 1)[3:4])
    for copy in basis:
        copy.wait()
    base[V - 1] = jnp.where(r4 == H, gram_row(old, prev), zero4)
    fill_tail(slots, counts[0] * counts[1] * counts[2], V - 1, base[V - 1])
    rows_up = [jnp.where(r4 < H, faces[8 * v : 8 * v + 4], base[v]) for v in range(V)]
    rows_down = [jnp.where(r4 < H, faces[8 * v + H : 8 * v + H + 4], base[v]) for v in range(V)]
    rows_up[2] = jnp.where(r4 < H, rows_up[2], jnp.where(l4 < 2 * n, c_up, zero4))
    rows_down[2] = jnp.where(r4 < H, rows_down[2], jnp.where(l4 < 2 * n, c_down, zero4))
    for dx in (-1, 0, 1):
        for dy in (-1, 0, 1):
            above, below = place.slot((dx, dy, 1)), place.slot((dx, dy, -1))
            for v in range(V):
                slots[above, v] = rows_up[v]
                slots[below, v] = rows_down[v]
            if dx and dy:
                t = place.slot((dx, dy, 0))
                for cell, (a, b) in enumerate(EDGE):
                    x = X - 1 - a if dx > 0 else a
                    y = Y - 1 - b if dy > 0 else b
                    for v in range(V):
                        slots[t, v, pl.ds(cell, 1)] = g[v, x, pl.ds(y, 1)]
                corner = c1[X1 - 1 if dx > 0 else 0, pl.ds(Y1 - 1 if dy > 0 else 0, 1)]
                slots[t, 2, pl.ds(H, 1)] = corner

    def packed(v, j, start, own):
        return jnp.where(own, g[v, 2 * j, pl.ds(start, 8)], roll(g[v, 2 * j + 1, pl.ds(start, 8)], 4, 0))

    for v in range(V):
        for j in range(X // 2):
            if merge_y:
                first = place.at[1] == 0
                start = pl.multiple_of(jnp.where(first, Y - 8, 0), 8)
                own = (sub + jnp.where(first, 0, 4)) % 8 >= 4
                ymsg[v * (X // 2) + j] = packed(v, j, start, own)
            else:
                yhi[v * (X // 2) + j] = packed(v, j, Y - 8, sub >= 4)
                ylo[v * (X // 2) + j] = packed(v, j, 0, sub < 4)


def spread(cur, below, above, zl, zr):
    return below + above + roll(cur, 1, 0) + roll(cur, -1, 0) + zl + zr


def fine_sum(ref, v, i, V, lane):
    cur = ref[v, i]
    zl, zr = roll(cur, 1, 1), roll(cur, -1, 1)
    if v < V:
        rim = ref[V, i]
        last = lane.shape[1] - 1
        zl = jnp.where(lane == 0, roll(rim, -(16 * v + 2), 1), zl)
        zr = jnp.where(lane == last, roll(rim, last - (16 * v + 8), 1), zr)
    return spread(cur, ref[v, i - 1], ref[v, i + 1], zl, zr)


def fine_masks(place, Y, Z):
    R = Y + 8
    row = iota((R, Z), 0)
    ym = onehot(row < Y) + onehot((row >= Y) & (row < Y + H)) * f32(place.hi(1))
    ym = ym + onehot(row >= R - H) * f32(place.lo(1))
    lane = iota((R, Z), 1)
    outside_lo, outside_hi = lane % 16 < H, lane % 16 >= 8
    zm = jnp.where(outside_lo, f32(place.lo(2)), jnp.where(outside_hi, f32(place.hi(2)), jnp.float32(1.0)))
    return ym, ym * zm


def x_flag(place, i, X):
    if i < H:
        return f32(place.lo(0))
    if i >= H + X:
        return f32(place.hi(0))
    return None


def scaled(flag, mask):
    return mask if flag is None else mask * flag


def second_kernel(counts, merge_y, g, c, c1, xl, xh, yl, yh, slots, G, S, p1, slots1, c2s, *refs):
    edges, (Q, CE, GL, VL) = refs[:-4], refs[-4:]
    V, X, Y, Z = g.shape
    R = Y + 8
    place = Place(counts)
    sub = iota((8, Z), 0)
    zero8 = jnp.zeros((8, Z), jnp.float32)
    zero_y = jnp.zeros((Y, Z), jnp.float32)
    has_yl, has_yh, has_xl, has_xh = place.lo(1), place.hi(1), place.lo(0), place.hi(0)
    m_hi = jnp.logical_and(sub < H, has_yh)
    m_lo = jnp.logical_and(sub >= 8 - H, has_yl)
    for v in range(V):
        for x in range(X):
            G[v, H + x, 0:Y] = g[v, x]
            hi, lo = yh[v * (X // 2) + x // 2], yl[v * (X // 2) + x // 2]
            if x % 2:
                hi, lo = roll(hi, 4, 0), roll(lo, 4, 0)
            G[v, H + x, Y:R] = jnp.where(m_hi, hi, jnp.where(m_lo, lo, zero8))
        for i in range(H):
            G[v, i, 0:Y] = keep(has_xl, xl[v * H + i])
            G[v, i, Y:R] = zero8
            G[v, H + X + i, 0:Y] = keep(has_xh, xh[v * H + i])
            G[v, H + X + i, Y:R] = zero8
    for dx in (-1, 1):
        for dy in (-1, 1):
            ok, t = place.has((dx, dy, 0)), place.slot((dx, dy, 0))
            for cell, (a, b) in enumerate(EDGE):
                i = H + X + a if dx > 0 else H - 1 - a
                r = Y + b if dy > 0 else R - 1 - b
                for v in range(V):
                    G[v, i, pl.ds(r, 1)] = keep(ok, slots[t, v, pl.ds(cell, 1)])
    r4 = iota((4, Z), 0)
    zero4 = jnp.zeros((4, Z), jnp.float32)

    def layers(dx, dy):
        tiles = []
        for v in range(V):
            for dz in (-1, 1):
                d = (dx, dy, dz)
                use = jnp.logical_and(r4 < H, place.has(d))
                tiles += [jnp.where(use, slots[place.slot(d), v], zero4), zero4]
        return jnp.concatenate(tiles, axis=0)

    wide = iota((16 * V, Z), 1)
    mid = layers(0, 0)
    sides = jnp.where(wide % Y < 8, layers(0, 1), layers(0, -1))
    first = jnp.concatenate([mid, sides], axis=0).T
    edges_x = jnp.where(wide < 2 * Y, layers(1, 0), layers(-1, 0))
    for d, start, to in (((1, 1), 0, 2), ((1, -1), 0, 3), ((-1, 1), X - 1, 4), ((-1, -1), X - 1, 5)):
        edges_x = jnp.where(wide // Y == to, roll(layers(*d), (to - start) * Y, 1), edges_x)
    second = jnp.concatenate([edges_x, jnp.zeros((Z - 16 * V, Z), jnp.float32)], axis=0).T
    lane_y, lane_8 = iota((Y, Z), 1) < 16 * V, iota((8, Z), 1) < 16 * V
    for i in (0, H + X + H - 1):
        G[V, i] = jnp.zeros((R, Z), jnp.float32)
    for x in range(X):
        tile = first[x * Y : (x + 1) * Y]
        G[V, H + x, 0:Y] = jnp.where(lane_y, tile, zero_y)
        other = roll(tile, Z - 16 * V, 1)
        edge = jnp.where(sub < 2, other[0:8], jnp.where(sub >= 6, other[Y - 8 : Y], zero8))
        G[V, H + x, Y:R] = jnp.where(lane_8, edge, zero8)
    for base, at in ((H + X, 0), (H - 2, X - 2)):
        for a in range(2):
            G[V, base + a, 0:Y] = second[(at + a) * Y : (at + a + 1) * Y]
            G[V, base + a, Y:R] = zero8
    for i, a in ((H + X, 2), (H - 1, 4)):
        up, down = second[a * Y : a * Y + 8], second[(a + 2) * Y - 8 : (a + 2) * Y]
        G[V, i, Y:R] = jnp.where(sub < 2, up, jnp.where(sub >= 6, down, zero8))
    lane = iota((R, Z), 1)
    for i in range(1, 2 * H + X - 1):
        rim = G[V, i]
        for v in range(V):
            body = G[v, i]
            rim = jnp.where((lane == 16 * v + 3) | (lane == 16 * v + 4), roll(body, 16 * v + 3, 1), rim)
            rim = jnp.where((lane == 16 * v + 6) | (lane == 16 * v + 7), roll(body, 16 * v + 8, 1), rim)
        G[V, i] = rim
    ym, zm = fine_masks(place, Y, Z)
    for i in range(1, 2 * H + X - 1):
        flag = x_flag(place, i, X)
        for v in range(V + 1):
            mask = scaled(flag, ym if v < V else zm)
            S[v, i] = mask * (PRE_G * G[v, i] + PRE_N * fine_sum(G, v, i, V, lane))
    for x in range(X // 2):
        for v in range(V):
            total = None
            for i in (2 * x, 2 * x + 1):
                inner = 6.0 * (G[v, H + i] - S[v, H + i]) + fine_sum(S, v, H + i, V, lane)
                part = c[i] * inner[0:Y]
                total = part if total is None else total + part
            Q[pl.ds((v * (X // 2) + x) * Y, Y)] = total
    li, lo = iota((Z, Z), 0), iota((Z, Z), 1)
    halve = onehot(lo == li // 2, 0.125)
    n, nc = V * X * Y // 4, X * Y // 4
    b1 = dot(Q[pl.ds(0, n, stride=2)] + Q[pl.ds(1, n, stride=2)], halve)
    cc = c1[...].reshape(nc, Z)
    scale = 1.0 / (1.5 * jnp.where(iota((nc, Z), 1) < Z // 2, cc, jnp.float32(1.0)))
    U = jnp.concatenate([b1[v * nc : (v + 1) * nc] * scale for v in range(V)], axis=0)
    per = nc
    for vp in range(V // 2):
        both = U[2 * vp * per : (2 * vp + 1) * per] + roll(U[(2 * vp + 1) * per : (2 * vp + 2) * per], Z // 2, 1)
        p1[vp] = both.reshape(X // 2, Y // 2, Z)
    half = Z // 2
    ends = jnp.where(iota(U.shape, 1) < 8, roll(U, H - half, 1), roll(U, 8, 1)).T
    faces = ends[0:16]
    X1, Y1 = X // 2, Y // 2
    if counts[0] * counts[1] * counts[2] <= 64:
        for t in range(counts[0] * counts[1] * counts[2]):
            for x in range(2):
                c2s[t, pl.ds(x, 1)] = slots[t, x, pl.ds(H, 1)]
    else:
        def move(t, carry):
            for x in range(2):
                c2s[t, pl.ds(x, 1)] = slots[t, x, pl.ds(H, 1)]
            return carry
        lax.fori_loop(0, c2s.shape[0], move, 0)
    around_c1(place, CE, c1, xl, xh, yl, yh, slots, V, X)
    tiles = contributions(place, U, CE, GL, VL, Q, V)
    r4, l4 = iota((4, Z), 0), iota((4, Z), 1)

    def spread_layers(rows):
        turned = [roll(rows, 32 * k, 1) for k in range(4)]
        out = jnp.zeros((4, Z), jnp.float32)
        for v in range(V):
            for k, chunk in enumerate(CHUNKS):
                out = jnp.where((r4 == v) & (l4 // 32 == chunk), turned[(chunk - v) % 4][k : k + 1], out)
        return out

    up, down = spread_layers(faces[0:8]), spread_layers(faces[8:16])
    rest = counts[1] * counts[2]
    for x in range(counts[0]):
        for k, tile in enumerate(tiles[x % 2]):
            fill_tail(slots1.at[pl.ds(x * rest, rest)], rest, k, tile)
    middle = l4 // 32 == 2
    for dx in (-1, 0, 1):
        even = (place.at[0] + 2 + dx) % 2 == 0
        ends = jnp.where(even, tiles[0][TAIL], tiles[1][TAIL])
        for dy in (-1, 0, 1):
            for dz, layer in ((1, up), (-1, down)):
                d = (dx, dy, dz)

                @pl.when(place.has(d))
                def _():
                    slots1[place.slot(d), TAIL] = jnp.where(middle, ends, layer)
    for ref, (dx, dy) in zip(edges, edge_steps(merge_y)):
        for cell, (a, b) in enumerate(EDGE1):
            x = X1 - 1 - a if dx > 0 else a
            if dy == 0:
                y = jnp.where(place.at[1] == 0, Y1 - 1 - b, b)
            else:
                y = Y1 - 1 - b if dy > 0 else b
            for vp in range(V // 2):
                ref[pl.ds(cell * (V // 2) + vp, 1)] = p1[vp, x, pl.ds(y, 1)]


def around_c1(place, CE, c1, xl, xh, yl, yh, slots, V, X):
    X1, Y1, Z = c1.shape
    half, n = Z // 2, X1 * Y1
    sub, lane = iota((8, Z), 0), iota((8, Z), 1)
    zero = jnp.zeros((8, Z), jnp.float32)
    body = lane < half
    for i in range(1, 2 * H + X1 - 1):
        CE[i, Y1 : 2 * Y1] = zero
    for x in range(X1):
        CE[H + x, 0:Y1] = c1[x]
        for b in range(2):
            k = 2 * x + b
            hi, lo = yh[V * (X // 2), pl.ds(k, 1)], yl[V * (X // 2), pl.ds(k, 1)]
            CE[H + x, pl.ds(Y1 + b, 1)] = keep(place.hi(1), hi)
            CE[H + x, pl.ds(2 * Y1 - 1 - b, 1)] = keep(place.lo(1), lo)
    for ref, ok, near, far in ((xl, place.lo(0), H - 1, H - 2), (xh, place.hi(0), H + X1, H + X1 + 1)):
        tile = keep(ok, ref[V * H, 0:Y1])
        CE[near, 0:Y1] = jnp.where(body, tile, zero)
        CE[far, 0:Y1] = jnp.where(body, roll(tile, half, 1), zero)
    for dx in (-1, 1):
        for dy in (-1, 1):
            d = (dx, dy, 0)
            line = keep(place.has(d), slots[place.slot(d), 2, pl.ds(H, 1)])
            CE[H + X1 if dx > 0 else H - 1, pl.ds(Y1 if dy > 0 else 2 * Y1 - 1, 1)] = line
    rows = []
    steps = ((0, 0), (-1, 0), (1, 0), (0, -1), (0, 1))
    wanted = [range(X1), (X1 - 1,), (0,), range(X1), range(X1)]
    for (dx, dy), xs in zip(steps, wanted):
        pair = []
        for dz in (-1, 1):
            d = (dx, dy, dz)
            pair.append(keep(place.has(d), slots[place.slot(d), 2, pl.ds(H, 1)]))
        for x in xs:
            own = lane % n == x * Y1 + sub
            rows.append(jnp.concatenate([jnp.where(own, line, zero) for line in pair], axis=1))
    li, lo = iota((2 * Z, Z), 0), iota((2 * Z, Z), 1)
    l = li % Z
    target = jnp.where(li < Z, Z - 1 - l // n, half + l // n)
    d = dot(jnp.concatenate(rows, axis=0), onehot((lo == target) & (l < 2 * n)))
    d = [d[8 * m : 8 * m + 8] for m in range(len(rows))]
    CE[H - 1, 0:Y1] = CE[H - 1, 0:Y1] + d[X1]
    CE[H + X1, 0:Y1] = CE[H + X1, 0:Y1] + d[X1 + 1]
    for x in range(X1):
        CE[H + x, 0:Y1] = CE[H + x, 0:Y1] + d[x]
        edge = jnp.where(sub == 7, d[X1 + 2 + x], jnp.where(sub == 0, d[2 * X1 + 2 + x], zero))
        CE[H + x, Y1 : 2 * Y1] = CE[H + x, Y1 : 2 * Y1] + edge


def contributions(place, U, CE, GL, VL, Q, V):
    X1, R1, Z = CE.shape[0] - 2 * H, CE.shape[1], CE.shape[2]
    Y1, half = R1 // 2, Z // 2
    zero = jnp.zeros((R1, Z), jnp.float32)
    n = X1 * Y1
    for v in range(V):
        for i in range(2 * H + X1):
            if H <= i < H + X1:
                k = v * n + (i - H) * Y1
                GL[v, i, 0:Y1] = U[k : k + Y1]
                GL[v, i, Y1:R1] = zero[0:Y1]
            else:
                GL[v, i] = zero
        for i in (0, 1, 2 * H + X1 - 2, 2 * H + X1 - 1):
            VL[v, i] = zero
    mask = coarse_masks(place, R1, Z)
    for i in range(H - 1, H + X1 + 1):
        m = scaled(x_flag(place, i, X1), mask)
        for v in range(V):
            get = lambda j: GL[v, j]
            if H <= i < H + X1:
                VL[v, i] = m * (PRE_G * GL[v, i] + PRE_N * level1_sum(get, i))
            else:
                VL[v, i] = m * (PRE_N * GL[v, i + 1 if i < H else i - 1])
    block = {1: 0, 2: 2, 3: 2 * V, 0: 2 * V + 2}
    for w in range(X1 // 2 + 2):
        for v in range(V):
            total = None
            for i in (H - 2 + 2 * w, H - 1 + 2 * w):
                get = lambda j: VL[v, j]
                if i == H - 2 or i == H + X1 + 1:
                    part = CE[i] * VL[v, i + 1 if i < H else i - 1]
                elif H <= i < H + X1:
                    part = CE[i] * (6.0 * (GL[v, i] - VL[v, i]) + level1_sum(get, i))
                else:
                    part = CE[i] * (level1_sum(get, i) - 6.0 * VL[v, i])
                total = part if total is None else total + part
            Q[pl.ds((block[w] + 4 * (v // 2) + v % 2) * R1, R1)] = total
    li, lo = iota((Z, Z), 0), iota((Z, Z), 1)
    width, m = half // 2, 4 * V
    stack = []
    for j in range(-1, Y1 // 2 + 1):
        r = (2 * j) % R1
        stack.append(Q[pl.ds(r, m, stride=R1)] + Q[pl.ds(r + 1, m, stride=R1)])
    to = jnp.where(li < half, li // 2, jnp.where(li < half + 2, width + 1, width))
    used = (li < half + 2) | (li >= Z - 2)
    small = dot(jnp.concatenate(stack, axis=0), onehot((lo == to) & used, 0.25 * 0.125))
    lane_m = iota((m, Z), 1)
    body, rims = jnp.zeros((m, Z), jnp.float32), jnp.zeros((m, Z), jnp.float32)
    for j in range(-1, Y1 // 2 + 1):
        piece = small[(j + 1) * m : (j + 2) * m]
        if 0 <= j < Y1 // 2:
            body = jnp.where(lane_m // width == j, roll(piece, j * width, 1), body)
        else:
            chunk = 0 if j < 0 else 1
            rims = jnp.where(lane_m // width == chunk, roll(piece, chunk * width, 1), rims)
        at = 2 * width + j + 1
        rims = jnp.where(lane_m == at, roll(piece, at - width, 1), rims)
        rims = jnp.where(lane_m == at + 8, roll(piece, at + 7 - width, 1), rims)
    lane4 = iota((4, Z), 1)
    pairs = []
    for p in range(V // 2):
        r, q = 4 * p, 2 * V + 4 * p
        own, rim = body[r : r + 4], rims[r : r + 4]
        beside, beside_rim = body[q : q + 4], rims[q : q + 4]
        edges = jnp.where(lane4 < half, rim, roll(beside_rim, half, 1))
        ends = jnp.where(lane4 < half + 16, rim, roll(beside_rim, 16, 1))
        pairs.append((own, edges, beside, ends))
    return pairs


def coarse_masks(place, R, Z):
    half = Z // 2
    row, lane = iota((R, Z), 0), iota((R, Z), 1)
    y = R // 2
    mask = onehot(row < y) + onehot((row >= y) & (row < y + H)) * f32(place.hi(1))
    mask = mask + onehot(row >= R - H) * f32(place.lo(1))
    lanes = onehot(lane < half) + onehot((lane >= half) & (lane < half + H)) * f32(place.hi(2))
    lanes = lanes + onehot(lane >= Z - H) * f32(place.lo(2))
    return mask * lanes


def level1_sum(get, i):
    cur = get(i)
    return spread(cur, get(i - 1), get(i + 1), roll(cur, 1, 1), roll(cur, -1, 1))


def third_kernel(counts, merge_y, p1, xl, xh, yl, yh, slots, *refs):
    edges, (G1, S1) = refs[:-2], refs[-2:]
    VP, X, Y, Z = p1.shape
    V, R, half = 2 * VP, 2 * Y, Z // 2
    place = Place(counts)
    row, lane = iota((Y, Z), 0), iota((Y, Z), 1)
    zero = jnp.zeros((Y, Z), jnp.float32)

    def unpack(tile, v):
        return jnp.where(lane < half, roll(tile, half, 1) if v % 2 else tile, zero)

    r8, l8 = iota((8, Z), 0), iota((8, Z), 1)
    target = jnp.where(r8 < 4, Z - H, half) + r8 % 4
    place_lanes = onehot((l8 == target) & (r8 % 4 < H))

    def layers(dx, dy):
        below, above = (dx, dy, -1), (dx, dy, 1)
        low = keep(place.has(below), slots[place.slot(below), TAIL])
        high = keep(place.has(above), slots[place.slot(above), TAIL])
        both = jnp.concatenate([low, high], axis=0)
        turned = [roll(both, 32 * k, 1) for k in range(4)]
        lines = jnp.zeros((8, Z), jnp.float32)
        for v in range(V):
            for k, chunk in enumerate(CHUNKS):
                source = turned[(v - chunk) % 4]
                here = l8 // 32 == v
                lines = jnp.where(here & (r8 == k), source[v : v + 1], lines)
                lines = jnp.where(here & (r8 == 4 + k), source[4 + v : 5 + v], lines)
        return dot(lines, place_lanes, TN)

    mid, up, down = layers(0, 0), layers(0, 1), layers(0, -1)
    m_hi = jnp.logical_and(row < H, place.hi(1))
    m_lo = jnp.logical_and(row >= Y - H, place.lo(1))

    def tile_of(d, v, x):
        k = (v * X + x) * Y
        return d[k : k + Y]

    for v in range(V):
        for x in range(X):
            G1[v, H + x, 0:Y] = unpack(p1[v // 2, x], v) + tile_of(mid, v, x)
            hi = unpack(yh[v // 2, x], v) + tile_of(up, v, x)
            lo = unpack(yl[v // 2, x], v) + tile_of(down, v, x)
            G1[v, H + x, Y:R] = jnp.where(m_hi, hi, jnp.where(m_lo, lo, zero))
    for dx in (-1, 1):
        side, up, down = layers(dx, 0), layers(dx, 1), layers(dx, -1)
        src = xh if dx > 0 else xl
        ok = place.hi(0) if dx > 0 else place.lo(0)
        for v in range(V):
            for a in range(H):
                x = a if dx > 0 else X - 1 - a
                i = H + X + a if dx > 0 else H - 1 - a
                G1[v, i, 0:Y] = keep(ok, unpack(src[v // 2, x], v) + tile_of(side, v, x))
                tile = zero
                if a < 2:
                    tile = jnp.where(m_hi, tile_of(up, v, x), jnp.where(m_lo, tile_of(down, v, x), zero))
                G1[v, i, Y:R] = tile
    for ref, (sx, sy) in zip(edges, edge_steps(merge_y)):
        dx = -sx
        for dy in (-1, 1) if sy == 0 else (-sy,):
            ok = place.has((dx, dy, 0))
            for cell, (a, b) in enumerate(EDGE1):
                i = H + X + a if dx > 0 else H - 1 - a
                r = Y + b if dy > 0 else R - 1 - b
                for v in range(V):
                    line = ref[pl.ds(cell * VP + v // 2, 1)]
                    line = roll(line, half, 1) if v % 2 else line
                    use = jnp.logical_and(lane[0:1] < half, ok)
                    line = jnp.where(use, line, jnp.zeros((1, Z), jnp.float32))
                    G1[v, i, pl.ds(r, 1)] = G1[v, i, pl.ds(r, 1)] + line
    mask = coarse_masks(place, R, Z)
    for i in range(1, 2 * H + X - 1):
        m = scaled(x_flag(place, i, X), mask)
        for v in range(V):
            get = lambda j: G1[v, j]
            S1[v, i] = m * (PRE_G * G1[v, i] + PRE_N * level1_sum(get, i))


def grid_of(count_y, count_x, fn):
    return [[fn(y, x) for x in range(count_x)] for y in range(count_y)]


def assemble(counts, parts_y, tile, lane):
    nx, ny, nz = counts
    width = lane.shape[1] // parts_y

    def one(y, x):
        y, j = y // parts_y, y % parts_y
        acc = roll(tile[x, y, 0], -width * j, 1)
        for z in range(1, nz):
            acc = jnp.where(lane // width == z, roll(tile[x, y, z], width * (z - j), 1), acc)
        return acc

    return grid_of(ny * parts_y, nx // 2, one)


def gather_parts(counts, parts_y, slots, lane, row):
    nx, ny, nz = counts
    width = lane.shape[1] // parts_y

    half = lane.shape[1] // 2

    def tile(x, y, z, k):
        t = (2 * x * ny + y) * nz + z
        return jnp.concatenate([slots[t, k], slots[t + ny * nz, k]], axis=0)

    every = [(x, y, z) for x in range(nx // 2) for y in range(ny) for z in range(nz)]
    edges, ends = {p: tile(*p, 1) for p in every}, {p: tile(*p, 3) for p in every}
    own = {p: tile(*p, 0) for p in every}
    beside = {p: roll(tile(*p, 2), 4, 0) for p in every}
    own_rim = {p: jnp.where(lane < half, edges[p], ends[p]) for p in every}
    beside_rim = {
        p: roll(jnp.where(lane < half, roll(edges[p], half, 1), roll(ends[p], -16, 1)), 4, 0) for p in every
    }
    zero = jnp.zeros(lane.shape, jnp.float32)

    def joined(own, beside, x, y, z):
        before = beside[x - 1, y, z] if x else zero
        after = beside[x + 1, y, z] if x < nx // 2 - 1 else zero
        return own[x, y, z] + jnp.where(row < 2, before, jnp.where(row >= 6, after, beside[x, y, z]))

    main = {p: joined(own, beside, *p) for p in every}
    rim = {p: joined(own_rim, beside_rim, *p) for p in every}

    def one(yy, x):
        y, j = yy // parts_y, yy % parts_y
        sources = [(main, y, j, j)]
        if j == 0 and y:
            sources.append((rim, y - 1, 1, parts_y))
        if j == parts_y - 1 and y < ny - 1:
            sources.append((rim, y + 1, 0, -1))
        total = None
        for grid, from_y, chunk, inner in sources:
            acc = roll(grid[x, from_y, 0], -width * chunk, 1)
            for z in range(1, nz):
                acc = jnp.where(lane // width == z, roll(grid[x, from_y, z], width * (z - chunk), 1), acc)
            for z in range(nz):
                at = 2 * width + inner + 1
                if z:
                    to = width * z - 1
                    acc = acc + jnp.where(lane == to, roll(rim[x, from_y, z], to - at, 1), jnp.zeros_like(acc))
                if z < nz - 1:
                    to = width * (z + 1)
                    acc = acc + jnp.where(lane == to, roll(rim[x, from_y, z], to - at - 8, 1), jnp.zeros_like(acc))
            total = acc if total is None else total + acc
        return total

    return grid_of(ny * parts_y, nx // 2, one)


def combine(fn, *grids):
    return [[fn(*ts) for ts in zip(*lines)] for lines in zip(*grids)]


def add(*terms):
    total = None
    for term in terms:
        if term is not None:
            total = term if total is None else total + term
    return total


def shrink_tiles(v, level, row, lane):
    step = 2 ** (level - 2)
    v = [[a + b for a, b in zip(v[2 * y], v[2 * y + 1])] for y in range(len(v) // 2)]
    if level == 2:
        v = combine(lambda t: t + jnp.where((row // 2) % 2 == 1, roll(t, 2, 0), roll(t, -2, 0)), v)
    elif level == 3:
        v = combine(lambda t: t + roll(t, 4, 0), v)
    else:
        v = [[line[2 * x] + line[2 * x + 1] for x in range(len(line) // 2)] for line in v]
    upper = (lane // step) % 2 == 1
    return combine(lambda t: 0.125 * (t + jnp.where(upper, roll(t, step, 1), roll(t, -step, 1))), v)


def weights_kernel(counts, parts_y, c2s, *outs):
    lane = iota((8, outs[0].shape[-1]), 1)
    row = iota(lane.shape, 0)
    nx, ny, nz = counts

    def tile(x, y, z):
        t = (2 * x * ny + y) * nz + z
        u = t + ny * nz
        low = jnp.where(row < 2, c2s[t, pl.ds(0, 1)], c2s[t, pl.ds(1, 1)])
        return jnp.where(row < 4, low, jnp.where(row < 6, c2s[u, pl.ds(0, 1)], c2s[u, pl.ds(1, 1)]))

    every = [(x, y, z) for x in range(nx // 2) for y in range(ny) for z in range(nz)]
    c = assemble(counts, parts_y, {p: tile(*p) for p in every}, lane)
    for level in range(2, LEVELS):
        for y in range(len(c)):
            for x in range(len(c[0])):
                outs[level - 2][y, x] = (0.25**level) * c[y][x]
        if level < LEVELS - 1:
            c = shrink_tiles(c, level, row, lane)


def coarse_kernel(counts, parts_y, slots1, *refs):
    *weights, mine, other, W, pre = refs
    nx, ny, nz = counts
    Z = slots1.shape[3]
    place = Place(counts)
    width = Z // parts_y
    lane = iota((8, Z), 1)
    row = iota((8, Z), 0)
    zero = jnp.zeros((8, Z), jnp.float32)
    scale = {2 + i: ref for i, ref in enumerate(weights)}
    inverse = {}
    for level, ref in scale.items():
        inverse[level] = grid_of(ref.shape[0], ref.shape[1], lambda y, x: 1.0 / (6.0 * ref[y, x]))

    def at(v, y, x):
        inside = 0 <= y < len(v) and 0 <= x < len(v[0])
        return v[y][x] if inside else None

    def neighbours(v, level):
        step = 2 ** (level - 2)
        shift = {2: 2, 3: 4}.get(level)
        ahead = combine(lambda t: roll(t, -shift, 0), v) if shift else v
        back = combine(lambda t: roll(t, shift, 0), v) if level == 2 else ahead

        def one(y, x):
            t = v[y][x]
            zs = jnp.where(lane < step, zero, roll(t, step, 1)) + jnp.where(lane >= Z - step, zero, roll(t, -step, 1))
            ys = add(zs, at(v, y - 1, x), at(v, y + 1, x))
            if not shift:
                return add(ys, at(v, y, x - 1), at(v, y, x + 1))
            after, before = at(ahead, y, x + 1), at(back, y, x - 1)
            after, before = zero if after is None else after, zero if before is None else before
            up = jnp.where(row >= 8 - shift, after, ahead[y][x])
            return ys + up + jnp.where(row < shift, before, back[y][x])

        return grid_of(len(v), len(v[0]), one)

    def grow(v, level):
        v = [line for line in v for _ in range(2)]
        return v if level < 4 else [[t for t in line for _ in range(2)] for line in v]

    def sweep(v, g, level):
        return combine(lambda a, b, s: KEEP * a + OMEGA * b + SIXTH * s, v, g, neighbours(v, level))

    def cycle(g, level):
        if level == LEVELS - 1:
            v = combine(lambda b: OMEGA * b, g)
            for _ in range(COARSE_SWEEPS - 1):
                v = sweep(v, g, level)
            return v
        v = combine(lambda b, s: PRE_G * b + PRE_N * s, g, neighbours(g, level))
        c = grid_of(len(g), len(g[0]), lambda y, x: scale[level][y, x])
        r = combine(lambda c, b, a, s: c * (6.0 * (b - a) + s), c, g, v, neighbours(v, level))
        down = shrink_tiles(r, level, row, lane)
        down = grid_of(len(down), len(down[0]), lambda y, x: down[y][x] * inverse[level + 1][y][x])
        v = combine(lambda a, b: a + b, v, grow(cycle(down, level + 1), level))
        return sweep(v, g, level)

    b2 = gather_parts(counts, parts_y, slots1, lane, row)
    v = cycle(grid_of(len(b2), nx // 2, lambda y, x: b2[y][x] * inverse[2][y][x]), 2)
    for y in range(len(v)):
        for x in range(nx // 2):
            W[y, x] = v[y][x]
    pre[...] = jnp.zeros_like(pre)
    ix, iy, iz = place.at
    for side, dev in enumerate((ix, ix + 1 - 2 * (ix % 2))):
        for xw in range(4):
            x = 2 * dev + xw - 1
            x_ok = jnp.logical_and(x >= 0, x < 2 * nx)
            x = jnp.clip(x, 0, 2 * nx - 1)
            for j in range(-1, parts_y + 1):
                y = iy * parts_y + j
                ok = jnp.logical_and(x_ok, jnp.logical_and(y >= 0, y < ny * parts_y))
                y = jnp.clip(y, 0, ny * parts_y - 1)
                for vec in range(2):
                    line = W[y, x // 4, pl.ds(2 * (x % 4) + vec, 1)]
                    pre[2 * side + vec, xw, pl.ds(j % 8, 1)] = keep(ok, line)
    li, lo = iota((Z, Z), 0), iota((Z, Z), 1)
    z1 = jnp.where(lo < 96, lo, lo - Z)
    window = onehot(li == iz * width + jnp.floor_divide(z1 + 2, 2) - 1)
    moved = dot(pre[...].reshape(4 * 4 * 8, Z), window).reshape(4, 4, 8, Z)
    mine[...] = moved[0:2]
    other[...] = moved[2:4]


def last_kernel(counts, mine, other, G1, S1, G, S, c, pre_hbm, op_hbm, E1, C1, E0, C0, pre, op, sems):
    V, X1, Y1, Z = S1.shape[0], S1.shape[1] - 2 * H, S1.shape[2] // 2, S1.shape[3]
    X, Y = 2 * X1, 2 * Y1
    R1, R = 2 * Y1, Y + 8
    place = Place(counts)
    for v in range(V):
        for x in range(X1):
            k = (v * X1 + x) * R1
            held = place.at[0] % 2 == v // 2
            tile = jnp.where(held, mine[v % 2, x], other[v % 2, x])
            E1[pl.ds(k, 8, stride=2)] = tile
            E1[pl.ds(k + 1, 8, stride=2)] = tile
    for v in range(V):
        for i in range(1, 2 * H + X1 - 1):
            C1[v, i] = S1[v, i] + E1[pl.ds((v * X1 + (i - 1) // 2) * R1, R1)]
    mask = coarse_masks(place, R1, Z)
    n = X1 + 2
    fine = []
    for v in range(V):
        tiles = []
        for i in range(H - 1, H + X1 + 1):
            m = scaled(x_flag(place, i, X1), mask)
            get = lambda j: C1[v, j]
            tiles.append(m * (KEEP * C1[v, i] + OMEGA * G1[v, i] + SIXTH * level1_sum(get, i)))
        fine.append(jnp.concatenate(tiles, axis=0))
    li, lo = iota((Z, 2 * Z), 0), iota((Z, 2 * Z), 1)
    half = Z // 2
    k = lo % 16
    source = jnp.where(k < H, Z - 1, jnp.where(k < 6, 0, jnp.where(k < 8, half - 1, half)))
    group = (lo - Z) // 16
    rim, doubled = None, []
    for v in range(V):
        both = dot(fine[v], onehot(((lo < Z) & (li == lo // 2)) | ((lo >= Z) & (li == source) & (group == v))))
        doubled.append(both[:, 0:Z])
        rim = both[:, Z:] if rim is None else rim + both[:, Z:]
    sub = iota((8, Z), 0)
    zero8 = jnp.zeros((8, Z), jnp.float32)
    for v in range(V + 1):
        wide = doubled[v] if v < V else rim
        for i in range(n):
            base = (v * n + i) * R
            tile = wide[i * R1 : i * R1 + Y1]
            edge = wide[i * R1 + Y1 : (i + 1) * R1]
            E0[pl.ds(base, 8, stride=2)] = tile
            E0[pl.ds(base + 1, 8, stride=2)] = tile
            E0[pl.ds(base + Y, 8)] = jnp.where(sub < 2, edge[0:1], jnp.where(sub >= 6, edge[7:8], zero8))
    for v in range(V + 1):
        for i in range(1, 2 * H + X - 1):
            C0[v, i] = S[v, i] + E0[pl.ds((v * n + (i - 1) // 2) * R, R)]
    ym, zm = fine_masks(place, Y, Z)
    lane = iota((R, Z), 1)
    for i in range(H - 1, H + X + 1):
        flag = x_flag(place, i, X)
        for v in range(V + 1):
            m = scaled(flag, ym if v < V else zm)
            value = m * (KEEP * C0[v, i] + OMEGA * G[v, i] + SIXTH * fine_sum(C0, v, i, V, lane))
            E0[pl.ds((v * (X + 2) + i - H + 1) * R, R)] = value
            if v < V and H <= i < H + X:
                pre[v, i - H] = value[0:Y]
    copies = [pltpu.make_async_copy(pre, pre_hbm, sems.at[0])]
    copies[0].start()

    class View:
        def __getitem__(self, key):
            v, i = key
            return E0[pl.ds((v * (X + 2) + i - H + 1) * R, R)]

    view = View()
    for x in range(X):
        for v in range(V):
            around = fine_sum(view, v, H + x, V, lane)
            op[v, x] = c[x] * (6.0 * view[v, H + x][0:Y] - around[0:Y])
        if x % 2:
            part = slice(x - 1, x + 1)
            copies.append(pltpu.make_async_copy(op.at[:, part], op_hbm.at[:, part], sems.at[1 + x // 2]))
            copies[-1].start()
    for copy in copies:
        copy.wait()


def gram_row(old, prev):
    M, X, Y, Z = old.shape
    J = prev.shape[0]
    pairs = [(a, b) for a in range(M + J) for b in range(a, M + J)]
    sums = [None] * len(pairs)
    for x in range(X):
        for y in range(0, Y, 8):
            tiles = [old[m, x, y : y + 8] for m in range(M)] + [prev[j, x, y : y + 8] for j in range(J)]
            for p, (a, b) in enumerate(pairs):
                term = tiles[a] * tiles[b]
                sums[p] = term if sums[p] is None else sums[p] + term
    ones = jnp.ones((8, Z), jnp.float32)
    lane = iota((8, Z), 1)
    rows = jnp.concatenate([jnp.sum(s, axis=0, keepdims=True) for s in sums], axis=0)
    pad = jnp.zeros((Z - len(pairs), Z), jnp.float32)
    return dot(ones, jnp.concatenate([rows, pad], axis=0), NT)[0:1]


def ortho_kernel(count, cells, old, prev, slots, orth, proj, tri):
    M, X, Y, Z = old.shape
    J = prev.shape[0]
    if count <= 64:
        total = slots[0, M - 1, pl.ds(H, 1)]
        for t in range(1, count):
            total = total + slots[t, M - 1, pl.ds(H, 1)]
    else:
        total = lax.fori_loop(0, count, lambda t, s: s + slots[t, M - 1, pl.ds(H, 1)], jnp.zeros((1, Z), jnp.float32))
    total = jnp.broadcast_to(total, (8, Z)) / cells
    value = {}
    p = 0
    for a in range(M + J):
        for b in range(a, M + J):
            one = jnp.broadcast_to(total[:, p : p + 1], (8, Z))
            value[a, b] = value[b, a] = one
            p += 1
    P_ = [[value[m, M + j] for j in range(J)] for m in range(M)]
    gram = {}
    for i in range(J):
        for j in range(i + 1):
            s = value[M + i, M + j]
            for m in range(M):
                inner = None
                for k in range(M):
                    term = value[m, k] * P_[k][j]
                    inner = term if inner is None else inner + term
                s = s - P_[m][i] * (P_[m][j] - inner) - P_[m][j] * P_[m][i]
            gram[i, j] = s
    L = {}
    for i in range(J):
        for j in range(i + 1):
            s = gram[i, j]
            for k in range(j):
                s = s - L[i, k] * L[j, k]
            L[i, j] = jnp.sqrt(s) if i == j else s / L[j, j]
    inv = {}
    for i in range(J):
        for j in range(i + 1):
            s = jnp.ones((8, Z), jnp.float32) if i == j else None
            for k in range(j, i):
                term = L[i, k] * inv[k, j]
                s = -term if s is None else s - term
            inv[i, j] = s / L[i, i]
    row, col = iota((M, J), 0), iota((M, J), 1)
    proj_v, tri_v = jnp.zeros((M, J), jnp.float32), jnp.zeros((J, J), jnp.float32)
    for m in range(M):
        for j in range(J):
            here = (row == m) & (col == j)
            proj_v = jnp.where(here, P_[m][j][0:M, 0:J], proj_v)
            if j >= m:
                tri_v = jnp.where(here, L[j, m][0:J, 0:J], tri_v)
    proj[...] = proj_v
    tri[...] = tri_v
    mix = {}
    for j in range(J):
        for m in range(M):
            s = None
            for i in range(j + 1):
                term = inv[j, i] * P_[m][i]
                s = term if s is None else s + term
            mix[j, m] = s
    for x in range(X):
        for y in range(0, Y, 8):
            olds = [old[m, x, y : y + 8] for m in range(M)]
            rem = []
            for i in range(J):
                r = prev[i, x, y : y + 8]
                for m in range(M):
                    r = r - P_[m][i] * olds[m]
                rem.append(r)
            for j in range(J):
                s = None
                for i in range(j + 1):
                    term = inv[j, i] * rem[i]
                    s = term if s is None else s + term
                orth[j, x, y : y + 8] = s


def run(near, kernel, shapes, args, scratch=(), name=None, result=(), plain=(), sems=0, out_sems=0):
    outs = []
    for i, shape in enumerate(shapes):
        kind = jax.ShapeDtypeStruct if i in result or not near else pltpu.VMEM
        outs.append(kind(shape, jnp.float32))
    if near:
        spaces = [pltpu.HBM if sems else None if i in plain else pltpu.VMEM for i in range(len(args))]
        args = [pltpu.with_memory_space_constraint(a, m) if m else a for a, m in zip(args, spaces)]
    fn = pl.pallas_call(
        kernel,
        out_shape=outs,
        in_specs=[HB if sems else VM] * len(args),
        out_specs=[HB if out_sems and i in result else VM for i in range(len(shapes))],
        scratch_shapes=[pltpu.VMEM(s, jnp.float32) for s in scratch] + [pltpu.SemaphoreType.DMA((sems + out_sems,))] * (sems + out_sems > 0),
        compiler_params=pltpu.CompilerParams(vmem_limit_bytes=16 * 2**20) if near else None,
        name=name,
    )
    return fn(*args)


def shift(value, axis, step):
    n = lax.axis_size(axis)
    return lax.ppermute(value, axis, [(i, (i + step) % n) for i in range(n)])


def diagonal(counts, value, dx, dy):
    nx, ny = counts[:2]
    step = dy if dy else 1
    pairs = [(x * ny + y, (x + dx) % nx * ny + (y + step) % ny) for x in range(nx) for y in range(ny)]
    return lax.ppermute(value, ("gx", "gy"), pairs)


def swap(slots):
    return lax.all_to_all(slots, AXES, split_axis=0, concat_axis=0, tiled=True)


def wide_coarse(counts, parts_y, c2s, slots1):
    nx, ny, nz = counts
    Z = slots1.shape[3]
    width = Z // parts_y
    lead, half = 2, Z // 2

    def across_x(own, beside):
        own, beside = (
            t.reshape(nx, ny, nz, 2, lead, Z).transpose(4, 3, 0, 1, 2, 5) for t in (own, beside)
        )
        pad = ((0, 0), (1, 1), (0, 0), (0, 0), (0, 0))
        first = own[:, 0] + jnp.pad(beside[:, 0], pad)[:, 0:nx]
        last = own[:, 1] + jnp.pad(beside[:, 1], pad)[:, 2:]
        return jnp.stack([first, last], axis=2).reshape(lead, 2 * nx, ny, nz, Z)

    edges, ends = slots1[:, 1], slots1[:, 3]
    low = iota((1, 1, Z), 2) < half
    main = across_x(slots1[:, 0], slots1[:, 2])
    rim = across_x(
        jnp.where(low, edges, ends), jnp.where(low, jnp.roll(edges, half, 2), jnp.roll(ends, -16, 2))
    )

    def with_z(line, low, high):
        pad = ((0, 0), (0, 0), (0, 0), (1, 1))
        first = jnp.pad(high, pad)[..., 0:nz]
        last = jnp.pad(low, pad)[..., 2:]
        lanes = iota((1, width), 1)[0]
        line = line + jnp.where(lanes == 0, first[..., None], 0.0) + jnp.where(lanes == width - 1, last[..., None], 0.0)
        return line.reshape(lead, 2 * nx, ny, nz * width)

    lines = []
    for j in range(-1, parts_y + 1):
        source, start = (rim, 0) if j < 0 else (rim, width) if j == parts_y else (main, j * width)
        at = 2 * width + j + 1
        lines.append(with_z(source[..., start : start + width], rim[..., at], rim[..., at + 8]))
    pad = ((0, 0), (0, 0), (1, 1), (0, 0))
    lines[1] = lines[1] + jnp.pad(lines[-1], pad)[:, :, 0:ny]
    lines[parts_y] = lines[parts_y] + jnp.pad(lines[0], pad)[:, :, 2:]
    b2 = jnp.stack(lines[1:-1], axis=3).reshape(lead, 2 * nx, ny * parts_y, nz * width)

    def whole(t, lead):
        t = t.reshape(nx, ny, nz, lead * 2, Z)
        parts = []
        for j in range(parts_y):
            part = t[..., j * width : (j + 1) * width].transpose(3, 0, 1, 2, 4)
            parts.append(part.reshape(lead * 2, nx, ny, nz * width))
        t = jnp.stack(parts, axis=3).reshape(lead, 2, nx, ny * parts_y, nz * width)
        return t.transpose(0, 2, 1, 3, 4).reshape(lead, nx * 2, ny * parts_y, nz * width)

    c2 = whole(c2s[:, 0:2], 1)
    g2 = b2 / (6.0 * 0.0625 * c2)

    def around(v):
        p = jnp.pad(v, ((0, 0), (1, 1), (1, 1), (1, 1)))
        m = slice(1, -1)
        return (
            p[:, 2:, m, m] + p[:, :-2, m, m] + p[:, m, 2:, m] + p[:, m, :-2, m] + p[:, m, m, 2:] + p[:, m, m, :-2]
        )

    def pairs(e):
        return onehot(iota((e, 2 * e), 0) == iota((e, 2 * e), 1) // 2)

    def shrink(v):
        d, a, b, e = v.shape
        v = v.reshape(d, a // 2, 2, b, e).sum(axis=2)
        v = v[:, :, 0::2] + v[:, :, 1::2]
        return dot(v.reshape(-1, e), pairs(e // 2).T * 0.125).reshape(d, a // 2, b // 2, e // 2)

    def grow(v):
        d, a, b, e = v.shape
        v = dot(v.reshape(-1, e), pairs(e)).reshape(d, a, b, 2 * e)
        return jnp.repeat(jnp.repeat(v, 2, axis=1), 2, axis=2)

    def cycle(g, c, level):
        if level == LEVELS - 1:
            v = OMEGA * g
            for _ in range(COARSE_SWEEPS - 1):
                v = KEEP * v + OMEGA * g + SIXTH * around(v)
            return v
        v = PRE_G * g + PRE_N * around(g)
        r = 0.25**level * c * (6.0 * (g - v) + around(v))
        down = shrink(c)
        v = v + grow(cycle(shrink(r) / (6.0 * 0.25 ** (level + 1) * down), down, level + 1))
        return KEEP * v + OMEGA * g + SIXTH * around(v)

    e = jnp.pad(cycle(g2, c2, 2), ((0, 0), (1, 1), (1, 1), (1, 1)))
    ix, iy, iz = (lax.axis_index(a) for a in AXES)

    def window(x):
        w = lax.dynamic_slice(
            e, (jnp.int32(0), x * 2, iy * parts_y, iz * width), (lead, 4, parts_y + 2, width + 2)
        )
        w = jnp.repeat(w, 2, axis=3)
        gap = jnp.zeros(w.shape[:3] + (Z - 2 * width - 4,), w.dtype)
        w = jnp.concatenate([w[..., 2:], gap, w[..., :2]], axis=3)
        pad = jnp.zeros((lead, 4, 8 - parts_y - 2, Z), w.dtype)
        return jnp.concatenate([w[:, :, 1:], pad, w[:, :, :1]], axis=2)

    return window(ix), window(ix + 1 - 2 * (ix % 2))


def per_device(counts, old, prev, inc, c):
    V, X, Y, Z = inc.shape
    count = counts[0] * counts[1] * counts[2]
    merge_y = counts[1] == 2
    near = count <= 64
    R = Y + 8
    X1, Y1 = X // 2, Y // 2
    y_shape, x_shape = (V * (X // 2) + 1, 8, Z), (V * H + 1, Y, Z)
    shapes = [(V, X, Y, Z), x_shape, x_shape, y_shape]
    shapes += [] if merge_y else [y_shape]
    shapes += [(count, V, H + 1, Z), (X1, Y1, Z)]
    outs = run(
        near,
        functools.partial(first_kernel, counts, merge_y),
        shapes,
        (inc, c, old, prev),
        [inc.shape, c.shape, (X1 * Y, Z), old.shape, prev.shape],
        name="first",
        result=(len(shapes) - 2,),
        sems=V + 3,
    )
    g, xlo, xhi = outs[:3]
    c1 = outs[-1]
    slots0 = swap(outs[-2])
    xl, xh = shift(xhi, "gx", 1), shift(xlo, "gx", -1)
    if merge_y:
        yl = yh = shift(outs[3], "gy", 1)
    else:
        yl, yh = shift(outs[4], "gy", 1), shift(outs[3], "gy", -1)
    ext0, ext1 = (V + 1, X + 2 * H, R, Z), (V, X1 + 2 * H, 2 * Y1, Z)
    steps = edge_steps(merge_y)
    G, S, p1, slots1, c2s, *edges = run(
        near,
        functools.partial(second_kernel, counts, merge_y),
        [ext0, ext0, (V // 2, X1, Y1, Z), (count, TAIL + 1, V, Z), (count, V, Z)] + [(16, Z)] * len(steps),
        (g, c, c1, xl, xh, yl, yh, slots0),
        [(V * X1 * Y, Z), ext1[1:], ext1, ext1],
        name="second",
        result=(3,),
    )
    slots1 = swap(slots1)
    edges = [diagonal(counts, e, dx, dy) for e, (dx, dy) in zip(edges, steps)]
    xl, xh = shift(p1, "gx", 1), shift(p1, "gx", -1)
    if merge_y:
        yl = yh = shift(p1, "gy", 1)
    else:
        yl, yh = shift(p1, "gy", 1), shift(p1, "gy", -1)
    slots1, xl, xh, yl, yh, *edges = lax.optimization_barrier((slots1, xl, xh, yl, yh, *edges))
    G1, S1 = run(
        near,
        functools.partial(third_kernel, counts, merge_y),
        [ext1, ext1],
        (p1, xl, xh, yl, yh, slots1, *edges),
        name="third",
    )
    orth, proj, tri = run(
        near,
        functools.partial(ortho_kernel, count, float(count * X * Y * Z)),
        [(V, X, Y, Z), (4, 4), (4, 4)],
        (old, prev, slots0),
        name="ortho",
        result=(0, 1, 2),
        plain=(0, 1),
    )
    parts_y = Y // 4
    if near and counts[2] * (Z // parts_y) == Z and counts[0] % 4 == 0:
        sizes = [(counts[1] * parts_y, counts[0] // 2, 8, Z)]
        for level in range(3, LEVELS):
            y, x = sizes[-1][:2]
            sizes.append((y // 2, x if level < 5 else x // 2, 8, Z))
        weights = run(
            near, functools.partial(weights_kernel, counts, parts_y), sizes, (c2s,), name="weights"
        )
        e2, others = run(
            near,
            functools.partial(coarse_kernel, counts, parts_y),
            [(V // 2, 4, 8, Z)] * 2,
            (slots1, *weights),
            [sizes[0], (V, 4, 8, Z)],
            name="coarse",
        )
    else:
        e2, others = wide_coarse(counts, parts_y, c2s, slots1)
    others = lax.ppermute(others, "gx", [(i, i ^ 1) for i in range(counts[0])])
    pre, op = run(
        near,
        functools.partial(last_kernel, counts),
        [(V, X, Y, Z), (V, X, Y, Z)],
        (e2, others, G1, S1, G, S, c),
        [(V * X1 * 2 * Y1, Z), ext1, ((V + 1) * (X + 2) * R, Z), ext0, (V, X, Y, Z), (V, X, Y, Z)],
        name="last",
        result=(0, 1),
        out_sems=1 + X // 2,
    )
    return orth, proj, tri, pre, op


def solution(mesh):
    block = P(None, *AXES)
    counts = tuple(mesh.shape[a] for a in AXES)
    return jax.shard_map(
        functools.partial(per_device, counts),
        mesh=mesh,
        in_specs=(block, block, block, P(*AXES)),
        out_specs=(block, P(), P(), block, block),
        check_vma=False,
    )
```
